128 devices in a mesh: data: 1, time: 128 (over z, y, x, core).
Axes of the slice: x: 4, y: 4, z: 4, core: 2. Of those that a mesh axis runs over, the one named last changes fastest.
Arguments:
- x_init: float32 [1, 4096, 64], P('data')
- w_in: bfloat16 [64, 1536], replicated
- w_out: bfloat16 [1536, 64], replicated
- mod_scale: bfloat16 [128, 1536], P('time')
- mod_shift: bfloat16 [128, 1536], P('time')
- step_size: float32 [128], P('time')
Outputs:
- output: float32 [128, 1, 4096, 64], P('time', 'data')
All inputs are finite; a program needn't handle non-finite values.
Results may differ from the reference program's by a relative error of at most 0.001.
Values are sent between devices in bfloat16 or wider.
A program may use at most 1 GiB of HBM per device.

```python
import jax
import jax.numpy as jnp
from jax import lax

TOKENS = 4096
CHANNELS = 64
HIDDEN = 1536
STEPS_DEV = 1
BATCH = 1
TIME_DEVS = 128
SWEEPS = 4


def setup_inputs(seed: int = 0, part: int = 0) -> dict:
    total_steps = TIME_DEVS * STEPS_DEV
    keys = jax.random.split(jax.random.key(seed), 6)
    x_init = jax.random.normal(jax.random.fold_in(keys[0], part), (BATCH, TOKENS, CHANNELS), jnp.float32)
    w_in = jax.random.normal(keys[1], (CHANNELS, HIDDEN), jnp.float32) * (CHANNELS * total_steps) ** -0.5
    w_raw = jax.random.normal(keys[2], (HIDDEN, CHANNELS), jnp.float32)
    w_out = (w_raw - jnp.mean(w_raw, axis=0, keepdims=True)) * HIDDEN ** -0.5
    mod_scale = 0.5 * jax.random.normal(keys[3], (total_steps, HIDDEN), jnp.float32)
    mod_shift = jax.random.normal(keys[4], (total_steps, HIDDEN), jnp.float32)
    step_size = jax.random.uniform(keys[5], (total_steps,), jnp.float32, 0.5, 1.5) * (2.5 * total_steps ** -0.5)
    return {'x_init': x_init, 'w_in': w_in.astype(jnp.bfloat16), 'w_out': w_out.astype(jnp.bfloat16), 'mod_scale': mod_scale.astype(jnp.bfloat16), 'mod_shift': mod_shift.astype(jnp.bfloat16), 'step_size': step_size}


def drift_block(latent, scale_rows, shift_rows, step_rows, w_in, w_out):
    x_rounded = latent.astype(jnp.bfloat16).astype(jnp.float32)
    pre_act = jnp.einsum('kbnc,cd->kbnd', x_rounded, w_in.astype(jnp.float32))
    gain_rows = 1.0 + scale_rows.astype(jnp.float32)
    hidden = jax.nn.gelu(pre_act * gain_rows[:, None, None, :] + shift_rows.astype(jnp.float32)[:, None, None, :], approximate=True)
    out_act = jnp.einsum('kbnd,dc->kbnc', hidden.astype(jnp.bfloat16).astype(jnp.float32), w_out.astype(jnp.float32))
    return step_rows[:, None, None, None] * out_act


def reference(x_init, w_in, w_out, mod_scale, mod_shift, step_size):
    total_steps = TIME_DEVS * STEPS_DEV
    lat_shape = (BATCH, TOKENS, CHANNELS)
    scale_blocks = mod_scale.reshape(TIME_DEVS, STEPS_DEV, HIDDEN)
    shift_blocks = mod_shift.reshape(TIME_DEVS, STEPS_DEV, HIDDEN)
    step_blocks = step_size.reshape(TIME_DEVS, STEPS_DEV)

    def one_block(block):
        return drift_block(block[0], block[1], block[2], block[3], w_in, w_out)

    def one_sweep(sweep_idx, latent):
        lat_blocks = latent.reshape((TIME_DEVS, STEPS_DEV) + lat_shape)
        drifts = lax.map(one_block, (lat_blocks, scale_blocks, shift_blocks, step_blocks))
        drifts = drifts.reshape((total_steps,) + lat_shape)
        inclusive = jnp.cumsum(drifts, axis=0)
        exclusive = jnp.concatenate([jnp.zeros_like(drifts[:1]), inclusive[:-1]], axis=0)
        return x_init[None] + exclusive

    start = jnp.broadcast_to(x_init[None], (total_steps,) + lat_shape)
    return lax.fori_loop(0, SWEEPS, one_sweep, start)
```

```python
import functools

import jax
import jax.numpy as jnp
from jax import lax
from jax.experimental import pallas as pl
from jax.experimental.pallas import tpu as pltpu
from jax.sharding import PartitionSpec as P

SWEEPS = 4
C0 = 0.7978845608028654
C1 = C0 * 0.044715
STEPS_PER_BLOCK = 16
TILE = 256


def half_gelu(h):
    t = jnp.tanh(h * (h * h * (8.0 * C1) + 2.0 * C0))
    return h + h * t


def kernel(n_time, tok, x_hbm, w1_ref, w2t_ref, scale_ref, shift_ref, step_ref, out_ref,
           xcol, xrow, w2, mod_send, mod_recv, mods, p0, xbf, send, prefix,
           x_sem, mod_send_sem, mod_recv_sem, out_send_sem, out_recv_sem):
    me = lax.axis_index('time')
    hidden = w1_ref.shape[1]
    chans = w1_ref.shape[0]
    n_rows = hidden // 128
    per_col = 128 // tok

    x_copy = pltpu.make_async_copy(
        x_hbm.at[:, pl.ds(pl.multiple_of((me // per_col) * 128, 128), 128)], xcol, x_sem)
    x_copy.start()

    for c in range(n_rows):
        mod_send[pl.ds(c, 1), :] = scale_ref[:, c * 128:(c + 1) * 128]
        mod_send[pl.ds(n_rows + c, 1), :] = shift_ref[:, c * 128:(c + 1) * 128]
    step = jnp.broadcast_to(step_ref[...], (1, 128))
    high = step.astype(jnp.bfloat16)
    rest = step - high.astype(jnp.float32)
    mid = rest.astype(jnp.bfloat16)
    low = (rest - mid.astype(jnp.float32)).astype(jnp.bfloat16)
    mod_send[pl.ds(2 * n_rows, 1), :] = high
    mod_send[pl.ds(2 * n_rows + 1, 1), :] = mid
    mod_send[pl.ds(2 * n_rows + 2, 1), :] = low

    def send_mod(k, carry):
        dst = lax.rem(me + k, n_time)
        pltpu.make_async_remote_copy(
            src_ref=mod_send, dst_ref=mod_recv.at[me], send_sem=mod_send_sem, recv_sem=mod_recv_sem,
            device_id={'time': dst}, device_id_type=pl.DeviceIdType.MESH).start()
        return carry

    lax.fori_loop(1, n_time, send_mod, 0)
    mod_recv[me] = mod_send[...]

    w2[...] = w2t_ref[...].astype(jnp.float32).T.astype(jnp.bfloat16)
    x_copy.wait()
    xrow[...] = xcol[...].T
    x0 = xrow[pl.ds(pl.multiple_of(lax.rem(me, per_col) * tok, tok), tok), :]
    for n in range(hidden // TILE):
        p0[:, n * TILE:(n + 1) * TILE] = jnp.dot(
            x0.astype(jnp.bfloat16), w1_ref[:, n * TILE:(n + 1) * TILE], preferred_element_type=jnp.float32)

    pltpu.make_async_copy(mod_recv.at[pl.ds(0, n_time - 1)], mod_recv.at[pl.ds(0, n_time - 1)], mod_recv_sem).wait()
    pltpu.make_async_copy(mod_recv.at[pl.ds(0, n_time - 1)], mod_recv.at[pl.ds(0, n_time - 1)], mod_send_sem).wait()

    def unpack(j, carry):
        block = mod_recv[j].astype(jnp.float32)
        mods[j, pl.ds(0, n_rows), :] = 0.5 * (1.0 + block[:n_rows])
        mods[j, pl.ds(n_rows, n_rows), :] = 0.5 * block[n_rows:2 * n_rows]
        mods[j, pl.ds(2 * n_rows, 1), :] = (block[2 * n_rows:2 * n_rows + 1] + block[2 * n_rows + 1:2 * n_rows + 2]) + block[2 * n_rows + 2:2 * n_rows + 3]
        return carry

    lax.fori_loop(0, n_time, unpack, 0, unroll=4)

    rows = STEPS_PER_BLOCK * tok

    def block_step(sweep, b, carry):
        acc = None
        if sweep > 0:
            x = xbf[pl.ds(pl.multiple_of(b * rows, rows), rows), :]
        for n in range(hidden // TILE):
            if sweep > 0:
                pre = jnp.dot(x, w1_ref[:, n * TILE:(n + 1) * TILE], preferred_element_type=jnp.float32)
            parts = []
            for s in range(STEPS_PER_BLOCK):
                j = b * STEPS_PER_BLOCK + s
                halves = []
                for half in range(TILE // 128):
                    c = n * (TILE // 128) + half
                    gain = mods[j, pl.ds(c, 1), :]
                    shift = mods[j, pl.ds(n_rows + c, 1), :]
                    if sweep > 0:
                        p = pre[s * tok:(s + 1) * tok, half * 128:(half + 1) * 128]
                    else:
                        p = p0[:, c * 128:(c + 1) * 128]
                    halves.append(half_gelu(p * gain + shift).astype(jnp.bfloat16))
                parts.append(jnp.concatenate(halves, axis=1))
            act = jnp.concatenate(parts, axis=0)
            prod = jnp.dot(act, w2[n * TILE:(n + 1) * TILE, :], preferred_element_type=jnp.float32)
            acc = prod if acc is None else acc + prod
        total = prefix[...]
        for s in range(STEPS_PER_BLOCK):
            j = b * STEPS_PER_BLOCK + s
            new = x0 + total
            if sweep < SWEEPS - 1:
                xbf[pl.ds(pl.multiple_of(j * tok, tok), tok), :] = new.astype(jnp.bfloat16)
            else:
                send[j, :, 0:chans] = new[:tok // 2]
                send[j, :, chans:2 * chans] = new[tok // 2:]
            total = total + mods[j, pl.ds(2 * n_rows, 1), :][:, :chans] * acc[s * tok:(s + 1) * tok, :]
        prefix[...] = total
        return carry

    for sweep in range(SWEEPS):
        prefix[...] = jnp.zeros_like(prefix)
        lax.fori_loop(0, n_time // STEPS_PER_BLOCK, functools.partial(block_step, sweep), 0)

    def send_out(k, carry):
        dst = lax.rem(me + k, n_time)
        pltpu.make_async_remote_copy(
            src_ref=send.at[dst], dst_ref=out_ref.at[me], send_sem=out_send_sem, recv_sem=out_recv_sem,
            device_id={'time': dst}, device_id_type=pl.DeviceIdType.MESH).start()
        return carry

    lax.fori_loop(1, n_time, send_out, 0)
    out_ref[me] = send[me]
    pltpu.make_async_copy(send.at[pl.ds(0, n_time - 1)], send.at[pl.ds(0, n_time - 1)], out_send_sem).wait()
    pltpu.make_async_copy(out_ref.at[pl.ds(0, n_time - 1)], out_ref.at[pl.ds(0, n_time - 1)], out_recv_sem).wait()


def solution(mesh):
    n_time = mesh.shape['time']

    def per_device(x_init, w_in, w_out, mod_scale, mod_shift, step_size):
        _, tokens, chans = x_init.shape
        hidden = w_in.shape[1]
        tok = tokens // n_time
        vmem = pl.BlockSpec(memory_space=pltpu.VMEM)
        out = pl.pallas_call(
            functools.partial(kernel, n_time, tok),
            out_shape=jax.ShapeDtypeStruct((n_time, tok // 2, 2 * chans), jnp.float32),
            in_specs=[pl.BlockSpec(memory_space=pl.ANY), vmem, vmem, vmem, vmem, vmem],
            out_specs=vmem,
            scratch_shapes=[
                pltpu.VMEM((chans, 128), jnp.float32),
                pltpu.VMEM((128, chans), jnp.float32),
                pltpu.VMEM((hidden, chans), jnp.bfloat16),
                pltpu.VMEM((32, 128), jnp.bfloat16),
                pltpu.VMEM((n_time, 32, 128), jnp.bfloat16),
                pltpu.VMEM((n_time, 32, 128), jnp.float32),
                pltpu.VMEM((tok, hidden), jnp.float32),
                pltpu.VMEM((n_time * tok, chans), jnp.bfloat16),
                pltpu.VMEM((n_time, tok // 2, 2 * chans), jnp.float32),
                pltpu.VMEM((tok, chans), jnp.float32),
            ] + [pltpu.SemaphoreType.DMA] * 5,
            compiler_params=pltpu.CompilerParams(has_side_effects=True),
            name='sweeps',
        )(x_init[0].T, w_in, w_out.T, mod_scale, mod_shift, step_size[None])
        out = out.reshape(n_time, tok // 2, 2, chans).transpose(0, 2, 1, 3)
        return out.reshape(1, 1, tokens, chans)

    return jax.shard_map(per_device, mesh=mesh, in_specs=(P('data'), P(), P(), P('time'), P('time'), P('time')), out_specs=P('time', 'data'), check_vma=False)
```

```python
import functools

import jax
import jax.numpy as jnp
from jax import lax
from jax.experimental import pallas as pl
from jax.experimental.pallas import tpu as pltpu
from jax.sharding import PartitionSpec as P

SWEEPS = 4
C0 = 0.7978845608028654
C1 = C0 * 0.044715
TILE = 256
ROWS = 512
CHUNKS = 2
GROUP = 8
CHIP_STRIDE = 27
DEV_STRIDE = 45
MESH = pl.DeviceIdType.MESH


def half_gelu(h):
    t = jnp.tanh(h * (h * h * (8.0 * C1) + 2.0 * C0))
    return h + h * t


def wait_bytes(ref, sem):
    pltpu.make_async_copy(ref, ref, sem).wait()


def kernel(n_time, x_hbm, w1_ref, w2t_ref, scale_ref, shift_ref, step_ref, out_ref,
           xcol, xrow, w2, mod_send, mod_recv, mods, p0, xbf, send, prefix,
           x_sem, mod_send_sem, mod_recv_sem, pair_send_sem, pair_recv_sem, out_send_sem, out_recv_sem):
    me = lax.axis_index('time')
    n_chips = n_time // 2
    chip = me // 2
    core = lax.rem(me, 2)
    partner = me + 1 - 2 * core
    chans, hidden = w1_ref.shape
    n_rows = hidden // 128
    tok = 2 * GROUP
    tokens = x_hbm.shape[1]

    barrier = pltpu.get_barrier_semaphore()

    def arrive(k, carry):
        pl.semaphore_signal(barrier, inc=1, device_id={'time': lax.rem(me + k * DEV_STRIDE, n_time)}, device_id_type=MESH)
        return carry

    lax.fori_loop(1, n_time, arrive, 0)

    x_copies = []
    for q in range(CHUNKS):
        for half in range(2):
            start = half * (tokens // 2) + q * (tokens // 2 // CHUNKS) + (me * GROUP // 128) * 128
            x_copies.append(pltpu.make_async_copy(
                x_hbm.at[:, pl.ds(pl.multiple_of(start, 128), 128)], xcol.at[2 * q + half], x_sem.at[2 * q + half]))
            x_copies[-1].start()

    for c in range(n_rows):
        mod_send[pl.ds(c, 1), :] = scale_ref[:, c * 128:(c + 1) * 128]
        mod_send[pl.ds(n_rows + c, 1), :] = shift_ref[:, c * 128:(c + 1) * 128]
    step = jnp.broadcast_to(step_ref[...], (1, 128))
    high = step.astype(jnp.bfloat16)
    rest = step - high.astype(jnp.float32)
    mid = rest.astype(jnp.bfloat16)
    low = (rest - mid.astype(jnp.float32)).astype(jnp.bfloat16)
    mod_send[pl.ds(2 * n_rows, 1), :] = high
    mod_send[pl.ds(2 * n_rows + 1, 1), :] = mid
    mod_send[pl.ds(2 * n_rows + 2, 1), :] = low

    w2[...] = w2t_ref[...].astype(jnp.float32).T.astype(jnp.bfloat16)
    for copy in x_copies:
        copy.wait()
    for i in range(2 * CHUNKS):
        xrow[i] = xcol[i].T

    def x_tokens(q):
        lo = pl.ds(pl.multiple_of(lax.rem(me * GROUP, 128), GROUP), GROUP)
        return jnp.concatenate([xrow[2 * q, lo, :], xrow[2 * q + 1, lo, :]], axis=0)

    for q in range(CHUNKS):
        x0 = x_tokens(q).astype(jnp.bfloat16)
        for n in range(hidden // TILE):
            p0[q, :, n * TILE:(n + 1) * TILE] = jnp.dot(
                x0, w1_ref[:, n * TILE:(n + 1) * TILE], preferred_element_type=jnp.float32)

    pl.semaphore_wait(barrier, n_time - 1)

    def mod_copy(offset):
        return pltpu.make_async_remote_copy(
            src_ref=mod_send, dst_ref=mod_recv.at[me], send_sem=mod_send_sem, recv_sem=mod_recv_sem.at[offset],
            device_id={'time': lax.rem(chip + offset, n_chips) * 2 + core}, device_id_type=MESH)

    def pair_copy(src, src_ref):
        return pltpu.make_async_remote_copy(
            src_ref=src_ref, dst_ref=mod_recv.at[src], send_sem=pair_send_sem, recv_sem=pair_recv_sem,
            device_id={'time': partner}, device_id_type=MESH)

    def send_mod(k, carry):
        mod_copy(lax.rem(k * CHIP_STRIDE, n_chips)).start()
        return carry

    pair_copy(me, mod_send).start()
    lax.fori_loop(1, n_chips, send_mod, 0)
    mod_recv[me] = mod_send[...]

    def relay(k, carry):
        offset = lax.rem(k * CHIP_STRIDE, n_chips)
        mod_copy(offset).wait_recv()
        src = lax.rem(chip - offset + n_chips, n_chips) * 2 + core
        pair_copy(src, mod_recv.at[src]).start()
        return carry

    lax.fori_loop(1, n_chips, relay, 0)
    half_block = mod_recv.at[pl.ds(0, n_chips)]
    wait_bytes(half_block, pair_recv_sem)
    wait_bytes(half_block, pair_send_sem)
    wait_bytes(mod_recv.at[pl.ds(0, n_chips - 1)], mod_send_sem)

    def unpack(j, carry):
        block = mod_recv[j].astype(jnp.float32)
        mods[j, pl.ds(0, n_rows), :] = 0.5 * (1.0 + block[:n_rows])
        mods[j, pl.ds(n_rows, n_rows), :] = 0.5 * block[n_rows:2 * n_rows]
        mods[j, pl.ds(2 * n_rows, 1), :] = (block[2 * n_rows:2 * n_rows + 1] + block[2 * n_rows + 1:2 * n_rows + 2]) + block[2 * n_rows + 2:2 * n_rows + 3]
        return carry

    lax.fori_loop(0, n_time, unpack, 0, unroll=4)

    steps = ROWS // tok

    def block_step(q, first, b, carry):
        acc = None
        if not first:
            x = xbf[pl.ds(pl.multiple_of(b * ROWS, ROWS), ROWS), :]
        for n in range(hidden // TILE):
            if not first:
                pre = jnp.dot(x, w1_ref[:, n * TILE:(n + 1) * TILE], preferred_element_type=jnp.float32)
            parts = []
            for s in range(steps):
                j = b * steps + s
                halves = []
                for half in range(TILE // 128):
                    c = n * (TILE // 128) + half
                    gain = mods[j, pl.ds(c, 1), :]
                    shift = mods[j, pl.ds(n_rows + c, 1), :]
                    if not first:
                        p = pre[s * tok:(s + 1) * tok, half * 128:(half + 1) * 128]
                    else:
                        p = p0[q, :, c * 128:(c + 1) * 128]
                    halves.append(half_gelu(p * gain + shift).astype(jnp.bfloat16))
                parts.append(jnp.concatenate(halves, axis=1))
            act = jnp.concatenate(parts, axis=0)
            prod = jnp.dot(act, w2[n * TILE:(n + 1) * TILE, :], preferred_element_type=jnp.float32)
            acc = prod if acc is None else acc + prod
        x0 = x_tokens(q)
        total = prefix[...]
        for s in range(steps):
            j = b * steps + s
            new = x0 + total
            xbf[pl.ds(pl.multiple_of(j * tok, tok), tok), :] = new.astype(jnp.bfloat16)
            send[q, j, :, 0:chans] = new[:GROUP]
            send[q, j, :, chans:2 * chans] = new[GROUP:]
            total = total + mods[j, pl.ds(2 * n_rows, 1), :][:, :chans] * acc[s * tok:(s + 1) * tok, :]
        prefix[...] = total
        return carry

    def chunk(q, carry):
        def sweep(first):
            prefix[...] = jnp.zeros_like(prefix)
            lax.fori_loop(0, n_time // steps, functools.partial(block_step, q, first), 0)

        def later_sweep(i, carry):
            sweep(False)
            return carry

        sweep(True)
        lax.fori_loop(1, SWEEPS, later_sweep, 0)

        def send_out(k, carry):
            dst = lax.rem(me + k * DEV_STRIDE, n_time)
            pltpu.make_async_remote_copy(
                src_ref=send.at[q, dst], dst_ref=out_ref.at[q, me], send_sem=out_send_sem, recv_sem=out_recv_sem,
                device_id={'time': dst}, device_id_type=MESH).start()
            return carry

        lax.fori_loop(1, n_time, send_out, 0)
        out_ref[q, me] = send[q, me]
        return carry

    lax.fori_loop(0, CHUNKS, chunk, 0)
    others = out_ref.at[:, pl.ds(0, n_time - 1)]
    wait_bytes(others, out_send_sem)
    wait_bytes(others, out_recv_sem)


def spread(rows_ref, out_ref):
    chans, tokens = out_ref.shape
    for i in range(rows_ref.shape[0] // 128):
        cols = rows_ref[i * 128:(i + 1) * 128, :].T
        out_ref[:, i * 128:(i + 1) * 128] = cols[:chans]
        out_ref[:, tokens // 2 + i * 128:tokens // 2 + (i + 1) * 128] = cols[chans:]


def solution(mesh):
    n_time = mesh.shape['time']

    def per_device(x_init, w_in, w_out, mod_scale, mod_shift, step_size):
        _, tokens, chans = x_init.shape
        hidden = w_in.shape[1]
        tok = 2 * GROUP
        vmem = pl.BlockSpec(memory_space=pltpu.VMEM)
        out = pl.pallas_call(
            functools.partial(kernel, n_time),
            out_shape=jax.ShapeDtypeStruct((CHUNKS, n_time, GROUP, 2 * chans), jnp.float32),
            in_specs=[pl.BlockSpec(memory_space=pl.ANY), vmem, vmem, vmem, vmem, vmem],
            out_specs=vmem,
            scratch_shapes=[
                pltpu.VMEM((2 * CHUNKS, chans, 128), jnp.float32),
                pltpu.VMEM((2 * CHUNKS, 128, chans), jnp.float32),
                pltpu.VMEM((hidden, chans), jnp.bfloat16),
                pltpu.VMEM((32, 128), jnp.bfloat16),
                pltpu.VMEM((n_time, 32, 128), jnp.bfloat16),
                pltpu.VMEM((n_time, 32, 128), jnp.float32),
                pltpu.VMEM((CHUNKS, tok, hidden), jnp.float32),
                pltpu.VMEM((n_time * tok, chans), jnp.bfloat16),
                pltpu.VMEM((CHUNKS, n_time, GROUP, 2 * chans), jnp.float32),
                pltpu.VMEM((tok, chans), jnp.float32),
                pltpu.SemaphoreType.DMA((2 * CHUNKS,)),
                pltpu.SemaphoreType.DMA,
                pltpu.SemaphoreType.DMA((n_time // 2,)),
            ] + [pltpu.SemaphoreType.DMA] * 4,
            compiler_params=pltpu.CompilerParams(has_side_effects=True, collective_id=0),
            name='sweeps',
        )(x_init[0].T, w_in, w_out.T, mod_scale, mod_shift, step_size[None])
        out = pl.pallas_call(
            spread, out_shape=jax.ShapeDtypeStruct((chans, tokens), jnp.float32),
            in_specs=[vmem], out_specs=vmem, name='spread',
        )(out.reshape(tokens // 2, 2 * chans))
        return out.T.reshape(1, 1, tokens, chans)

    return jax.shard_map(per_device, mesh=mesh, in_specs=(P('data'), P(), P(), P('time'), P('time'), P('time')), out_specs=P('time', 'data'), check_vma=False)
```

```python
import functools

import jax
import jax.numpy as jnp
from jax import lax
from jax.experimental import pallas as pl
from jax.experimental.pallas import tpu as pltpu
from jax.sharding import PartitionSpec as P

SWEEPS = 4
C0 = 0.7978845608028654
C1 = C0 * 0.044715
TILE = 256
ROWS = 1024
CHUNKS = 2
GROUP = 8
SIDE = 4
ARRIVE = 8
DEV_STRIDE = 45
MESH = pl.DeviceIdType.MESH


def half_gelu(h):
    t = jnp.tanh(h * (h * h * (8.0 * C1) + 2.0 * C0))
    return h + h * t


def wait_bytes(ref, sem):
    pltpu.make_async_copy(ref, ref, sem).wait()


def hop(t):
    return t + (t // 2) * (1 - 2 * lax.rem(t, 2))


def chip_at(chip, k, sign):
    pos, out, scale = chip, 0, 1
    for _ in range(3):
        out = out + scale * lax.rem(lax.rem(pos, SIDE) + sign * hop(lax.rem(k, SIDE)) + SIDE, SIDE)
        pos, k, scale = pos // SIDE, k // SIDE, scale * SIDE
    return out


def kernel(n_time, x_hbm, w1_ref, w2t_ref, scale_ref, shift_ref, step_ref, out_ref,
           xcol, xrow, x0, w2, mod_send, mod_recv, mods, p0, drift, xbf, send, recv, prefix,
           x_sem, mod_send_sem, mod_recv_sem, pair_send_sem, pair_recv_sem, out_send_sem, out_recv_sem):
    me = lax.axis_index('time')
    n_chips = n_time // 2
    chip = me // 2
    core = lax.rem(me, 2)
    partner = me + 1 - 2 * core
    chans, hidden = w1_ref.shape
    n_rows = hidden // 128
    tok = 2 * GROUP
    tokens = x_hbm.shape[1]

    barrier = pltpu.get_barrier_semaphore()

    def arrive(k, carry):
        pl.semaphore_signal(barrier, inc=1, device_id={'time': lax.rem(me + k * DEV_STRIDE, n_time)}, device_id_type=MESH)
        return carry

    lax.fori_loop(1, n_time, arrive, 0)

    x_copies = []
    for i in range(2 * CHUNKS):
        start = (i % 2) * (tokens // 2) + (i // 2) * (tokens // 2 // CHUNKS) + (me * GROUP // 128) * 128
        x_copies.append(pltpu.make_async_copy(
            x_hbm.at[:, pl.ds(pl.multiple_of(start, 128), 128)], xcol.at[i], x_sem.at[i]))
        x_copies[-1].start()

    for c in range(n_rows):
        mod_send[pl.ds(c, 1), :] = scale_ref[:, c * 128:(c + 1) * 128]
        mod_send[pl.ds(n_rows + c, 1), :] = shift_ref[:, c * 128:(c + 1) * 128]
    step = jnp.broadcast_to(step_ref[...], (1, 128))
    high = step.astype(jnp.bfloat16)
    rest = step - high.astype(jnp.float32)
    mid = rest.astype(jnp.bfloat16)
    low = (rest - mid.astype(jnp.float32)).astype(jnp.bfloat16)
    mod_send[pl.ds(2 * n_rows, 1), :] = high
    mod_send[pl.ds(2 * n_rows + 1, 1), :] = mid
    mod_send[pl.ds(2 * n_rows + 2, 1), :] = low
    mod_recv[me] = mod_send[...]

    w2[...] = w2t_ref[...].astype(jnp.float32).T.astype(jnp.bfloat16)
    lo = pl.ds(pl.multiple_of(lax.rem(me * GROUP, 128), GROUP), GROUP)
    for i in range(2 * CHUNKS):
        x_copies[i].wait()
        xrow[i] = xcol[i].T
        x0[i * GROUP:(i + 1) * GROUP, :] = xrow[i, lo, :]
    x0_rounded = x0[...].astype(jnp.bfloat16)
    for n in range(hidden // TILE):
        p0[:, n * TILE:(n + 1) * TILE] = jnp.dot(
            x0_rounded, w1_ref[:, n * TILE:(n + 1) * TILE], preferred_element_type=jnp.float32)

    pl.semaphore_wait(barrier, n_time - 1)

    def mod_copy(k):
        return pltpu.make_async_remote_copy(
            src_ref=mod_send, dst_ref=mod_recv.at[me], send_sem=mod_send_sem, recv_sem=mod_recv_sem.at[k],
            device_id={'time': chip_at(chip, k, 1) * 2 + core}, device_id_type=MESH)

    def pair_copy(k, src, src_ref):
        return pltpu.make_async_remote_copy(
            src_ref=src_ref, dst_ref=mod_recv.at[src], send_sem=pair_send_sem, recv_sem=pair_recv_sem.at[k],
            device_id={'time': partner}, device_id_type=MESH)

    def send_mod(k, carry):
        mod_copy(k).start()
        return carry

    def relay(k, carry):
        mod_copy(k).wait_recv()
        src = chip_at(chip, k, -1) * 2 + core
        pair_copy(k, src, mod_recv.at[src]).start()
        return carry

    def pair_wait(k, carry):
        pair_copy(k, me, mod_send).wait_recv()
        return carry

    pair_copy(0, me, mod_send).start()
    lax.fori_loop(1, n_chips, send_mod, 0)
    lax.fori_loop(1, ARRIVE, relay, 0)

    def first_sweep(g, carry):
        lax.fori_loop((g + 1) * ARRIVE, jnp.minimum((g + 2) * ARRIVE, n_chips), relay, 0)
        lax.fori_loop(g * ARRIVE, (g + 1) * ARRIVE, pair_wait, 0)
        steps = []
        for i in range(ARRIVE):
            owner = chip_at(chip, g * ARRIVE + i, -1)
            steps += [2 * owner, 2 * owner + 1]
        for j in steps:
            block = mod_recv[j].astype(jnp.float32)
            mods[j, pl.ds(0, n_rows), :] = 0.5 * (1.0 + block[:n_rows])
            mods[j, pl.ds(n_rows, n_rows), :] = 0.5 * block[n_rows:2 * n_rows]
            mods[j, pl.ds(2 * n_rows, 1), :] = (block[2 * n_rows:2 * n_rows + 1] + block[2 * n_rows + 1:2 * n_rows + 2]) + block[2 * n_rows + 2:2 * n_rows + 3]
        acc = None
        for n in range(hidden // TILE):
            parts = []
            for j in steps:
                halves = []
                for c in range(n * (TILE // 128), (n + 1) * (TILE // 128)):
                    h = p0[:, c * 128:(c + 1) * 128] * mods[j, pl.ds(c, 1), :] + mods[j, pl.ds(n_rows + c, 1), :]
                    halves.append(half_gelu(h).astype(jnp.bfloat16))
                parts.append(jnp.concatenate(halves, axis=1))
            act = jnp.concatenate(parts, axis=0)
            prod = jnp.dot(act, w2[n * TILE:(n + 1) * TILE, :], preferred_element_type=jnp.float32)
            acc = prod if acc is None else acc + prod
        for i, j in enumerate(steps):
            drift[j] = mods[j, pl.ds(2 * n_rows, 1), :][:, :chans] * acc[i * CHUNKS * tok:(i + 1) * CHUNKS * tok, :]
        return carry

    lax.fori_loop(0, n_chips // ARRIVE, first_sweep, 0)

    def first_prefix(j, total):
        new = (x0[...] + total).astype(jnp.bfloat16)
        for q in range(CHUNKS):
            xbf[q, pl.ds(pl.multiple_of(j * tok, tok), tok), :] = new[q * tok:(q + 1) * tok]
        return total + drift[j]

    lax.fori_loop(0, n_time, first_prefix, jnp.zeros((CHUNKS * tok, chans), jnp.float32), unroll=8)

    steps = ROWS // tok

    def block_step(q, b, carry):
        acc = None
        x = xbf[q, pl.ds(pl.multiple_of(b * ROWS, ROWS), ROWS), :]
        for n in range(hidden // TILE):
            pre = jnp.dot(x, w1_ref[:, n * TILE:(n + 1) * TILE], preferred_element_type=jnp.float32)
            parts = []
            for s in range(steps):
                j = b * steps + s
                halves = []
                for half in range(TILE // 128):
                    c = n * (TILE // 128) + half
                    p = pre[s * tok:(s + 1) * tok, half * 128:(half + 1) * 128]
                    h = p * mods[j, pl.ds(c, 1), :] + mods[j, pl.ds(n_rows + c, 1), :]
                    halves.append(half_gelu(h).astype(jnp.bfloat16))
                parts.append(jnp.concatenate(halves, axis=1))
            act = jnp.concatenate(parts, axis=0)
            prod = jnp.dot(act, w2[n * TILE:(n + 1) * TILE, :], preferred_element_type=jnp.float32)
            acc = prod if acc is None else acc + prod
        start = x0[pl.ds(pl.multiple_of(q * tok, tok), tok), :]
        total = prefix[...]
        for s in range(steps):
            j = b * steps + s
            new = start + total
            xbf[q, pl.ds(pl.multiple_of(j * tok, tok), tok), :] = new.astype(jnp.bfloat16)
            send[q, j, :, 0:chans] = new[:GROUP]
            send[q, j, :, chans:2 * chans] = new[GROUP:]
            total = total + mods[j, pl.ds(2 * n_rows, 1), :][:, :chans] * acc[s * tok:(s + 1) * tok, :]
        prefix[...] = total
        return carry

    def chunk(q, carry):
        def sweep(i, carry):
            prefix[...] = jnp.zeros_like(prefix)
            return lax.fori_loop(0, n_time // steps, functools.partial(block_step, q), carry)

        lax.fori_loop(1, SWEEPS, sweep, 0)

        def out_copy(dst):
            return pltpu.make_async_remote_copy(
                src_ref=send.at[q, dst], dst_ref=recv.at[q, me], send_sem=out_send_sem, recv_sem=out_recv_sem.at[q],
                device_id={'time': dst}, device_id_type=MESH)

        def send_out(i, carry):
            other = chip_at(chip, n_chips - 1 - i, 1)
            out_copy(2 * other + core).start()
            out_copy(2 * other + 1 - core).start()
            return carry

        lax.fori_loop(0, n_chips - 1, send_out, 0)
        out_copy(partner).start()
        recv[q, me] = send[q, me]
        return carry

    lax.fori_loop(0, CHUNKS, chunk, 0)

    half_block = mod_recv.at[pl.ds(0, n_chips)]
    wait_bytes(half_block, pair_send_sem)
    wait_bytes(mod_recv.at[pl.ds(0, n_chips - 1)], mod_send_sem)
    for q in range(CHUNKS):
        wait_bytes(recv.at[q, pl.ds(0, n_time - 1)], out_recv_sem.at[q])
        for i in range(n_time * GROUP // 128):
            rows = recv[q, i * (128 // GROUP):(i + 1) * (128 // GROUP)].reshape(128, 2 * chans).T
            at = (q * n_time * GROUP) + i * 128
            out_ref[:, at:at + 128] = rows[:chans]
            out_ref[:, tokens // 2 + at:tokens // 2 + at + 128] = rows[chans:]
    wait_bytes(recv.at[:, pl.ds(0, n_time - 1)], out_send_sem)


def solution(mesh):
    n_time = mesh.shape['time']

    def per_device(x_init, w_in, w_out, mod_scale, mod_shift, step_size):
        _, tokens, chans = x_init.shape
        hidden = w_in.shape[1]
        tok = 2 * GROUP
        f32, bf16 = jnp.float32, jnp.bfloat16
        vmem = pl.BlockSpec(memory_space=pltpu.VMEM)
        out = pl.pallas_call(
            functools.partial(kernel, n_time),
            out_shape=jax.ShapeDtypeStruct((chans, tokens), f32),
            in_specs=[pl.BlockSpec(memory_space=pl.ANY), vmem, vmem, vmem, vmem, vmem],
            out_specs=vmem,
            scratch_shapes=[
                pltpu.VMEM((2 * CHUNKS, chans, 128), f32),
                pltpu.VMEM((2 * CHUNKS, 128, chans), f32),
                pltpu.VMEM((CHUNKS * tok, chans), f32),
                pltpu.VMEM((hidden, chans), bf16),
                pltpu.VMEM((32, 128), bf16),
                pltpu.VMEM((n_time, 32, 128), bf16),
                pltpu.VMEM((n_time, 32, 128), f32),
                pltpu.VMEM((CHUNKS * tok, hidden), f32),
                pltpu.VMEM((n_time, CHUNKS * tok, chans), f32),
                pltpu.VMEM((CHUNKS, n_time * tok, chans), bf16),
                pltpu.VMEM((CHUNKS, n_time, GROUP, 2 * chans), f32),
                pltpu.VMEM((CHUNKS, n_time, GROUP, 2 * chans), f32),
                pltpu.VMEM((tok, chans), f32),
                pltpu.SemaphoreType.DMA((2 * CHUNKS,)),
                pltpu.SemaphoreType.DMA,
                pltpu.SemaphoreType.DMA((n_time // 2,)),
                pltpu.SemaphoreType.DMA,
                pltpu.SemaphoreType.DMA((n_time // 2,)),
                pltpu.SemaphoreType.DMA,
                pltpu.SemaphoreType.DMA((CHUNKS,)),
            ],
            compiler_params=pltpu.CompilerParams(has_side_effects=True, collective_id=0),
            name='sweeps',
        )(x_init[0].T, w_in, w_out.T, mod_scale, mod_shift, step_size[None])
        return out.T.reshape(1, 1, tokens, chans)

    return jax.shard_map(per_device, mesh=mesh, in_specs=(P('data'), P(), P(), P('time'), P('time'), P('time')), out_specs=P('time', 'data'), check_vma=False)
```

```python
import functools

import jax
import jax.numpy as jnp
from jax import lax
from jax.experimental import pallas as pl
from jax.experimental.pallas import tpu as pltpu
from jax.sharding import PartitionSpec as P

SWEEPS = 4
C0 = 0.7978845608028654
C1 = C0 * 0.044715
TILE = 256
ROWS = 1024
CHUNKS = 2
GROUP = 8
SIDE = 4
ARRIVE = 8
AHEAD = 4
DEV_STRIDE = 45
MESH = pl.DeviceIdType.MESH


def half_gelu(h):
    t = jnp.tanh(h * (h * h * (8.0 * C1) + 2.0 * C0))
    return h + h * t


def wait_bytes(ref, sem):
    pltpu.make_async_copy(ref, ref, sem).wait()


def hop(t):
    return t + (t // 2) * (1 - 2 * lax.rem(t, 2))


def chip_at(chip, k, sign):
    pos, out, scale = chip, 0, 1
    for _ in range(3):
        out = out + scale * lax.rem(lax.rem(pos, SIDE) + sign * hop(lax.rem(k, SIDE)) + SIDE, SIDE)
        pos, k, scale = pos // SIDE, k // SIDE, scale * SIDE
    return out


def kernel(n_time, x_hbm, w1_hbm, w2t_hbm, scale_hbm, shift_hbm, step_ref, out_ref,
           w1_ref, w2t_ref, scale_ref, shift_ref, xcol, xrow, x0, w2, mod_send, mod_recv, mods, p0, drift, xbf, send, recv, prefix,
           load_sem, x_sem, mod_send_sem, mod_recv_sem, pair_send_sem, pair_recv_sem, out_send_sem, out_recv_sem):
    me = lax.axis_index('time')
    n_chips = n_time // 2
    chip = me // 2
    core = lax.rem(me, 2)
    partner = me + 1 - 2 * core
    chans, hidden = w1_ref.shape
    n_rows = hidden // 128
    tok = 2 * GROUP
    tokens = x_hbm.shape[1]

    barrier = pltpu.get_barrier_semaphore()

    def arrive(k, carry):
        pl.semaphore_signal(barrier, inc=1, device_id={'time': lax.rem(me + k * DEV_STRIDE, n_time)}, device_id_type=MESH)
        return carry

    lax.fori_loop(1, n_time, arrive, 0)

    loads = [pltpu.make_async_copy(src, dst, load_sem.at[i]) for i, (src, dst) in enumerate(
        [(scale_hbm, scale_ref), (shift_hbm, shift_ref), (w2t_hbm, w2t_ref), (w1_hbm, w1_ref)])]
    for load in loads:
        load.start()
    x_copies = []
    for i in range(2 * CHUNKS):
        start = (i % 2) * (tokens // 2) + (i // 2) * (tokens // 2 // CHUNKS) + (me * GROUP // 128) * 128
        x_copies.append(pltpu.make_async_copy(
            x_hbm.at[:, pl.ds(pl.multiple_of(start, 128), 128)], xcol.at[i], x_sem.at[i]))
        x_copies[-1].start()

    loads[0].wait()
    loads[1].wait()
    for c in range(n_rows):
        mod_send[pl.ds(c, 1), :] = scale_ref[:, c * 128:(c + 1) * 128]
        mod_send[pl.ds(n_rows + c, 1), :] = shift_ref[:, c * 128:(c + 1) * 128]
    step = jnp.broadcast_to(step_ref[...], (1, 128))
    high = step.astype(jnp.bfloat16)
    rest = step - high.astype(jnp.float32)
    mid = rest.astype(jnp.bfloat16)
    low = (rest - mid.astype(jnp.float32)).astype(jnp.bfloat16)
    mod_send[pl.ds(2 * n_rows, 1), :] = high
    mod_send[pl.ds(2 * n_rows + 1, 1), :] = mid
    mod_send[pl.ds(2 * n_rows + 2, 1), :] = low
    mod_recv[me] = mod_send[...]

    loads[2].wait()
    w2[...] = w2t_ref[...].astype(jnp.float32).T.astype(jnp.bfloat16)
    lo = pl.ds(pl.multiple_of(lax.rem(me * GROUP, 128), GROUP), GROUP)
    for i in range(2 * CHUNKS):
        x_copies[i].wait()
        xrow[i] = xcol[i].T
        x0[i * GROUP:(i + 1) * GROUP, :] = xrow[i, lo, :]
    loads[3].wait()
    x0_rounded = x0[...].astype(jnp.bfloat16)
    for n in range(hidden // TILE):
        p0[:, n * TILE:(n + 1) * TILE] = jnp.dot(
            x0_rounded, w1_ref[:, n * TILE:(n + 1) * TILE], preferred_element_type=jnp.float32)

    pl.semaphore_wait(barrier, n_time - 1)

    def mod_copy(k):
        return pltpu.make_async_remote_copy(
            src_ref=mod_send, dst_ref=mod_recv.at[me], send_sem=mod_send_sem, recv_sem=mod_recv_sem.at[k],
            device_id={'time': chip_at(chip, k, 1) * 2 + core}, device_id_type=MESH)

    def pair_copy(k, src, src_ref):
        return pltpu.make_async_remote_copy(
            src_ref=src_ref, dst_ref=mod_recv.at[src], send_sem=pair_send_sem, recv_sem=pair_recv_sem.at[k],
            device_id={'time': partner}, device_id_type=MESH)

    def send_mod(k, carry):
        mod_copy(k).start()
        return carry

    def relay(k, carry):
        mod_copy(k).wait_recv()
        src = chip_at(chip, k, -1) * 2 + core
        pair_copy(k, src, mod_recv.at[src]).start()
        return carry

    def pair_wait(k, carry):
        pair_copy(k, me, mod_send).wait_recv()
        return carry

    def group(g):
        steps = []
        for i in range(ARRIVE):
            owner = chip_at(chip, g * ARRIVE + i, -1)
            steps += [2 * owner, 2 * owner + 1]
        return steps

    def unpack(g):
        for j in group(g):
            block = mod_recv[j].astype(jnp.float32)
            mods[j, pl.ds(0, n_rows), :] = 0.5 * (1.0 + block[:n_rows])
            mods[j, pl.ds(n_rows, n_rows), :] = 0.5 * block[n_rows:2 * n_rows]
            mods[j, pl.ds(2 * n_rows, 1), :] = (block[2 * n_rows:2 * n_rows + 1] + block[2 * n_rows + 1:2 * n_rows + 2]) + block[2 * n_rows + 2:2 * n_rows + 3]

    def each(g, body):
        lax.fori_loop(jnp.minimum(g * ARRIVE, n_chips), jnp.minimum((g + 1) * ARRIVE, n_chips), body, 0)

    pair_copy(0, me, mod_send).start()
    lax.fori_loop(1, AHEAD * ARRIVE, send_mod, 0)
    lax.fori_loop(1, 2 * ARRIVE, relay, 0)
    each(0, pair_wait)
    unpack(0)

    def first_sweep(g, carry):
        each(g + AHEAD, send_mod)
        each(g + 2, relay)
        each(g + 1, pair_wait)
        steps = group(g)
        acc = None
        for n in range(hidden // TILE):
            parts = []
            for j in steps:
                halves = []
                for c in range(n * (TILE // 128), (n + 1) * (TILE // 128)):
                    h = p0[:, c * 128:(c + 1) * 128] * mods[j, pl.ds(c, 1), :] + mods[j, pl.ds(n_rows + c, 1), :]
                    halves.append(half_gelu(h).astype(jnp.bfloat16))
                parts.append(jnp.concatenate(halves, axis=1))
            act = jnp.concatenate(parts, axis=0)
            prod = jnp.dot(act, w2[n * TILE:(n + 1) * TILE, :], preferred_element_type=jnp.float32)
            acc = prod if acc is None else acc + prod
        for i, j in enumerate(steps):
            drift[j] = mods[j, pl.ds(2 * n_rows, 1), :][:, :chans] * acc[i * CHUNKS * tok:(i + 1) * CHUNKS * tok, :]
        unpack(lax.rem(g + 1, n_chips // ARRIVE))
        return carry

    lax.fori_loop(0, n_chips // ARRIVE, first_sweep, 0)

    def first_prefix(j, total):
        new = (x0[...] + total).astype(jnp.bfloat16)
        for q in range(CHUNKS):
            xbf[q, pl.ds(pl.multiple_of(j * tok, tok), tok), :] = new[q * tok:(q + 1) * tok]
        return total + drift[j]

    lax.fori_loop(0, n_time, first_prefix, jnp.zeros((CHUNKS * tok, chans), jnp.float32), unroll=8)

    steps = ROWS // tok

    def block_step(q, b, carry):
        acc = None
        x = xbf[q, pl.ds(pl.multiple_of(b * ROWS, ROWS), ROWS), :]
        for n in range(hidden // TILE):
            pre = jnp.dot(x, w1_ref[:, n * TILE:(n + 1) * TILE], preferred_element_type=jnp.float32)
            parts = []
            for s in range(steps):
                j = b * steps + s
                halves = []
                for half in range(TILE // 128):
                    c = n * (TILE // 128) + half
                    p = pre[s * tok:(s + 1) * tok, half * 128:(half + 1) * 128]
                    h = p * mods[j, pl.ds(c, 1), :] + mods[j, pl.ds(n_rows + c, 1), :]
                    halves.append(half_gelu(h).astype(jnp.bfloat16))
                parts.append(jnp.concatenate(halves, axis=1))
            act = jnp.concatenate(parts, axis=0)
            prod = jnp.dot(act, w2[n * TILE:(n + 1) * TILE, :], preferred_element_type=jnp.float32)
            acc = prod if acc is None else acc + prod
        start = x0[pl.ds(pl.multiple_of(q * tok, tok), tok), :]
        total = prefix[...]
        for s in range(steps):
            j = b * steps + s
            new = start + total
            xbf[q, pl.ds(pl.multiple_of(j * tok, tok), tok), :] = new.astype(jnp.bfloat16)
            send[q, j, :, 0:chans] = new[:GROUP]
            send[q, j, :, chans:2 * chans] = new[GROUP:]
            total = total + mods[j, pl.ds(2 * n_rows, 1), :][:, :chans] * acc[s * tok:(s + 1) * tok, :]
        prefix[...] = total
        return carry

    def chunk(q, carry):
        def sweep(i, carry):
            prefix[...] = jnp.zeros_like(prefix)
            return lax.fori_loop(0, n_time // steps, functools.partial(block_step, q), carry)

        lax.fori_loop(1, SWEEPS, sweep, 0)

        def out_copy(dst):
            return pltpu.make_async_remote_copy(
                src_ref=send.at[q, dst], dst_ref=recv.at[q, me], send_sem=out_send_sem, recv_sem=out_recv_sem.at[q],
                device_id={'time': dst}, device_id_type=MESH)

        def send_out(i, carry):
            other = chip_at(chip, n_chips - 1 - i, 1)
            out_copy(2 * other + core).start()
            out_copy(2 * other + 1 - core).start()
            return carry

        lax.fori_loop(0, n_chips - 1, send_out, 0)
        out_copy(partner).start()
        recv[q, me] = send[q, me]
        return carry

    lax.fori_loop(0, CHUNKS, chunk, 0)

    half_block = mod_recv.at[pl.ds(0, n_chips)]
    wait_bytes(half_block, pair_send_sem)
    wait_bytes(mod_recv.at[pl.ds(0, n_chips - 1)], mod_send_sem)
    for q in range(CHUNKS):
        wait_bytes(recv.at[q, pl.ds(0, n_time - 1)], out_recv_sem.at[q])
        for i in range(n_time * GROUP // 128):
            rows = recv[q, i * (128 // GROUP):(i + 1) * (128 // GROUP)].reshape(128, 2 * chans).T
            at = (q * n_time * GROUP) + i * 128
            out_ref[:, at:at + 128] = rows[:chans]
            out_ref[:, tokens // 2 + at:tokens // 2 + at + 128] = rows[chans:]
    wait_bytes(recv.at[:, pl.ds(0, n_time - 1)], out_send_sem)


def solution(mesh):
    n_time = mesh.shape['time']

    def per_device(x_init, w_in, w_out, mod_scale, mod_shift, step_size):
        _, tokens, chans = x_init.shape
        hidden = w_in.shape[1]
        tok = 2 * GROUP
        f32, bf16 = jnp.float32, jnp.bfloat16
        vmem = pl.BlockSpec(memory_space=pltpu.VMEM)
        out = pl.pallas_call(
            functools.partial(kernel, n_time),
            out_shape=jax.ShapeDtypeStruct((chans, tokens), f32),
            in_specs=[pl.BlockSpec(memory_space=pltpu.HBM)] * 5 + [vmem],
            out_specs=vmem,
            scratch_shapes=[
                pltpu.VMEM((chans, hidden), bf16),
                pltpu.VMEM((chans, hidden), bf16),
                pltpu.VMEM((1, hidden), bf16),
                pltpu.VMEM((1, hidden), bf16),
                pltpu.VMEM((2 * CHUNKS, chans, 128), f32),
                pltpu.VMEM((2 * CHUNKS, 128, chans), f32),
                pltpu.VMEM((CHUNKS * tok, chans), f32),
                pltpu.VMEM((hidden, chans), bf16),
                pltpu.VMEM((32, 128), bf16),
                pltpu.VMEM((n_time, 32, 128), bf16),
                pltpu.VMEM((n_time, 32, 128), f32),
                pltpu.VMEM((CHUNKS * tok, hidden), f32),
                pltpu.VMEM((n_time, CHUNKS * tok, chans), f32),
                pltpu.VMEM((CHUNKS, n_time * tok, chans), bf16),
                pltpu.VMEM((CHUNKS, n_time, GROUP, 2 * chans), f32),
                pltpu.VMEM((CHUNKS, n_time, GROUP, 2 * chans), f32),
                pltpu.VMEM((tok, chans), f32),
                pltpu.SemaphoreType.DMA((4,)),
                pltpu.SemaphoreType.DMA((2 * CHUNKS,)),
                pltpu.SemaphoreType.DMA,
                pltpu.SemaphoreType.DMA((n_time // 2,)),
                pltpu.SemaphoreType.DMA,
                pltpu.SemaphoreType.DMA((n_time // 2,)),
                pltpu.SemaphoreType.DMA,
                pltpu.SemaphoreType.DMA((CHUNKS,)),
            ],
            compiler_params=pltpu.CompilerParams(has_side_effects=True, collective_id=0, vmem_limit_bytes=32 * 1024 * 1024),
            name='sweeps',
        )(x_init[0].T, w_in, w_out.T, mod_scale, mod_shift, step_size[None])
        return out.T.reshape(1, 1, tokens, chans)

    return jax.shard_map(per_device, mesh=mesh, in_specs=(P('data'), P(), P(), P('time'), P('time'), P('time')), out_specs=P('time', 'data'), check_vma=False)
```

```python
import functools

import jax
import jax.numpy as jnp
from jax import lax
from jax.experimental import pallas as pl
from jax.experimental.pallas import tpu as pltpu
from jax.sharding import PartitionSpec as P

SWEEPS = 4
C0 = 0.7978845608028654
C1 = C0 * 0.044715
TILE = 256
ROWS = 1024
CHUNKS = 2
GROUP = 8
SIDE = 4
ARRIVE = 8
AHEAD = 4
DEV_STRIDE = 45
MESH = pl.DeviceIdType.MESH


def half_gelu(h):
    t = jnp.tanh(h * (h * h * (8.0 * C1) + 2.0 * C0))
    return h + h * t


def wait_bytes(ref, sem):
    pltpu.make_async_copy(ref, ref, sem).wait()


NEAR = (0, 1, 3, 2)


def hop(t):
    return t + (t // 2) * (1 - 2 * lax.rem(t, 2))


def kernel(n_time, x_hbm, w1_hbm, w2t_hbm, scale_hbm, shift_hbm, step_ref, out_ref,
           w1_ref, w2t_ref, scale_ref, shift_ref, xcol, xrow, x0, w2, mod_send, mod_recv, mods, p0, drift, xbf, send, recv, prefix,
           load_sem, x_sem, mod_send_sem, mod_recv_sem, pair_send_sem, pair_recv_sem, out_send_sem, out_recv_sem):
    me = lax.axis_index('time')
    n_chips = n_time // 2
    chip = me // 2
    core = lax.rem(me, 2)
    partner = me + 1 - 2 * core
    chans, hidden = w1_ref.shape
    n_rows = hidden // 128
    tok = 2 * GROUP
    tokens = x_hbm.shape[1]

    barrier = pltpu.get_barrier_semaphore()

    def arrive(k, carry):
        pl.semaphore_signal(barrier, inc=1, device_id={'time': lax.rem(me + k * DEV_STRIDE, n_time)}, device_id_type=MESH)
        return carry

    lax.fori_loop(1, n_time, arrive, 0)

    loads = [pltpu.make_async_copy(src, dst, load_sem.at[i]) for i, (src, dst) in enumerate(
        [(scale_hbm, scale_ref), (shift_hbm, shift_ref), (w2t_hbm, w2t_ref), (w1_hbm, w1_ref)])]
    for load in loads:
        load.start()
    x_copies = []
    for i in range(2 * CHUNKS):
        start = (i % 2) * (tokens // 2) + (i // 2) * (tokens // 2 // CHUNKS) + (me * GROUP // 128) * 128
        x_copies.append(pltpu.make_async_copy(
            x_hbm.at[:, pl.ds(pl.multiple_of(start, 128), 128)], xcol.at[i], x_sem.at[i]))
        x_copies[-1].start()

    loads[0].wait()
    loads[1].wait()
    for c in range(n_rows):
        mod_send[pl.ds(c, 1), :] = scale_ref[:, c * 128:(c + 1) * 128]
        mod_send[pl.ds(n_rows + c, 1), :] = shift_ref[:, c * 128:(c + 1) * 128]
    step = jnp.broadcast_to(step_ref[...], (1, 128))
    high = step.astype(jnp.bfloat16)
    rest = step - high.astype(jnp.float32)
    mid = rest.astype(jnp.bfloat16)
    low = (rest - mid.astype(jnp.float32)).astype(jnp.bfloat16)
    mod_send[pl.ds(2 * n_rows, 1), :] = high
    mod_send[pl.ds(2 * n_rows + 1, 1), :] = mid
    mod_send[pl.ds(2 * n_rows + 2, 1), :] = low
    mod_recv[me] = mod_send[...]

    loads[2].wait()
    w2[...] = w2t_ref[...].astype(jnp.float32).T.astype(jnp.bfloat16)
    lo = pl.ds(pl.multiple_of(lax.rem(me * GROUP, 128), GROUP), GROUP)
    for i in range(2 * CHUNKS):
        x_copies[i].wait()
        xrow[i] = xcol[i].T
        x0[i * GROUP:(i + 1) * GROUP, :] = xrow[i, lo, :]
    loads[3].wait()
    x0_rounded = x0[...].astype(jnp.bfloat16)
    for n in range(hidden // TILE):
        p0[:, n * TILE:(n + 1) * TILE] = jnp.dot(
            x0_rounded, w1_ref[:, n * TILE:(n + 1) * TILE], preferred_element_type=jnp.float32)

    pl.semaphore_wait(barrier, n_time - 1)

    place_x, place_y, place_z = lax.rem(chip, SIDE), lax.rem(chip // SIDE, SIDE), chip // (SIDE * SIDE)

    def along(place, step):
        return lax.rem(place + step + SIDE, SIDE)

    def group(g, sign):
        z = along(place_z, sign * hop(g // 2)) * (SIDE * SIDE)
        chips = []
        for i in range(2):
            zy = z + along(place_y, sign * hop(2 * lax.rem(g, 2) + i)) * SIDE
            chips += [zy + along(place_x, sign * step) for step in NEAR]
        return chips

    def mod_copy(k, dst):
        return pltpu.make_async_remote_copy(
            src_ref=mod_send, dst_ref=mod_recv.at[me], send_sem=mod_send_sem, recv_sem=mod_recv_sem.at[k],
            device_id={'time': dst}, device_id_type=MESH)

    def pair_copy(k, src, src_ref):
        return pltpu.make_async_remote_copy(
            src_ref=src_ref, dst_ref=mod_recv.at[src], send_sem=pair_send_sem, recv_sem=pair_recv_sem.at[k],
            device_id={'time': partner}, device_id_type=MESH)

    def send_group(g, first=0):
        for i, other in enumerate(group(g, 1)[first:], first):
            mod_copy(g * ARRIVE + i, 2 * other + core).start()

    def relay_group(g, first=0):
        for i, other in enumerate(group(g, -1)[first:], first):
            mod_copy(g * ARRIVE + i, me).wait_recv()
            src = 2 * other + core
            pair_copy(g * ARRIVE + i, src, mod_recv.at[src]).start()

    def pair_wait(g):
        for i in range(ARRIVE):
            pair_copy(g * ARRIVE + i, me, mod_send).wait_recv()

    def unpack(g):
        for other in group(g, -1):
            for j in (2 * other, 2 * other + 1):
                block = mod_recv[j].astype(jnp.float32)
                mods[j, pl.ds(0, n_rows), :] = 0.5 * (1.0 + block[:n_rows])
                mods[j, pl.ds(n_rows, n_rows), :] = 0.5 * block[n_rows:2 * n_rows]
                mods[j, pl.ds(2 * n_rows, 1), :] = (block[2 * n_rows:2 * n_rows + 1] + block[2 * n_rows + 1:2 * n_rows + 2]) + block[2 * n_rows + 2:2 * n_rows + 3]

    n_groups = n_chips // ARRIVE
    pair_copy(0, me, mod_send).start()
    send_group(0, 1)
    for g in range(1, AHEAD):
        send_group(g)
    relay_group(0, 1)
    relay_group(1)
    pair_wait(0)
    unpack(0)

    def first_sweep(g, carry):
        pl.when(g + AHEAD < n_groups)(lambda: send_group(g + AHEAD))
        pl.when(g + 2 < n_groups)(lambda: relay_group(g + 2))
        pl.when(g + 1 < n_groups)(lambda: pair_wait(g + 1))
        steps = [2 * other + c for other in group(g, -1) for c in range(2)]
        acc = None
        for n in range(hidden // TILE):
            parts = []
            for j in steps:
                halves = []
                for c in range(n * (TILE // 128), (n + 1) * (TILE // 128)):
                    h = p0[:, c * 128:(c + 1) * 128] * mods[j, pl.ds(c, 1), :] + mods[j, pl.ds(n_rows + c, 1), :]
                    halves.append(half_gelu(h).astype(jnp.bfloat16))
                parts.append(jnp.concatenate(halves, axis=1))
            act = jnp.concatenate(parts, axis=0)
            prod = jnp.dot(act, w2[n * TILE:(n + 1) * TILE, :], preferred_element_type=jnp.float32)
            acc = prod if acc is None else acc + prod
        for i, j in enumerate(steps):
            drift[j] = mods[j, pl.ds(2 * n_rows, 1), :][:, :chans] * acc[i * CHUNKS * tok:(i + 1) * CHUNKS * tok, :]
        unpack(lax.rem(g + 1, n_groups))
        return carry

    lax.fori_loop(0, n_groups, first_sweep, 0)

    def first_prefix(j, total):
        new = (x0[...] + total).astype(jnp.bfloat16)
        for q in range(CHUNKS):
            xbf[q, pl.ds(pl.multiple_of(j * tok, tok), tok), :] = new[q * tok:(q + 1) * tok]
        return total + drift[j]

    lax.fori_loop(0, n_time, first_prefix, jnp.zeros((CHUNKS * tok, chans), jnp.float32), unroll=8)

    steps = ROWS // tok

    def block_step(q, b, carry):
        acc = None
        x = xbf[q, pl.ds(pl.multiple_of(b * ROWS, ROWS), ROWS), :]
        for n in range(hidden // TILE):
            pre = jnp.dot(x, w1_ref[:, n * TILE:(n + 1) * TILE], preferred_element_type=jnp.float32)
            parts = []
            for s in range(steps):
                j = b * steps + s
                halves = []
                for half in range(TILE // 128):
                    c = n * (TILE // 128) + half
                    p = pre[s * tok:(s + 1) * tok, half * 128:(half + 1) * 128]
                    h = p * mods[j, pl.ds(c, 1), :] + mods[j, pl.ds(n_rows + c, 1), :]
                    halves.append(half_gelu(h).astype(jnp.bfloat16))
                parts.append(jnp.concatenate(halves, axis=1))
            act = jnp.concatenate(parts, axis=0)
            prod = jnp.dot(act, w2[n * TILE:(n + 1) * TILE, :], preferred_element_type=jnp.float32)
            acc = prod if acc is None else acc + prod
        start = x0[pl.ds(pl.multiple_of(q * tok, tok), tok), :]
        total = prefix[...]
        for s in range(steps):
            j = b * steps + s
            new = start + total
            xbf[q, pl.ds(pl.multiple_of(j * tok, tok), tok), :] = new.astype(jnp.bfloat16)
            send[q, j, :, 0:chans] = new[:GROUP]
            send[q, j, :, chans:2 * chans] = new[GROUP:]
            total = total + mods[j, pl.ds(2 * n_rows, 1), :][:, :chans] * acc[s * tok:(s + 1) * tok, :]
        prefix[...] = total
        return carry

    def chunk(q, carry):
        def sweep(i, carry):
            prefix[...] = jnp.zeros_like(prefix)
            return lax.fori_loop(0, n_time // steps, functools.partial(block_step, q), carry)

        lax.fori_loop(1, SWEEPS, sweep, 0)

        def out_copy(dst):
            return pltpu.make_async_remote_copy(
                src_ref=send.at[q, dst], dst_ref=recv.at[q, me], send_sem=out_send_sem, recv_sem=out_recv_sem.at[q],
                device_id={'time': dst}, device_id_type=MESH)

        for k in range(n_chips - 1, 0, -1):
            other = (along(place_z, NEAR[k // (SIDE * SIDE)]) * SIDE + along(place_y, NEAR[k // SIDE % SIDE])) * SIDE + along(place_x, NEAR[k % SIDE])
            out_copy(2 * other + core).start()
            out_copy(2 * other + 1 - core).start()
        out_copy(partner).start()
        recv[q, me] = send[q, me]
        return carry

    lax.fori_loop(0, CHUNKS, chunk, 0)

    half_block = mod_recv.at[pl.ds(0, n_chips)]
    wait_bytes(half_block, pair_send_sem)
    wait_bytes(mod_recv.at[pl.ds(0, n_chips - 1)], mod_send_sem)
    for q in range(CHUNKS):
        wait_bytes(recv.at[q, pl.ds(0, n_time - 1)], out_recv_sem.at[q])
        for i in range(n_time * GROUP // 128):
            rows = recv[q, i * (128 // GROUP):(i + 1) * (128 // GROUP)].reshape(128, 2 * chans).T
            at = (q * n_time * GROUP) + i * 128
            out_ref[:, at:at + 128] = rows[:chans]
            out_ref[:, tokens // 2 + at:tokens // 2 + at + 128] = rows[chans:]
    wait_bytes(recv.at[:, pl.ds(0, n_time - 1)], out_send_sem)


def solution(mesh):
    n_time = mesh.shape['time']

    def per_device(x_init, w_in, w_out, mod_scale, mod_shift, step_size):
        _, tokens, chans = x_init.shape
        hidden = w_in.shape[1]
        tok = 2 * GROUP
        f32, bf16 = jnp.float32, jnp.bfloat16
        vmem = pl.BlockSpec(memory_space=pltpu.VMEM)
        out = pl.pallas_call(
            functools.partial(kernel, n_time),
            out_shape=jax.ShapeDtypeStruct((chans, tokens), f32),
            in_specs=[pl.BlockSpec(memory_space=pltpu.HBM)] * 5 + [vmem],
            out_specs=vmem,
            scratch_shapes=[
                pltpu.VMEM((chans, hidden), bf16),
                pltpu.VMEM((chans, hidden), bf16),
                pltpu.VMEM((1, hidden), bf16),
                pltpu.VMEM((1, hidden), bf16),
                pltpu.VMEM((2 * CHUNKS, chans, 128), f32),
                pltpu.VMEM((2 * CHUNKS, 128, chans), f32),
                pltpu.VMEM((CHUNKS * tok, chans), f32),
                pltpu.VMEM((hidden, chans), bf16),
                pltpu.VMEM((32, 128), bf16),
                pltpu.VMEM((n_time, 32, 128), bf16),
                pltpu.VMEM((n_time, 32, 128), f32),
                pltpu.VMEM((CHUNKS * tok, hidden), f32),
                pltpu.VMEM((n_time, CHUNKS * tok, chans), f32),
                pltpu.VMEM((CHUNKS, n_time * tok, chans), bf16),
                pltpu.VMEM((CHUNKS, n_time, GROUP, 2 * chans), f32),
                pltpu.VMEM((CHUNKS, n_time, GROUP, 2 * chans), f32),
                pltpu.VMEM((tok, chans), f32),
                pltpu.SemaphoreType.DMA((4,)),
                pltpu.SemaphoreType.DMA((2 * CHUNKS,)),
                pltpu.SemaphoreType.DMA,
                pltpu.SemaphoreType.DMA((n_time // 2,)),
                pltpu.SemaphoreType.DMA,
                pltpu.SemaphoreType.DMA((n_time // 2,)),
                pltpu.SemaphoreType.DMA,
                pltpu.SemaphoreType.DMA((CHUNKS,)),
            ],
            compiler_params=pltpu.CompilerParams(has_side_effects=True, collective_id=0),
            name='sweeps',
        )(x_init[0].T, w_in, w_out.T, mod_scale, mod_shift, step_size[None])
        return out.T.reshape(1, 1, tokens, chans)

    return jax.shard_map(per_device, mesh=mesh, in_specs=(P('data'), P(), P(), P('time'), P('time'), P('time')), out_specs=P('time', 'data'), check_vma=False)
```

```python
import functools

import jax
import jax.numpy as jnp
from jax import lax
from jax.experimental import pallas as pl
from jax.experimental.pallas import tpu as pltpu
from jax.sharding import PartitionSpec as P

SWEEPS = 4
C0 = 0.7978845608028654
C1 = C0 * 0.044715
TILE = 256
ROWS = 1024
CHUNKS = 2
GROUP = 8
SPREAD = 4
SIDE = 4
ARRIVE = 8
DEV_STRIDE = 45
MESH = pl.DeviceIdType.MESH


def half_gelu(h):
    t = jnp.tanh(h * (h * h * (8.0 * C1) + 2.0 * C0))
    return h + h * t


def wait_bytes(ref, sem):
    pltpu.make_async_copy(ref, ref, sem).wait()


NEAR = (0, 1, 3, 2)


def hop(t):
    return t + (t // 2) * (1 - 2 * lax.rem(t, 2))


def kernel(n_time, x_hbm, w1_hbm, w2t_hbm, scale_hbm, shift_hbm, step_ref, out_ref,
           w1_ref, w2t_ref, scale_ref, shift_ref, xcol, xrow, x0, w2, mod_send, mod_recv, mods, p0, drift, xbf, send, prefix,
           load_sem, x_sem, mod_send_sem, mod_recv_sem, pair_send_sem, pair_recv_sem, out_send_sem, out_recv_sem, own_sem):
    me = lax.axis_index('time')
    n_chips = n_time // 2
    chip = me // 2
    core = lax.rem(me, 2)
    partner = me + 1 - 2 * core
    chans, hidden = w1_ref.shape
    n_rows = hidden // 128
    tok = 2 * GROUP
    tokens = x_hbm.shape[1]

    barrier = pltpu.get_barrier_semaphore()

    def arrive(k, carry):
        pl.semaphore_signal(barrier, inc=1, device_id={'time': lax.rem(me + k * DEV_STRIDE, n_time)}, device_id_type=MESH)
        return carry

    lax.fori_loop(1, n_time, arrive, 0)

    loads = [pltpu.make_async_copy(src, dst, load_sem.at[i]) for i, (src, dst) in enumerate(
        [(scale_hbm, scale_ref), (shift_hbm, shift_ref), (w2t_hbm, w2t_ref), (w1_hbm, w1_ref)])]
    for load in loads:
        load.start()
    x_copies = []
    for i in range(2 * CHUNKS):
        start = (i % 2) * (tokens // 2) + (i // 2) * (tokens // 2 // CHUNKS) + (me * GROUP // 128) * 128
        x_copies.append(pltpu.make_async_copy(
            x_hbm.at[:, pl.ds(pl.multiple_of(start, 128), 128)], xcol.at[i], x_sem.at[i]))
        x_copies[-1].start()

    loads[0].wait()
    loads[1].wait()
    for c in range(n_rows):
        mod_send[pl.ds(c, 1), :] = scale_ref[:, c * 128:(c + 1) * 128]
        mod_send[pl.ds(n_rows + c, 1), :] = shift_ref[:, c * 128:(c + 1) * 128]
    step = jnp.broadcast_to(step_ref[...], (1, 128))
    high = step.astype(jnp.bfloat16)
    rest = step - high.astype(jnp.float32)
    mid = rest.astype(jnp.bfloat16)
    low = (rest - mid.astype(jnp.float32)).astype(jnp.bfloat16)
    mod_send[pl.ds(2 * n_rows, 1), :] = high
    mod_send[pl.ds(2 * n_rows + 1, 1), :] = mid
    mod_send[pl.ds(2 * n_rows + 2, 1), :] = low
    mod_recv[me] = mod_send[...]

    loads[2].wait()
    w2[...] = w2t_ref[...].astype(jnp.float32).T.astype(jnp.bfloat16)
    lo = pl.ds(pl.multiple_of(lax.rem(me * GROUP, 128), GROUP), GROUP)
    for i in range(2 * CHUNKS):
        x_copies[i].wait()
        xrow[i] = xcol[i].T
        x0[i * GROUP:(i + 1) * GROUP, :] = xrow[i, lo, :]
    loads[3].wait()
    x0_rounded = x0[...].astype(jnp.bfloat16)
    for n in range(hidden // TILE):
        p0[:, n * TILE:(n + 1) * TILE] = jnp.dot(
            x0_rounded, w1_ref[:, n * TILE:(n + 1) * TILE], preferred_element_type=jnp.float32)

    pl.semaphore_wait(barrier, n_time - 1)

    place_x, place_y, place_z = lax.rem(chip, SIDE), lax.rem(chip // SIDE, SIDE), chip // (SIDE * SIDE)

    def along(place, step):
        return lax.rem(place + step + SIDE, SIDE)

    def group(g, sign):
        z = along(place_z, sign * hop(g // 2)) * (SIDE * SIDE)
        chips = []
        for i in range(2):
            zy = z + along(place_y, sign * hop(2 * lax.rem(g, 2) + i)) * SIDE
            chips += [zy + along(place_x, sign * step) for step in NEAR]
        return chips

    def mod_copy(k, dst):
        return pltpu.make_async_remote_copy(
            src_ref=mod_send, dst_ref=mod_recv.at[me], send_sem=mod_send_sem, recv_sem=mod_recv_sem.at[k],
            device_id={'time': dst}, device_id_type=MESH)

    def pair_copy(k, src, src_ref):
        return pltpu.make_async_remote_copy(
            src_ref=src_ref, dst_ref=mod_recv.at[src], send_sem=pair_send_sem, recv_sem=pair_recv_sem.at[k],
            device_id={'time': partner}, device_id_type=MESH)

    def send_group(g, first=0):
        for i, other in enumerate(group(g, 1)[first:], first):
            mod_copy(g * ARRIVE + i, 2 * other + core).start()

    def relay_group(g, first=0):
        for i, other in enumerate(group(g, -1)[first:], first):
            mod_copy(g * ARRIVE + i, me).wait_recv()
            src = 2 * other + core
            pair_copy(g * ARRIVE + i, src, mod_recv.at[src]).start()

    def pair_wait(g):
        for i in range(ARRIVE):
            pair_copy(g * ARRIVE + i, me, mod_send).wait_recv()

    def unpack(g):
        for other in group(g, -1):
            for j in (2 * other, 2 * other + 1):
                block = mod_recv[j].astype(jnp.float32)
                mods[j, pl.ds(0, n_rows), :] = 0.5 * (1.0 + block[:n_rows])
                mods[j, pl.ds(n_rows, n_rows), :] = 0.5 * block[n_rows:2 * n_rows]
                mods[j, pl.ds(2 * n_rows, 1), :] = (block[2 * n_rows:2 * n_rows + 1] + block[2 * n_rows + 1:2 * n_rows + 2]) + block[2 * n_rows + 2:2 * n_rows + 3]

    n_groups = n_chips // ARRIVE
    pair_copy(0, me, mod_send).start()
    send_group(0, 1)
    for g in range(1, n_groups):
        send_group(g)
    relay_group(0, 1)
    relay_group(1)
    pair_wait(0)
    unpack(0)

    def first_sweep(g, carry):
        pl.when(g + 2 < n_groups)(lambda: relay_group(g + 2))
        pl.when(g + 1 < n_groups)(lambda: pair_wait(g + 1))
        steps = [2 * other + c for other in group(g, -1) for c in range(2)]
        acc = None
        for n in range(hidden // TILE):
            parts = []
            for j in steps:
                halves = []
                for c in range(n * (TILE // 128), (n + 1) * (TILE // 128)):
                    h = p0[:, c * 128:(c + 1) * 128] * mods[j, pl.ds(c, 1), :] + mods[j, pl.ds(n_rows + c, 1), :]
                    halves.append(half_gelu(h).astype(jnp.bfloat16))
                parts.append(jnp.concatenate(halves, axis=1))
            act = jnp.concatenate(parts, axis=0)
            prod = jnp.dot(act, w2[n * TILE:(n + 1) * TILE, :], preferred_element_type=jnp.float32)
            acc = prod if acc is None else acc + prod
        for i, j in enumerate(steps):
            drift[j] = mods[j, pl.ds(2 * n_rows, 1), :][:, :chans] * acc[i * CHUNKS * tok:(i + 1) * CHUNKS * tok, :]
        unpack(lax.rem(g + 1, n_groups))
        return carry

    lax.fori_loop(0, n_groups, first_sweep, 0)

    def first_prefix(j, total):
        new = (x0[...] + total).astype(jnp.bfloat16)
        for q in range(CHUNKS):
            xbf[q, pl.ds(pl.multiple_of(j * tok, tok), tok), :] = new[q * tok:(q + 1) * tok]
        return total + drift[j]

    lax.fori_loop(0, n_time, first_prefix, jnp.zeros((CHUNKS * tok, chans), jnp.float32), unroll=8)

    steps = ROWS // tok

    def block_step(q, b, carry):
        acc = None
        x = xbf[q, pl.ds(pl.multiple_of(b * ROWS, ROWS), ROWS), :]
        for n in range(hidden // TILE):
            pre = jnp.dot(x, w1_ref[:, n * TILE:(n + 1) * TILE], preferred_element_type=jnp.float32)
            parts = []
            for s in range(steps):
                j = b * steps + s
                halves = []
                for half in range(TILE // 128):
                    c = n * (TILE // 128) + half
                    p = pre[s * tok:(s + 1) * tok, half * 128:(half + 1) * 128]
                    h = p * mods[j, pl.ds(c, 1), :] + mods[j, pl.ds(n_rows + c, 1), :]
                    halves.append(half_gelu(h).astype(jnp.bfloat16))
                parts.append(jnp.concatenate(halves, axis=1))
            act = jnp.concatenate(parts, axis=0)
            prod = jnp.dot(act, w2[n * TILE:(n + 1) * TILE, :], preferred_element_type=jnp.float32)
            acc = prod if acc is None else acc + prod
        start = x0[pl.ds(pl.multiple_of(q * tok, tok), tok), :]
        total = prefix[...]
        for s in range(steps):
            j = b * steps + s
            new = start + total
            xbf[q, pl.ds(pl.multiple_of(j * tok, tok), tok), :] = new.astype(jnp.bfloat16)
            send[q, j, :, 0:chans] = new[:GROUP]
            send[q, j, :, chans:2 * chans] = new[GROUP:]
            total = total + mods[j, pl.ds(2 * n_rows, 1), :][:, :chans] * acc[s * tok:(s + 1) * tok, :]
        prefix[...] = total
        return carry

    def own_copy(q):
        return pltpu.make_async_copy(send.at[q, me], out_ref.at[q, me], own_sem.at[q])

    def chunk(q, carry):
        def sweep(i, carry):
            prefix[...] = jnp.zeros_like(prefix)
            return lax.fori_loop(0, n_time // steps, functools.partial(block_step, q), carry)

        lax.fori_loop(1, SWEEPS, sweep, 0)

        def out_copy(dst):
            return pltpu.make_async_remote_copy(
                src_ref=send.at[q, dst], dst_ref=out_ref.at[q, me], send_sem=out_send_sem, recv_sem=out_recv_sem.at[q],
                device_id={'time': dst}, device_id_type=MESH)

        for k in range(n_chips - 1, 0, -1):
            other = (along(place_z, NEAR[k // (SIDE * SIDE)]) * SIDE + along(place_y, NEAR[k // SIDE % SIDE])) * SIDE + along(place_x, NEAR[k % SIDE])
            out_copy(2 * other + core).start()
            out_copy(2 * other + 1 - core).start()
        out_copy(partner).start()
        own_copy(q).start()
        return carry

    lax.fori_loop(0, CHUNKS, chunk, 0)

    half_block = mod_recv.at[pl.ds(0, n_chips)]
    wait_bytes(half_block, pair_send_sem)
    wait_bytes(mod_recv.at[pl.ds(0, n_chips - 1)], mod_send_sem)
    for q in range(CHUNKS):
        own_copy(q).wait()
        wait_bytes(out_ref.at[q, pl.ds(0, n_time - 1)], out_recv_sem.at[q])
    wait_bytes(send.at[:, pl.ds(0, n_time - 1)], out_send_sem)


def spread(rows_hbm, out_hbm, rows, cols, in_sem, out_sem):
    chans, tokens = out_hbm.shape
    part = rows_hbm.shape[0] // SPREAD
    loads = [pltpu.make_async_copy(rows_hbm.at[pl.ds(i * part, part)], rows.at[pl.ds(i * part, part)], in_sem.at[i])
             for i in range(SPREAD)]
    for load in loads:
        load.start()
    stores = []
    for i in range(SPREAD):
        loads[i].wait()
        for at in range(i * part, (i + 1) * part, 128):
            block = rows[at:at + 128, :].T
            cols[:, at:at + 128] = block[:chans]
            cols[:, tokens // 2 + at:tokens // 2 + at + 128] = block[chans:]
        for half in range(2):
            at = pl.ds(half * (tokens // 2) + i * part, part)
            stores.append(pltpu.make_async_copy(cols.at[:, at], out_hbm.at[:, at], out_sem.at[2 * i + half]))
            stores[-1].start()
    for store in stores:
        store.wait()


def solution(mesh):
    n_time = mesh.shape['time']

    def per_device(x_init, w_in, w_out, mod_scale, mod_shift, step_size):
        _, tokens, chans = x_init.shape
        hidden = w_in.shape[1]
        tok = 2 * GROUP
        f32, bf16 = jnp.float32, jnp.bfloat16
        vmem, hbm = pl.BlockSpec(memory_space=pltpu.VMEM), pl.BlockSpec(memory_space=pltpu.HBM)
        out = pl.pallas_call(
            functools.partial(kernel, n_time),
            out_shape=jax.ShapeDtypeStruct((CHUNKS, n_time, GROUP, 2 * chans), f32),
            in_specs=[hbm] * 5 + [vmem],
            out_specs=hbm,
            scratch_shapes=[
                pltpu.VMEM((chans, hidden), bf16),
                pltpu.VMEM((chans, hidden), bf16),
                pltpu.VMEM((1, hidden), bf16),
                pltpu.VMEM((1, hidden), bf16),
                pltpu.VMEM((2 * CHUNKS, chans, 128), f32),
                pltpu.VMEM((2 * CHUNKS, 128, chans), f32),
                pltpu.VMEM((CHUNKS * tok, chans), f32),
                pltpu.VMEM((hidden, chans), bf16),
                pltpu.VMEM((32, 128), bf16),
                pltpu.VMEM((n_time, 32, 128), bf16),
                pltpu.VMEM((n_time, 32, 128), f32),
                pltpu.VMEM((CHUNKS * tok, hidden), f32),
                pltpu.VMEM((n_time, CHUNKS * tok, chans), f32),
                pltpu.VMEM((CHUNKS, n_time * tok, chans), bf16),
                pltpu.VMEM((CHUNKS, n_time, GROUP, 2 * chans), f32),
                pltpu.VMEM((tok, chans), f32),
                pltpu.SemaphoreType.DMA((4,)),
                pltpu.SemaphoreType.DMA((2 * CHUNKS,)),
                pltpu.SemaphoreType.DMA,
                pltpu.SemaphoreType.DMA((n_time // 2,)),
                pltpu.SemaphoreType.DMA,
                pltpu.SemaphoreType.DMA((n_time // 2,)),
                pltpu.SemaphoreType.DMA,
                pltpu.SemaphoreType.DMA((CHUNKS,)),
                pltpu.SemaphoreType.DMA((CHUNKS,)),
            ],
            compiler_params=pltpu.CompilerParams(has_side_effects=True, collective_id=0),
            name='sweeps',
        )(x_init[0].T, w_in, w_out.T, mod_scale, mod_shift, step_size[None])
        out = pl.pallas_call(
            spread, out_shape=jax.ShapeDtypeStruct((chans, tokens), f32), in_specs=[hbm], out_specs=hbm,
            scratch_shapes=[
                pltpu.VMEM((tokens // 2, 2 * chans), f32),
                pltpu.VMEM((chans, tokens), f32),
                pltpu.SemaphoreType.DMA((SPREAD,)),
                pltpu.SemaphoreType.DMA((2 * SPREAD,)),
            ],
            name='spread',
        )(out.reshape(tokens // 2, 2 * chans))
        return out.T.reshape(1, 1, tokens, chans)

    return jax.shard_map(per_device, mesh=mesh, in_specs=(P('data'), P(), P(), P('time'), P('time'), P('time')), out_specs=P('time', 'data'), check_vma=False)
```

```python
import functools

import jax
import jax.numpy as jnp
from jax import lax
from jax.experimental import pallas as pl
from jax.experimental.pallas import tpu as pltpu
from jax.sharding import PartitionSpec as P

SWEEPS = 4
C0 = 0.7978845608028654
C1 = C0 * 0.044715
TILE = 256
ROWS = 1024
CHUNKS = 2
GROUP = 8
SPREAD = 4
SIDE = 4
ARRIVE = 8
MESH = pl.DeviceIdType.MESH


def half_gelu(h):
    t = jnp.tanh(h * (h * h * (8.0 * C1) + 2.0 * C0))
    return h + h * t


def wait_bytes(ref, sem):
    pltpu.make_async_copy(ref, ref, sem).wait()


NEAR = (0, 1, 3, 2)


def hop(t):
    return t + (t // 2) * (1 - 2 * lax.rem(t, 2))


def kernel(n_time, x_hbm, w1_hbm, w2t_hbm, scale_hbm, shift_hbm, step_ref, out_ref,
           w1_ref, w2t_ref, scale_ref, shift_ref, xcol, xrow, x0, w2, mod_send, mod_recv, mods, p0, drift, xbf, send, prefix,
           load_sem, x_sem, mod_send_sem, mod_recv_sem, pair_send_sem, pair_recv_sem, out_send_sem, out_recv_sem, own_sem):
    me = lax.axis_index('time')
    n_chips = n_time // 2
    chip = me // 2
    core = lax.rem(me, 2)
    partner = me + 1 - 2 * core
    chans, hidden = w1_ref.shape
    n_rows = hidden // TILE
    tok = 2 * GROUP
    tokens = x_hbm.shape[1]

    barrier = pltpu.get_barrier_semaphore()

    place_x, place_y, place_z = lax.rem(chip, SIDE), lax.rem(chip // SIDE, SIDE), chip // (SIDE * SIDE)

    def along(place, step):
        return lax.rem(place + step + SIDE, SIDE)

    xs = [along(place_x, step) for step in NEAR]
    ys = [along(place_y, step) * SIDE for step in NEAR]
    zs = [along(place_z, step) * (SIDE * SIDE) for step in NEAR]

    def other_chips():
        for k in range(n_chips - 1, 0, -1):
            yield zs[k // (SIDE * SIDE)] + ys[k // SIDE % SIDE] + xs[k % SIDE]

    def arrive(dst):
        pl.semaphore_signal(barrier, inc=1, device_id={'time': dst}, device_id_type=MESH)

    for other in other_chips():
        arrive(2 * other)
        arrive(2 * other + 1)
    arrive(partner)

    loads = [pltpu.make_async_copy(src, dst, load_sem.at[i]) for i, (src, dst) in enumerate(
        [(scale_hbm, scale_ref), (shift_hbm, shift_ref), (w2t_hbm, w2t_ref), (w1_hbm, w1_ref)])]
    for load in loads:
        load.start()
    x_copies = []
    for i in range(2 * CHUNKS):
        start = (i % 2) * (tokens // 2) + (i // 2) * (tokens // 2 // CHUNKS) + (me * GROUP // 128) * 128
        x_copies.append(pltpu.make_async_copy(
            x_hbm.at[:, pl.ds(pl.multiple_of(start, 128), 128)], xcol.at[i], x_sem.at[i]))
        x_copies[-1].start()

    loads[0].wait()
    loads[1].wait()
    for n in range(n_rows):
        mod_send[pl.ds(n, 1), :] = scale_ref[:, n * TILE:(n + 1) * TILE]
        mod_send[pl.ds(n_rows + n, 1), :] = shift_ref[:, n * TILE:(n + 1) * TILE]
    step = jnp.broadcast_to(step_ref[...], (1, TILE))
    high = step.astype(jnp.bfloat16)
    rest = step - high.astype(jnp.float32)
    mid = rest.astype(jnp.bfloat16)
    low = (rest - mid.astype(jnp.float32)).astype(jnp.bfloat16)
    mod_send[pl.ds(2 * n_rows, 1), :] = high
    mod_send[pl.ds(2 * n_rows + 1, 1), :] = mid
    mod_send[pl.ds(2 * n_rows + 2, 1), :] = low
    mod_recv[me] = mod_send[...]

    loads[2].wait()
    w2[...] = w2t_ref[...].astype(jnp.float32).T.astype(jnp.bfloat16)
    lo = pl.ds(pl.multiple_of(lax.rem(me * GROUP, 128), GROUP), GROUP)
    for i in range(2 * CHUNKS):
        x_copies[i].wait()
        xrow[i] = xcol[i].T
        x0[i * GROUP:(i + 1) * GROUP, :] = xrow[i, lo, :]
    loads[3].wait()
    x0_rounded = x0[...].astype(jnp.bfloat16)
    for n in range(hidden // TILE):
        p0[:, n * TILE:(n + 1) * TILE] = jnp.dot(
            x0_rounded, w1_ref[:, n * TILE:(n + 1) * TILE], preferred_element_type=jnp.float32)

    pl.semaphore_wait(barrier, n_time - 1)

    def group(g, sign):
        z = along(place_z, sign * hop(g // 2)) * (SIDE * SIDE)
        chips = []
        for i in range(2):
            zy = z + along(place_y, sign * hop(2 * lax.rem(g, 2) + i)) * SIDE
            chips += [zy + along(place_x, sign * step) for step in NEAR]
        return chips

    def mod_copy(k, dst):
        return pltpu.make_async_remote_copy(
            src_ref=mod_send, dst_ref=mod_recv.at[me], send_sem=mod_send_sem, recv_sem=mod_recv_sem.at[k],
            device_id={'time': dst}, device_id_type=MESH)

    def pair_copy(k, src, src_ref):
        return pltpu.make_async_remote_copy(
            src_ref=src_ref, dst_ref=mod_recv.at[src], send_sem=pair_send_sem, recv_sem=pair_recv_sem.at[k],
            device_id={'time': partner}, device_id_type=MESH)

    def send_group(g, first=0):
        for i, other in enumerate(group(g, 1)[first:], first):
            mod_copy(g * ARRIVE + i, 2 * other + core).start()

    def relay_group(g, first=0):
        for i, other in enumerate(group(g, -1)[first:], first):
            mod_copy(g * ARRIVE + i, me).wait_recv()
            src = 2 * other + core
            pair_copy(g * ARRIVE + i, src, mod_recv.at[src]).start()

    def pair_wait(g):
        for i in range(ARRIVE):
            pair_copy(g * ARRIVE + i, me, mod_send).wait_recv()

    def unpack(g):
        for other in group(g, -1):
            for j in (2 * other, 2 * other + 1):
                block = mod_recv[j].astype(jnp.float32)
                mods[j, pl.ds(0, n_rows), :] = 0.5 * (1.0 + block[:n_rows])
                mods[j, pl.ds(n_rows, n_rows), :] = 0.5 * block[n_rows:2 * n_rows]
                mods[j, pl.ds(2 * n_rows, 1), :] = (block[2 * n_rows:2 * n_rows + 1] + block[2 * n_rows + 1:2 * n_rows + 2]) + block[2 * n_rows + 2:2 * n_rows + 3]

    n_groups = n_chips // ARRIVE
    pair_copy(0, me, mod_send).start()
    send_group(0, 1)
    for g in range(1, n_groups):
        send_group(g)
    relay_group(0, 1)
    relay_group(1)
    pair_wait(0)
    unpack(0)

    def first_sweep(g, carry):
        pl.when(g + 2 < n_groups)(lambda: relay_group(g + 2))
        pl.when(g + 1 < n_groups)(lambda: pair_wait(g + 1))
        steps = [2 * other + c for other in group(g, -1) for c in range(2)]
        acc = None
        for n in range(hidden // TILE):
            parts = []
            for j in steps:
                h = p0[:, n * TILE:(n + 1) * TILE] * mods[j, pl.ds(n, 1), :] + mods[j, pl.ds(n_rows + n, 1), :]
                parts.append(half_gelu(h).astype(jnp.bfloat16))
            act = jnp.concatenate(parts, axis=0)
            prod = jnp.dot(act, w2[n * TILE:(n + 1) * TILE, :], preferred_element_type=jnp.float32)
            acc = prod if acc is None else acc + prod
        for i, j in enumerate(steps):
            drift[j] = mods[j, pl.ds(2 * n_rows, 1), :][:, :chans] * acc[i * CHUNKS * tok:(i + 1) * CHUNKS * tok, :]
        unpack(lax.rem(g + 1, n_groups))
        return carry

    lax.fori_loop(0, n_groups, first_sweep, 0)

    def first_prefix(j, total):
        new = (x0[...] + total).astype(jnp.bfloat16)
        for q in range(CHUNKS):
            xbf[q, pl.ds(pl.multiple_of(j * tok, tok), tok), :] = new[q * tok:(q + 1) * tok]
        return total + drift[j]

    lax.fori_loop(0, n_time, first_prefix, jnp.zeros((CHUNKS * tok, chans), jnp.float32), unroll=8)

    steps = ROWS // tok

    def block_step(q, b, carry):
        acc = None
        x = xbf[q, pl.ds(pl.multiple_of(b * ROWS, ROWS), ROWS), :]
        for n in range(hidden // TILE):
            pre = jnp.dot(x, w1_ref[:, n * TILE:(n + 1) * TILE], preferred_element_type=jnp.float32)
            parts = []
            for s in range(steps):
                j = b * steps + s
                h = pre[s * tok:(s + 1) * tok] * mods[j, pl.ds(n, 1), :] + mods[j, pl.ds(n_rows + n, 1), :]
                parts.append(half_gelu(h).astype(jnp.bfloat16))
            act = jnp.concatenate(parts, axis=0)
            prod = jnp.dot(act, w2[n * TILE:(n + 1) * TILE, :], preferred_element_type=jnp.float32)
            acc = prod if acc is None else acc + prod
        start = x0[pl.ds(pl.multiple_of(q * tok, tok), tok), :]
        total = prefix[...]
        for s in range(steps):
            j = b * steps + s
            new = start + total
            xbf[q, pl.ds(pl.multiple_of(j * tok, tok), tok), :] = new.astype(jnp.bfloat16)
            send[q, j, :, 0:chans] = new[:GROUP]
            send[q, j, :, chans:2 * chans] = new[GROUP:]
            total = total + mods[j, pl.ds(2 * n_rows, 1), :][:, :chans] * acc[s * tok:(s + 1) * tok, :]
        prefix[...] = total
        return carry

    def own_copy(q):
        return pltpu.make_async_copy(send.at[q, me], out_ref.at[q, me], own_sem.at[q])

    def chunk(q, carry):
        def sweep(i, carry):
            prefix[...] = jnp.zeros_like(prefix)
            return lax.fori_loop(0, n_time // steps, functools.partial(block_step, q), carry)

        lax.fori_loop(1, SWEEPS, sweep, 0)

        def out_copy(dst):
            return pltpu.make_async_remote_copy(
                src_ref=send.at[q, dst], dst_ref=out_ref.at[q, me], send_sem=out_send_sem, recv_sem=out_recv_sem.at[q],
                device_id={'time': dst}, device_id_type=MESH)

        for other in other_chips():
            out_copy(2 * other + core).start()
            out_copy(2 * other + 1 - core).start()
        out_copy(partner).start()
        own_copy(q).start()
        return carry

    lax.fori_loop(0, CHUNKS, chunk, 0)

    half_block = mod_recv.at[pl.ds(0, n_chips)]
    wait_bytes(half_block, pair_send_sem)
    wait_bytes(mod_recv.at[pl.ds(0, n_chips - 1)], mod_send_sem)
    for q in range(CHUNKS):
        own_copy(q).wait()
        wait_bytes(out_ref.at[q, pl.ds(0, n_time - 1)], out_recv_sem.at[q])
    wait_bytes(send.at[:, pl.ds(0, n_time - 1)], out_send_sem)


def spread(rows_hbm, out_hbm, rows, cols, in_sem, out_sem):
    chans, tokens = out_hbm.shape
    part = rows_hbm.shape[0] // SPREAD
    loads = [pltpu.make_async_copy(rows_hbm.at[pl.ds(i * part, part)], rows.at[pl.ds(i * part, part)], in_sem.at[i])
             for i in range(SPREAD)]
    for load in loads:
        load.start()
    stores = []
    for i in range(SPREAD):
        loads[i].wait()
        for at in range(i * part, (i + 1) * part, 128):
            block = rows[at:at + 128, :].T
            cols[:, at:at + 128] = block[:chans]
            cols[:, tokens // 2 + at:tokens // 2 + at + 128] = block[chans:]
        for half in range(2):
            at = pl.ds(half * (tokens // 2) + i * part, part)
            stores.append(pltpu.make_async_copy(cols.at[:, at], out_hbm.at[:, at], out_sem.at[2 * i + half]))
            stores[-1].start()
    for store in stores:
        store.wait()


def solution(mesh):
    n_time = mesh.shape['time']

    def per_device(x_init, w_in, w_out, mod_scale, mod_shift, step_size):
        _, tokens, chans = x_init.shape
        hidden = w_in.shape[1]
        tok = 2 * GROUP
        f32, bf16 = jnp.float32, jnp.bfloat16
        vmem, hbm = pl.BlockSpec(memory_space=pltpu.VMEM), pl.BlockSpec(memory_space=pltpu.HBM)
        out = pl.pallas_call(
            functools.partial(kernel, n_time),
            out_shape=jax.ShapeDtypeStruct((CHUNKS, n_time, GROUP, 2 * chans), f32),
            in_specs=[hbm] * 5 + [vmem],
            out_specs=hbm,
            scratch_shapes=[
                pltpu.VMEM((chans, hidden), bf16),
                pltpu.VMEM((chans, hidden), bf16),
                pltpu.VMEM((1, hidden), bf16),
                pltpu.VMEM((1, hidden), bf16),
                pltpu.VMEM((2 * CHUNKS, chans, 128), f32),
                pltpu.VMEM((2 * CHUNKS, 128, chans), f32),
                pltpu.VMEM((CHUNKS * tok, chans), f32),
                pltpu.VMEM((hidden, chans), bf16),
                pltpu.VMEM((16, TILE), bf16),
                pltpu.VMEM((n_time, 16, TILE), bf16),
                pltpu.VMEM((n_time, 16, TILE), f32),
                pltpu.VMEM((CHUNKS * tok, hidden), f32),
                pltpu.VMEM((n_time, CHUNKS * tok, chans), f32),
                pltpu.VMEM((CHUNKS, n_time * tok, chans), bf16),
                pltpu.VMEM((CHUNKS, n_time, GROUP, 2 * chans), f32),
                pltpu.VMEM((tok, chans), f32),
                pltpu.SemaphoreType.DMA((4,)),
                pltpu.SemaphoreType.DMA((2 * CHUNKS,)),
                pltpu.SemaphoreType.DMA,
                pltpu.SemaphoreType.DMA((n_time // 2,)),
                pltpu.SemaphoreType.DMA,
                pltpu.SemaphoreType.DMA((n_time // 2,)),
                pltpu.SemaphoreType.DMA,
                pltpu.SemaphoreType.DMA((CHUNKS,)),
                pltpu.SemaphoreType.DMA((CHUNKS,)),
            ],
            compiler_params=pltpu.CompilerParams(has_side_effects=True, collective_id=0),
            name='sweeps',
        )(x_init[0].T, w_in, w_out.T, mod_scale, mod_shift, step_size[None])
        out = pl.pallas_call(
            spread, out_shape=jax.ShapeDtypeStruct((chans, tokens), f32), in_specs=[hbm], out_specs=hbm,
            scratch_shapes=[
                pltpu.VMEM((tokens // 2, 2 * chans), f32),
                pltpu.VMEM((chans, tokens), f32),
                pltpu.SemaphoreType.DMA((SPREAD,)),
                pltpu.SemaphoreType.DMA((2 * SPREAD,)),
            ],
            name='spread',
        )(out.reshape(tokens // 2, 2 * chans))
        return out.T.reshape(1, 1, tokens, chans)

    return jax.shard_map(per_device, mesh=mesh, in_specs=(P('data'), P(), P(), P('time'), P('time'), P('time')), out_specs=P('time', 'data'), check_vma=False)
```

```python
import functools

import jax
import jax.numpy as jnp
from jax import lax
from jax.experimental import pallas as pl
from jax.experimental.pallas import tpu as pltpu
from jax.sharding import PartitionSpec as P

SWEEPS = 4
C0 = 0.7978845608028654
C1 = C0 * 0.044715
TILE = 256
ROWS = 1024
CHUNKS = 2
GROUP = 8
SPREAD = 4
SIDE = 4
ARRIVE = 8
MESH = pl.DeviceIdType.MESH


def half_gelu(h):
    t = jnp.tanh(h * (h * h * (8.0 * C1) + 2.0 * C0))
    return h + h * t


def wait_bytes(ref, sem):
    pltpu.make_async_copy(ref, ref, sem).wait()


NEAR = (0, 1, 3, 2)


def hop(t):
    return t + (t // 2) * (1 - 2 * lax.rem(t, 2))


def kernel(n_time, x_hbm, w1_hbm, w2t_hbm, scale_hbm, shift_hbm, step_ref, out_ref,
           w1_ref, w2t_ref, scale_ref, shift_ref, xcol, xrow, x0, w2, mod_send, mod_recv, mods, p0, drift, xbf, send, prefix, w1p,
           load_sem, x_sem, mod_send_sem, mod_recv_sem, pair_send_sem, pair_recv_sem, out_send_sem, out_recv_sem, own_sem):
    me = lax.axis_index('time')
    n_chips = n_time // 2
    chip = me // 2
    core = lax.rem(me, 2)
    partner = me + 1 - 2 * core
    chans, hidden = w1_ref.shape
    n_rows = hidden // TILE
    tok = 2 * GROUP
    tokens = x_hbm.shape[1]

    barrier = pltpu.get_barrier_semaphore()

    place_x, place_y, place_z = lax.rem(chip, SIDE), lax.rem(chip // SIDE, SIDE), chip // (SIDE * SIDE)

    def along(place, step):
        return lax.rem(place + step + SIDE, SIDE)

    xs = [along(place_x, step) for step in NEAR]
    ys = [along(place_y, step) * SIDE for step in NEAR]
    zs = [along(place_z, step) * (SIDE * SIDE) for step in NEAR]

    def other_chips():
        for k in range(n_chips - 1, 0, -1):
            yield zs[k // (SIDE * SIDE)] + ys[k // SIDE % SIDE] + xs[k % SIDE]

    def arrive(dst):
        pl.semaphore_signal(barrier, inc=1, device_id={'time': dst}, device_id_type=MESH)

    for other in other_chips():
        arrive(2 * other)
        arrive(2 * other + 1)
    arrive(partner)

    loads = [pltpu.make_async_copy(src, dst, load_sem.at[i]) for i, (src, dst) in enumerate(
        [(scale_hbm, scale_ref), (shift_hbm, shift_ref), (w2t_hbm, w2t_ref), (w1_hbm, w1_ref)])]
    for load in loads:
        load.start()
    x_copies = []
    for i in range(2 * CHUNKS):
        start = (i % 2) * (tokens // 2) + (i // 2) * (tokens // 2 // CHUNKS) + (me * GROUP // 128) * 128
        x_copies.append(pltpu.make_async_copy(
            x_hbm.at[:, pl.ds(pl.multiple_of(start, 128), 128)], xcol.at[i], x_sem.at[i]))
        x_copies[-1].start()

    loads[0].wait()
    loads[1].wait()
    for n in range(n_rows):
        mod_send[pl.ds(n, 1), :] = scale_ref[:, n * TILE:(n + 1) * TILE]
        mod_send[pl.ds(n_rows + n, 1), :] = shift_ref[:, n * TILE:(n + 1) * TILE]
    step = jnp.broadcast_to(step_ref[...], (1, TILE))
    high = step.astype(jnp.bfloat16)
    rest = step - high.astype(jnp.float32)
    mid = rest.astype(jnp.bfloat16)
    low = (rest - mid.astype(jnp.float32)).astype(jnp.bfloat16)
    mod_send[pl.ds(2 * n_rows, 1), :] = high
    mod_send[pl.ds(2 * n_rows + 1, 1), :] = mid
    mod_send[pl.ds(2 * n_rows + 2, 1), :] = low
    mod_recv[me] = mod_send[...]

    loads[2].wait()
    w2[...] = w2t_ref[...].astype(jnp.float32).T.astype(jnp.bfloat16)
    lo = pl.ds(pl.multiple_of(lax.rem(me * GROUP, 128), GROUP), GROUP)
    for i in range(2 * CHUNKS):
        x_copies[i].wait()
        xrow[i] = xcol[i].T
        x0[i * GROUP:(i + 1) * GROUP, :] = xrow[i, lo, :]
    loads[3].wait()
    w1p[...] = jnp.concatenate([w1_ref[...], jnp.zeros_like(w1_ref)], axis=0)
    xbf[...] = jnp.zeros_like(xbf)
    x0_rounded = x0[...].astype(jnp.bfloat16)
    for n in range(hidden // TILE):
        p0[:, n * TILE:(n + 1) * TILE] = jnp.dot(
            x0_rounded, w1_ref[:, n * TILE:(n + 1) * TILE], preferred_element_type=jnp.float32)

    pl.semaphore_wait(barrier, n_time - 1)

    def group(g, sign):
        z = along(place_z, sign * hop(g // 2)) * (SIDE * SIDE)
        chips = []
        for i in range(2):
            zy = z + along(place_y, sign * hop(2 * lax.rem(g, 2) + i)) * SIDE
            chips += [zy + along(place_x, sign * step) for step in NEAR]
        return chips

    def mod_copy(k, dst):
        return pltpu.make_async_remote_copy(
            src_ref=mod_send, dst_ref=mod_recv.at[me], send_sem=mod_send_sem, recv_sem=mod_recv_sem.at[k],
            device_id={'time': dst}, device_id_type=MESH)

    def pair_copy(k, src, src_ref):
        return pltpu.make_async_remote_copy(
            src_ref=src_ref, dst_ref=mod_recv.at[src], send_sem=pair_send_sem, recv_sem=pair_recv_sem.at[k],
            device_id={'time': partner}, device_id_type=MESH)

    def send_group(g, first=0):
        for i, other in enumerate(group(g, 1)[first:], first):
            mod_copy(g * ARRIVE + i, 2 * other + core).start()

    def relay_group(g, first=0):
        for i, other in enumerate(group(g, -1)[first:], first):
            mod_copy(g * ARRIVE + i, me).wait_recv()
            src = 2 * other + core
            pair_copy(g * ARRIVE + i, src, mod_recv.at[src]).start()

    def pair_wait(g):
        for i in range(ARRIVE):
            pair_copy(g * ARRIVE + i, me, mod_send).wait_recv()

    def unpack(g):
        for other in group(g, -1):
            for j in (2 * other, 2 * other + 1):
                block = mod_recv[j].astype(jnp.float32)
                mods[j, pl.ds(0, n_rows), :] = 0.5 * (1.0 + block[:n_rows])
                mods[j, pl.ds(n_rows, n_rows), :] = 0.5 * block[n_rows:2 * n_rows]
                mods[j, pl.ds(2 * n_rows, 1), :] = (block[2 * n_rows:2 * n_rows + 1] + block[2 * n_rows + 1:2 * n_rows + 2]) + block[2 * n_rows + 2:2 * n_rows + 3]

    n_groups = n_chips // ARRIVE
    pair_copy(0, me, mod_send).start()
    send_group(0, 1)
    for g in range(1, n_groups):
        send_group(g)
    relay_group(0, 1)
    relay_group(1)
    pair_wait(0)
    unpack(0)

    def first_sweep(g, carry):
        pl.when(g + 2 < n_groups)(lambda: relay_group(g + 2))
        pl.when(g + 1 < n_groups)(lambda: pair_wait(g + 1))
        steps = [2 * other + c for other in group(g, -1) for c in range(2)]
        acc = None
        for n in range(hidden // TILE):
            parts = []
            for j in steps:
                h = p0[:, n * TILE:(n + 1) * TILE] * mods[j, pl.ds(n, 1), :] + mods[j, pl.ds(n_rows + n, 1), :]
                parts.append(half_gelu(h).astype(jnp.bfloat16))
            act = jnp.concatenate(parts, axis=0)
            prod = jnp.dot(act, w2[n * TILE:(n + 1) * TILE, :], preferred_element_type=jnp.float32)
            acc = prod if acc is None else acc + prod
        for i, j in enumerate(steps):
            drift[j] = mods[j, pl.ds(2 * n_rows, 1), :][:, :chans] * acc[i * CHUNKS * tok:(i + 1) * CHUNKS * tok, :]
        unpack(lax.rem(g + 1, n_groups))
        return carry

    lax.fori_loop(0, n_groups, first_sweep, 0)

    def first_prefix(j, total):
        new = (x0[...] + total).astype(jnp.bfloat16)
        for q in range(CHUNKS):
            xbf[q, pl.ds(pl.multiple_of(j * tok, tok), tok), 0:chans] = new[q * tok:(q + 1) * tok]
        return total + drift[j]

    lax.fori_loop(0, n_time, first_prefix, jnp.zeros((CHUNKS * tok, chans), jnp.float32), unroll=8)

    steps = ROWS // tok

    def block_step(q, b, carry):
        acc = None
        x = xbf[q, pl.ds(pl.multiple_of(b * ROWS, ROWS), ROWS), :]
        for n in range(hidden // TILE):
            pre = jnp.dot(x, w1p[:, n * TILE:(n + 1) * TILE], preferred_element_type=jnp.float32)
            parts = []
            for s in range(steps):
                j = b * steps + s
                h = pre[s * tok:(s + 1) * tok] * mods[j, pl.ds(n, 1), :] + mods[j, pl.ds(n_rows + n, 1), :]
                parts.append(half_gelu(h).astype(jnp.bfloat16))
            act = jnp.concatenate(parts, axis=0)
            prod = jnp.dot(act, w2[n * TILE:(n + 1) * TILE, :], preferred_element_type=jnp.float32)
            acc = prod if acc is None else acc + prod
        start = x0[pl.ds(pl.multiple_of(q * tok, tok), tok), :]
        total = prefix[...]
        for s in range(steps):
            j = b * steps + s
            new = start + total
            xbf[q, pl.ds(pl.multiple_of(j * tok, tok), tok), 0:chans] = new.astype(jnp.bfloat16)
            send[q, j, :, 0:chans] = new[:GROUP]
            send[q, j, :, chans:2 * chans] = new[GROUP:]
            total = total + mods[j, pl.ds(2 * n_rows, 1), :][:, :chans] * acc[s * tok:(s + 1) * tok, :]
        prefix[...] = total
        return carry

    def own_copy(q):
        return pltpu.make_async_copy(send.at[q, me], out_ref.at[q, me], own_sem.at[q])

    def chunk(q, carry):
        def sweep(i, carry):
            prefix[...] = jnp.zeros_like(prefix)
            return lax.fori_loop(0, n_time // steps, functools.partial(block_step, q), carry)

        lax.fori_loop(1, SWEEPS, sweep, 0)

        def out_copy(dst):
            return pltpu.make_async_remote_copy(
                src_ref=send.at[q, dst], dst_ref=out_ref.at[q, me], send_sem=out_send_sem, recv_sem=out_recv_sem.at[q],
                device_id={'time': dst}, device_id_type=MESH)

        for other in other_chips():
            out_copy(2 * other + core).start()
            out_copy(2 * other + 1 - core).start()
        out_copy(partner).start()
        own_copy(q).start()
        return carry

    lax.fori_loop(0, CHUNKS, chunk, 0)

    half_block = mod_recv.at[pl.ds(0, n_chips)]
    wait_bytes(half_block, pair_send_sem)
    wait_bytes(mod_recv.at[pl.ds(0, n_chips - 1)], mod_send_sem)
    for q in range(CHUNKS):
        own_copy(q).wait()
        wait_bytes(out_ref.at[q, pl.ds(0, n_time - 1)], out_recv_sem.at[q])
    wait_bytes(send.at[:, pl.ds(0, n_time - 1)], out_send_sem)


def spread(rows_hbm, out_hbm, rows, cols, in_sem, out_sem):
    chans, tokens = out_hbm.shape
    part = rows_hbm.shape[0] // SPREAD
    loads = [pltpu.make_async_copy(rows_hbm.at[pl.ds(i * part, part)], rows.at[pl.ds(i * part, part)], in_sem.at[i])
             for i in range(SPREAD)]
    for load in loads:
        load.start()
    stores = []
    for i in range(SPREAD):
        loads[i].wait()
        for at in range(i * part, (i + 1) * part, 128):
            block = rows[at:at + 128, :].T
            cols[:, at:at + 128] = block[:chans]
            cols[:, tokens // 2 + at:tokens // 2 + at + 128] = block[chans:]
        for half in range(2):
            at = pl.ds(half * (tokens // 2) + i * part, part)
            stores.append(pltpu.make_async_copy(cols.at[:, at], out_hbm.at[:, at], out_sem.at[2 * i + half]))
            stores[-1].start()
    for store in stores:
        store.wait()


def solution(mesh):
    n_time = mesh.shape['time']

    def per_device(x_init, w_in, w_out, mod_scale, mod_shift, step_size):
        _, tokens, chans = x_init.shape
        hidden = w_in.shape[1]
        tok = 2 * GROUP
        f32, bf16 = jnp.float32, jnp.bfloat16
        vmem, hbm = pl.BlockSpec(memory_space=pltpu.VMEM), pl.BlockSpec(memory_space=pltpu.HBM)
        out = pl.pallas_call(
            functools.partial(kernel, n_time),
            out_shape=jax.ShapeDtypeStruct((CHUNKS, n_time, GROUP, 2 * chans), f32),
            in_specs=[hbm] * 5 + [vmem],
            out_specs=hbm,
            scratch_shapes=[
                pltpu.VMEM((chans, hidden), bf16),
                pltpu.VMEM((chans, hidden), bf16),
                pltpu.VMEM((1, hidden), bf16),
                pltpu.VMEM((1, hidden), bf16),
                pltpu.VMEM((2 * CHUNKS, chans, 128), f32),
                pltpu.VMEM((2 * CHUNKS, 128, chans), f32),
                pltpu.VMEM((CHUNKS * tok, chans), f32),
                pltpu.VMEM((hidden, chans), bf16),
                pltpu.VMEM((16, TILE), bf16),
                pltpu.VMEM((n_time, 16, TILE), bf16),
                pltpu.VMEM((n_time, 16, TILE), f32),
                pltpu.VMEM((CHUNKS * tok, hidden), f32),
                pltpu.VMEM((n_time, CHUNKS * tok, chans), f32),
                pltpu.VMEM((CHUNKS, n_time * tok, 128), bf16),
                pltpu.VMEM((CHUNKS, n_time, GROUP, 2 * chans), f32),
                pltpu.VMEM((tok, chans), f32),
                pltpu.VMEM((128, hidden), bf16),
                pltpu.SemaphoreType.DMA((4,)),
                pltpu.SemaphoreType.DMA((2 * CHUNKS,)),
                pltpu.SemaphoreType.DMA,
                pltpu.SemaphoreType.DMA((n_time // 2,)),
                pltpu.SemaphoreType.DMA,
                pltpu.SemaphoreType.DMA((n_time // 2,)),
                pltpu.SemaphoreType.DMA,
                pltpu.SemaphoreType.DMA((CHUNKS,)),
                pltpu.SemaphoreType.DMA((CHUNKS,)),
            ],
            compiler_params=pltpu.CompilerParams(has_side_effects=True, collective_id=0),
            name='sweeps',
        )(x_init[0].T, w_in, w_out.T, mod_scale, mod_shift, step_size[None])
        out = pl.pallas_call(
            spread, out_shape=jax.ShapeDtypeStruct((chans, tokens), f32), in_specs=[hbm], out_specs=hbm,
            scratch_shapes=[
                pltpu.VMEM((tokens // 2, 2 * chans), f32),
                pltpu.VMEM((chans, tokens), f32),
                pltpu.SemaphoreType.DMA((SPREAD,)),
                pltpu.SemaphoreType.DMA((2 * SPREAD,)),
            ],
            name='spread',
        )(out.reshape(tokens // 2, 2 * chans))
        return out.T.reshape(1, 1, tokens, chans)

    return jax.shard_map(per_device, mesh=mesh, in_specs=(P('data'), P(), P(), P('time'), P('time'), P('time')), out_specs=P('time', 'data'), check_vma=False)
```

```python
import functools

import jax
import jax.numpy as jnp
from jax import lax
from jax.experimental import pallas as pl
from jax.experimental.pallas import tpu as pltpu
from jax.sharding import PartitionSpec as P

SWEEPS = 4
C0 = 0.7978845608028654
C1 = C0 * 0.044715
TILE = 256
ROWS = 1024
TOKENS = (16, 8, 8)
SPREAD = 4
SIDE = 4
ARRIVE = 8
MESH = pl.DeviceIdType.MESH


def half_gelu(h):
    t = jnp.tanh(h * (h * h * (8.0 * C1) + 2.0 * C0))
    return h + h * t


def wait_bytes(ref, sem):
    pltpu.make_async_copy(ref, ref, sem).wait()


NEAR = (0, 1, 3, 2)


def hop(t):
    return t + (t // 2) * (1 - 2 * lax.rem(t, 2))


def kernel(n_time, x_hbm, w1_hbm, w2t_hbm, scale_hbm, shift_hbm, step_ref, out_a, out_b,
           w1_ref, w2t_ref, scale_ref, shift_ref, xcol, xrow, x0, w2, mod_send, mod_recv, mods, p0, drift, x_a, x_b, send_a, send_b, prefix,
           load_sem, x_sem, mod_send_sem, mod_recv_sem, pair_send_sem, pair_recv_sem, out_send_sem, out_recv_sem, own_sem):
    me = lax.axis_index('time')
    n_chips = n_time // 2
    chip = me // 2
    core = lax.rem(me, 2)
    partner = me + 1 - 2 * core
    chans, hidden = w1_ref.shape
    n_rows = hidden // TILE
    tokens = x_hbm.shape[1]
    n_chunks, n_tok = len(TOKENS), sum(TOKENS)
    first_tok = [sum(TOKENS[:q]) for q in range(n_chunks)]

    barrier = pltpu.get_barrier_semaphore()

    place_x, place_y, place_z = lax.rem(chip, SIDE), lax.rem(chip // SIDE, SIDE), chip // (SIDE * SIDE)

    def along(place, step):
        return lax.rem(place + step + SIDE, SIDE)

    xs = [along(place_x, step) for step in NEAR]
    ys = [along(place_y, step) * SIDE for step in NEAR]
    zs = [along(place_z, step) * (SIDE * SIDE) for step in NEAR]

    def other_chips():
        for k in range(n_chips - 1, 0, -1):
            yield zs[k // (SIDE * SIDE)] + ys[k // SIDE % SIDE] + xs[k % SIDE]

    def arrive(dst):
        pl.semaphore_signal(barrier, inc=1, device_id={'time': dst}, device_id_type=MESH)

    for other in other_chips():
        arrive(2 * other)
        arrive(2 * other + 1)
    arrive(partner)

    loads = [pltpu.make_async_copy(src, dst, load_sem.at[i]) for i, (src, dst) in enumerate(
        [(scale_hbm, scale_ref), (shift_hbm, shift_ref), (w2t_hbm, w2t_ref), (w1_hbm, w1_ref)])]
    for load in loads:
        load.start()
    x_copies = []
    for q in range(n_chunks):
        near = TOKENS[q] // 2
        for half in range(2):
            i = 2 * q + half
            start = half * (tokens // 2) + first_tok[q] // 2 * n_time + (me * near // 128) * 128
            x_copies.append(pltpu.make_async_copy(
                x_hbm.at[:, pl.ds(pl.multiple_of(start, 128), 128)], xcol.at[i], x_sem.at[i]))
            x_copies[-1].start()

    loads[0].wait()
    loads[1].wait()
    for n in range(n_rows):
        mod_send[pl.ds(n, 1), :] = scale_ref[:, n * TILE:(n + 1) * TILE]
        mod_send[pl.ds(n_rows + n, 1), :] = shift_ref[:, n * TILE:(n + 1) * TILE]
    step = jnp.broadcast_to(step_ref[...], (1, TILE))
    high = step.astype(jnp.bfloat16)
    rest = step - high.astype(jnp.float32)
    mid = rest.astype(jnp.bfloat16)
    low = (rest - mid.astype(jnp.float32)).astype(jnp.bfloat16)
    mod_send[pl.ds(2 * n_rows, 1), :] = high
    mod_send[pl.ds(2 * n_rows + 1, 1), :] = mid
    mod_send[pl.ds(2 * n_rows + 2, 1), :] = low
    mod_recv[me] = mod_send[...]

    loads[2].wait()
    w2[...] = w2t_ref[...].astype(jnp.float32).T.astype(jnp.bfloat16)
    for q in range(n_chunks):
        near = TOKENS[q] // 2
        lo = lax.rem(me * near, 128) // 8 * 8
        for half in range(2):
            i = 2 * q + half
            x_copies[i].wait()
            xrow[i] = xcol[i].T
            eight = xrow[i, pl.ds(pl.multiple_of(lo, 8), 8), :]
            if near == 4:
                eight = jnp.where(core == 1, eight[4:], eight[:4])
            x0[first_tok[q] + half * near:first_tok[q] + (half + 1) * near, :] = eight
    loads[3].wait()
    x0_rounded = x0[...].astype(jnp.bfloat16)
    for n in range(hidden // TILE):
        p0[:, n * TILE:(n + 1) * TILE] = jnp.dot(
            x0_rounded, w1_ref[:, n * TILE:(n + 1) * TILE], preferred_element_type=jnp.float32)

    pl.semaphore_wait(barrier, n_time - 1)

    def group(g, sign):
        z = along(place_z, sign * hop(g // 2)) * (SIDE * SIDE)
        chips = []
        for i in range(2):
            zy = z + along(place_y, sign * hop(2 * lax.rem(g, 2) + i)) * SIDE
            chips += [zy + along(place_x, sign * step) for step in NEAR]
        return chips

    def mod_copy(k, dst):
        return pltpu.make_async_remote_copy(
            src_ref=mod_send, dst_ref=mod_recv.at[me], send_sem=mod_send_sem, recv_sem=mod_recv_sem.at[k],
            device_id={'time': dst}, device_id_type=MESH)

    def pair_copy(k, src, src_ref):
        return pltpu.make_async_remote_copy(
            src_ref=src_ref, dst_ref=mod_recv.at[src], send_sem=pair_send_sem, recv_sem=pair_recv_sem.at[k],
            device_id={'time': partner}, device_id_type=MESH)

    def send_group(g, first=0):
        for i, other in enumerate(group(g, 1)[first:], first):
            mod_copy(g * ARRIVE + i, 2 * other + core).start()

    def relay_group(g, first=0):
        for i, other in enumerate(group(g, -1)[first:], first):
            mod_copy(g * ARRIVE + i, me).wait_recv()
            src = 2 * other + core
            pair_copy(g * ARRIVE + i, src, mod_recv.at[src]).start()

    def pair_wait(g):
        for i in range(ARRIVE):
            pair_copy(g * ARRIVE + i, me, mod_send).wait_recv()

    def unpack(g):
        for other in group(g, -1):
            for j in (2 * other, 2 * other + 1):
                block = mod_recv[j].astype(jnp.float32)
                mods[j, pl.ds(0, n_rows), :] = 0.5 * (1.0 + block[:n_rows])
                mods[j, pl.ds(n_rows, n_rows), :] = 0.5 * block[n_rows:2 * n_rows]
                mods[j, pl.ds(2 * n_rows, 1), :] = (block[2 * n_rows:2 * n_rows + 1] + block[2 * n_rows + 1:2 * n_rows + 2]) + block[2 * n_rows + 2:2 * n_rows + 3]

    n_groups = n_chips // ARRIVE
    pair_copy(0, me, mod_send).start()
    send_group(0, 1)
    for g in range(1, n_groups):
        send_group(g)
    relay_group(0, 1)
    relay_group(1)
    pair_wait(0)
    unpack(0)

    def first_sweep(g, carry):
        pl.when(g + 2 < n_groups)(lambda: relay_group(g + 2))
        pl.when(g + 1 < n_groups)(lambda: pair_wait(g + 1))
        steps = [2 * other + c for other in group(g, -1) for c in range(2)]
        acc = None
        for n in range(hidden // TILE):
            parts = []
            for j in steps:
                h = p0[:, n * TILE:(n + 1) * TILE] * mods[j, pl.ds(n, 1), :] + mods[j, pl.ds(n_rows + n, 1), :]
                parts.append(half_gelu(h).astype(jnp.bfloat16))
            act = jnp.concatenate(parts, axis=0)
            prod = jnp.dot(act, w2[n * TILE:(n + 1) * TILE, :], preferred_element_type=jnp.float32)
            acc = prod if acc is None else acc + prod
        for i, j in enumerate(steps):
            drift[j] = mods[j, pl.ds(2 * n_rows, 1), :][:, :chans] * acc[i * n_tok:(i + 1) * n_tok, :]
        unpack(lax.rem(g + 1, n_groups))
        return carry

    lax.fori_loop(0, n_groups, first_sweep, 0)

    def first_prefix(i, total):
        news = []
        for j in (2 * i, 2 * i + 1):
            news.append(x0[...] + total)
            total = total + drift[j]
        for q in range(n_chunks):
            rows = slice(first_tok[q], first_tok[q] + TOKENS[q])
            pair = jnp.concatenate([news[0][rows], news[1][rows]], axis=0).astype(jnp.bfloat16)
            at = pl.ds(pl.multiple_of(i * 2 * TOKENS[q], 16), 2 * TOKENS[q])
            if q == 0:
                x_a[at, :] = pair
            else:
                x_b[q - 1, at, :] = pair
        return total

    lax.fori_loop(0, n_time // 2, first_prefix, jnp.zeros((n_tok, chans), jnp.float32), unroll=4)

    def block_step(tok, x_at, send_at, start, b, carry):
        steps = ROWS // tok
        acc = None
        x = x_at[pl.ds(pl.multiple_of(b * ROWS, ROWS), ROWS), :]
        for n in range(hidden // TILE):
            pre = jnp.dot(x, w1_ref[:, n * TILE:(n + 1) * TILE], preferred_element_type=jnp.float32)
            parts = []
            for s in range(steps):
                j = b * steps + s
                h = pre[s * tok:(s + 1) * tok] * mods[j, pl.ds(n, 1), :] + mods[j, pl.ds(n_rows + n, 1), :]
                parts.append(h)
            act = half_gelu(jnp.concatenate(parts, axis=0)).astype(jnp.bfloat16)
            prod = jnp.dot(act, w2[n * TILE:(n + 1) * TILE, :], preferred_element_type=jnp.float32)
            acc = prod if acc is None else acc + prod
        total = prefix[0:tok, :]
        for s in range(0, steps, 2):
            j = b * steps + s
            news = []
            for i in range(2):
                news.append(start + total)
                send_at[j + i, :, 0:chans] = news[i][:tok // 2]
                send_at[j + i, :, chans:2 * chans] = news[i][tok // 2:]
                total = total + mods[j + i, pl.ds(2 * n_rows, 1), :][:, :chans] * acc[(s + i) * tok:(s + i + 1) * tok, :]
            x_at[pl.ds(pl.multiple_of(j * tok, 2 * tok), 2 * tok), :] = jnp.concatenate(news, axis=0).astype(jnp.bfloat16)
        prefix[0:tok, :] = total
        return carry

    def later_sweeps(tok, x_at, send_at, start):
        def sweep(i, carry):
            prefix[...] = jnp.zeros_like(prefix)
            return lax.fori_loop(0, n_time * tok // ROWS, functools.partial(block_step, tok, x_at, send_at, start), carry)

        lax.fori_loop(1, SWEEPS, sweep, 0)

    def own_copy(q, send_at, out_at):
        return pltpu.make_async_copy(send_at.at[me], out_at.at[me], own_sem.at[q])

    def exchange(q, send_at, out_at):
        def out_copy(dst):
            return pltpu.make_async_remote_copy(
                src_ref=send_at.at[dst], dst_ref=out_at.at[me], send_sem=out_send_sem.at[q], recv_sem=out_recv_sem.at[q],
                device_id={'time': dst}, device_id_type=MESH)

        for other in other_chips():
            out_copy(2 * other + core).start()
            out_copy(2 * other + 1 - core).start()
        out_copy(partner).start()
        own_copy(q, send_at, out_at).start()

    later_sweeps(TOKENS[0], x_a, send_a, x0[0:TOKENS[0], :])
    exchange(0, send_a, out_a)

    def small_chunk(i, carry):
        start = x0[pl.ds(pl.multiple_of(TOKENS[0] + i * TOKENS[1], TOKENS[1]), TOKENS[1]), :]
        later_sweeps(TOKENS[1], x_b.at[i], send_b.at[i], start)
        exchange(1 + i, send_b.at[i], out_b.at[i])
        return carry

    lax.fori_loop(0, n_chunks - 1, small_chunk, 0)

    half_block = mod_recv.at[pl.ds(0, n_chips)]
    wait_bytes(half_block, pair_send_sem)
    wait_bytes(mod_recv.at[pl.ds(0, n_chips - 1)], mod_send_sem)
    for q in range(n_chunks):
        send_at, out_at = (send_a, out_a) if q == 0 else (send_b.at[q - 1], out_b.at[q - 1])
        own_copy(q, send_at, out_at).wait()
        wait_bytes(out_at.at[pl.ds(0, n_time - 1)], out_recv_sem.at[q])
        wait_bytes(send_at.at[pl.ds(0, n_time - 1)], out_send_sem.at[q])


def spread(a_hbm, b_hbm, out_hbm, rows, cols, in_sem, out_sem):
    chans, tokens = out_hbm.shape
    part = rows.shape[0] // SPREAD
    loads = []
    for i in range(SPREAD):
        src, at = (a_hbm, i * part) if i < SPREAD // 2 else (b_hbm, i * part - a_hbm.shape[0])
        loads.append(pltpu.make_async_copy(src.at[pl.ds(at, part)], rows.at[pl.ds(i * part, part)], in_sem.at[i]))
    for load in loads:
        load.start()
    stores = []
    for i in range(SPREAD):
        loads[i].wait()
        for at in range(i * part, (i + 1) * part, 128):
            block = rows[at:at + 128, :].T
            cols[:, at:at + 128] = block[:chans]
            cols[:, tokens // 2 + at:tokens // 2 + at + 128] = block[chans:]
        for half in range(2):
            at = pl.ds(half * (tokens // 2) + i * part, part)
            stores.append(pltpu.make_async_copy(cols.at[:, at], out_hbm.at[:, at], out_sem.at[2 * i + half]))
            stores[-1].start()
    for store in stores:
        store.wait()


def solution(mesh):
    n_time = mesh.shape['time']

    def per_device(x_init, w_in, w_out, mod_scale, mod_shift, step_size):
        _, tokens, chans = x_init.shape
        hidden = w_in.shape[1]
        n_tok = sum(TOKENS)
        f32, bf16 = jnp.float32, jnp.bfloat16
        vmem, hbm = pl.BlockSpec(memory_space=pltpu.VMEM), pl.BlockSpec(memory_space=pltpu.HBM)
        shape_a = (n_time, TOKENS[0] // 2, 2 * chans)
        shape_b = (len(TOKENS) - 1, n_time, TOKENS[1] // 2, 2 * chans)
        out_a, out_b = pl.pallas_call(
            functools.partial(kernel, n_time),
            out_shape=[jax.ShapeDtypeStruct(shape_a, f32), jax.ShapeDtypeStruct(shape_b, f32)],
            in_specs=[hbm] * 5 + [vmem],
            out_specs=[hbm, hbm],
            scratch_shapes=[
                pltpu.VMEM((chans, hidden), bf16),
                pltpu.VMEM((chans, hidden), bf16),
                pltpu.VMEM((1, hidden), bf16),
                pltpu.VMEM((1, hidden), bf16),
                pltpu.VMEM((2 * len(TOKENS), chans, 128), f32),
                pltpu.VMEM((2 * len(TOKENS), 128, chans), f32),
                pltpu.VMEM((n_tok, chans), f32),
                pltpu.VMEM((hidden, chans), bf16),
                pltpu.VMEM((16, TILE), bf16),
                pltpu.VMEM((n_time, 16, TILE), bf16),
                pltpu.VMEM((n_time, 16, TILE), f32),
                pltpu.VMEM((n_tok, hidden), f32),
                pltpu.VMEM((n_time, n_tok, chans), f32),
                pltpu.VMEM((n_time * TOKENS[0], chans), bf16),
                pltpu.VMEM((len(TOKENS) - 1, n_time * TOKENS[1], chans), bf16),
                pltpu.VMEM(shape_a, f32),
                pltpu.VMEM(shape_b, f32),
                pltpu.VMEM((TOKENS[0], chans), f32),
                pltpu.SemaphoreType.DMA((4,)),
                pltpu.SemaphoreType.DMA((2 * len(TOKENS),)),
                pltpu.SemaphoreType.DMA,
                pltpu.SemaphoreType.DMA((n_time // 2,)),
                pltpu.SemaphoreType.DMA,
                pltpu.SemaphoreType.DMA((n_time // 2,)),
                pltpu.SemaphoreType.DMA((len(TOKENS),)),
                pltpu.SemaphoreType.DMA((len(TOKENS),)),
                pltpu.SemaphoreType.DMA((len(TOKENS),)),
            ],
            compiler_params=pltpu.CompilerParams(has_side_effects=True, collective_id=0),
            name='sweeps',
        )(x_init[0].T, w_in, w_out.T, mod_scale, mod_shift, step_size[None])
        out = pl.pallas_call(
            spread, out_shape=jax.ShapeDtypeStruct((chans, tokens), f32), in_specs=[hbm, hbm], out_specs=hbm,
            scratch_shapes=[
                pltpu.VMEM((tokens // 2, 2 * chans), f32),
                pltpu.VMEM((chans, tokens), f32),
                pltpu.SemaphoreType.DMA((SPREAD,)),
                pltpu.SemaphoreType.DMA((2 * SPREAD,)),
            ],
            name='spread',
        )(out_a.reshape(-1, 2 * chans), out_b.reshape(-1, 2 * chans))
        return out.T.reshape(1, 1, tokens, chans)

    return jax.shard_map(per_device, mesh=mesh, in_specs=(P('data'), P(), P(), P('time'), P('time'), P('time')), out_specs=P('time', 'data'), check_vma=False)
```

```python
import functools

import jax
import jax.numpy as jnp
from jax import lax
from jax.experimental import pallas as pl
from jax.experimental.pallas import tpu as pltpu
from jax.sharding import PartitionSpec as P

SWEEPS = 4
C0 = 0.7978845608028654
C1 = C0 * 0.044715
TILE = 256
ROWS = 1024
TOKENS = (16, 8, 8)
SPREAD = 8
SIDE = 4
ARRIVE = 8
MESH = pl.DeviceIdType.MESH


def half_gelu(h):
    t = jnp.tanh(h * (h * h * (8.0 * C1) + 2.0 * C0))
    return h + h * t


def wait_bytes(ref, sem):
    pltpu.make_async_copy(ref, ref, sem).wait()


NEAR = (0, 1, 3, 2)


def hop(t):
    return t + (t // 2) * (1 - 2 * lax.rem(t, 2))


def kernel(n_time, x_hbm, w1_hbm, w2t_hbm, scale_hbm, shift_hbm, step_ref, out_a, out_b,
           w1_ref, w2t_ref, scale_ref, shift_ref, xcol, xrow, x0, w2, mod_send, mod_recv, mods, p0, drift, x_a, x_b, send_a, send_b, prefix,
           load_sem, x_sem, mod_send_sem, mod_recv_sem, pair_send_sem, pair_recv_sem, out_send_sem, out_recv_sem, own_sem):
    me = lax.axis_index('time')
    n_chips = n_time // 2
    chip = me // 2
    core = lax.rem(me, 2)
    partner = me + 1 - 2 * core
    chans, hidden = w1_ref.shape
    n_rows = hidden // TILE
    tokens = x_hbm.shape[1]
    n_chunks, n_tok = len(TOKENS), sum(TOKENS)
    first_tok = [sum(TOKENS[:q]) for q in range(n_chunks)]

    barrier = pltpu.get_barrier_semaphore()

    place_x, place_y, place_z = lax.rem(chip, SIDE), lax.rem(chip // SIDE, SIDE), chip // (SIDE * SIDE)

    def along(place, step):
        return lax.rem(place + step + SIDE, SIDE)

    xs = [along(place_x, step) for step in NEAR]
    ys = [along(place_y, step) * SIDE for step in NEAR]
    zs = [along(place_z, step) * (SIDE * SIDE) for step in NEAR]

    def other_chips():
        for k in range(n_chips - 1, 0, -1):
            yield zs[k // (SIDE * SIDE)] + ys[k // SIDE % SIDE] + xs[k % SIDE]

    def arrive(dst):
        pl.semaphore_signal(barrier, inc=1, device_id={'time': dst}, device_id_type=MESH)

    for other in other_chips():
        arrive(2 * other)
        arrive(2 * other + 1)
    arrive(partner)

    loads = [pltpu.make_async_copy(src, dst, load_sem.at[i]) for i, (src, dst) in enumerate(
        [(scale_hbm, scale_ref), (shift_hbm, shift_ref), (w2t_hbm, w2t_ref), (w1_hbm, w1_ref)])]
    for load in loads:
        load.start()
    x_copies = []
    for q in range(n_chunks):
        near = TOKENS[q] // 2
        for half in range(2):
            i = 2 * q + half
            start = half * (tokens // 2) + first_tok[q] // 2 * n_time + (me * near // 128) * 128
            x_copies.append(pltpu.make_async_copy(
                x_hbm.at[:, pl.ds(pl.multiple_of(start, 128), 128)], xcol.at[i], x_sem.at[i]))
            x_copies[-1].start()

    loads[0].wait()
    loads[1].wait()
    for n in range(n_rows):
        mod_send[pl.ds(n, 1), :] = scale_ref[:, n * TILE:(n + 1) * TILE]
        mod_send[pl.ds(n_rows + n, 1), :] = shift_ref[:, n * TILE:(n + 1) * TILE]
    step = jnp.broadcast_to(step_ref[...], (1, TILE))
    high = step.astype(jnp.bfloat16)
    rest = step - high.astype(jnp.float32)
    mid = rest.astype(jnp.bfloat16)
    low = (rest - mid.astype(jnp.float32)).astype(jnp.bfloat16)
    mod_send[pl.ds(2 * n_rows, 1), :] = high
    mod_send[pl.ds(2 * n_rows + 1, 1), :] = mid
    mod_send[pl.ds(2 * n_rows + 2, 1), :] = low
    mod_recv[me] = mod_send[...]

    loads[2].wait()
    w2[...] = w2t_ref[...].astype(jnp.float32).T.astype(jnp.bfloat16)
    for q in range(n_chunks):
        near = TOKENS[q] // 2
        lo = lax.rem(me * near, 128) // 8 * 8
        for half in range(2):
            i = 2 * q + half
            x_copies[i].wait()
            xrow[i] = xcol[i].T
            eight = xrow[i, pl.ds(pl.multiple_of(lo, 8), 8), :]
            if near == 4:
                eight = jnp.where(core == 1, eight[4:], eight[:4])
            x0[first_tok[q] + half * near:first_tok[q] + (half + 1) * near, :] = eight
    loads[3].wait()
    x0_rounded = x0[...].astype(jnp.bfloat16)
    for n in range(hidden // TILE):
        p0[:, n * TILE:(n + 1) * TILE] = jnp.dot(
            x0_rounded, w1_ref[:, n * TILE:(n + 1) * TILE], preferred_element_type=jnp.float32)

    pl.semaphore_wait(barrier, n_time - 1)

    def group(g, sign):
        z = along(place_z, sign * hop(g // 2)) * (SIDE * SIDE)
        chips = []
        for i in range(2):
            zy = z + along(place_y, sign * hop(2 * lax.rem(g, 2) + i)) * SIDE
            chips += [zy + along(place_x, sign * step) for step in NEAR]
        return chips

    def mod_copy(k, dst):
        return pltpu.make_async_remote_copy(
            src_ref=mod_send, dst_ref=mod_recv.at[me], send_sem=mod_send_sem, recv_sem=mod_recv_sem.at[k],
            device_id={'time': dst}, device_id_type=MESH)

    def pair_copy(k, src, src_ref):
        return pltpu.make_async_remote_copy(
            src_ref=src_ref, dst_ref=mod_recv.at[src], send_sem=pair_send_sem, recv_sem=pair_recv_sem.at[k],
            device_id={'time': partner}, device_id_type=MESH)

    def send_group(g, first=0):
        for i, other in enumerate(group(g, 1)[first:], first):
            mod_copy(g * ARRIVE + i, 2 * other + core).start()

    def relay_group(g, first=0):
        for i, other in enumerate(group(g, -1)[first:], first):
            mod_copy(g * ARRIVE + i, me).wait_recv()
            src = 2 * other + core
            pair_copy(g * ARRIVE + i, src, mod_recv.at[src]).start()

    def pair_wait(g):
        for i in range(ARRIVE):
            pair_copy(g * ARRIVE + i, me, mod_send).wait_recv()

    def unpack(g):
        for other in group(g, -1):
            for j in (2 * other, 2 * other + 1):
                block = mod_recv[j].astype(jnp.float32)
                mods[j, pl.ds(0, n_rows), :] = 0.5 * (1.0 + block[:n_rows])
                mods[j, pl.ds(n_rows, n_rows), :] = 0.5 * block[n_rows:2 * n_rows]
                mods[j, pl.ds(2 * n_rows, 1), :] = (block[2 * n_rows:2 * n_rows + 1] + block[2 * n_rows + 1:2 * n_rows + 2]) + block[2 * n_rows + 2:2 * n_rows + 3]

    n_groups = n_chips // ARRIVE
    pair_copy(0, me, mod_send).start()
    send_group(0, 1)
    for g in range(1, n_groups):
        send_group(g)
    relay_group(0, 1)
    pair_wait(0)
    unpack(0)

    def first_sweep(g, carry):
        pl.when(g + 1 < n_groups)(lambda: relay_group(g + 1))
        steps = [2 * other + c for other in group(g, -1) for c in range(2)]
        acc = None
        for n in range(hidden // TILE):
            parts = []
            for j in steps:
                h = p0[:, n * TILE:(n + 1) * TILE] * mods[j, pl.ds(n, 1), :] + mods[j, pl.ds(n_rows + n, 1), :]
                parts.append(half_gelu(h).astype(jnp.bfloat16))
            act = jnp.concatenate(parts, axis=0)
            prod = jnp.dot(act, w2[n * TILE:(n + 1) * TILE, :], preferred_element_type=jnp.float32)
            acc = prod if acc is None else acc + prod
        for i, j in enumerate(steps):
            drift[j] = mods[j, pl.ds(2 * n_rows, 1), :][:, :chans] * acc[i * n_tok:(i + 1) * n_tok, :]

        @pl.when(g + 1 < n_groups)
        def _():
            pair_wait(g + 1)
            unpack(g + 1)

        return carry

    lax.fori_loop(0, n_groups, first_sweep, 0)

    def first_prefix(i, total):
        news = []
        for j in (2 * i, 2 * i + 1):
            news.append(x0[...] + total)
            total = total + drift[j]
        for q in range(n_chunks):
            rows = slice(first_tok[q], first_tok[q] + TOKENS[q])
            pair = jnp.concatenate([news[0][rows], news[1][rows]], axis=0).astype(jnp.bfloat16)
            at = pl.ds(pl.multiple_of(i * 2 * TOKENS[q], 16), 2 * TOKENS[q])
            if q == 0:
                x_a[at, :] = pair
            else:
                x_b[q - 1, at, :] = pair
        return total

    lax.fori_loop(0, n_time // 2, first_prefix, jnp.zeros((n_tok, chans), jnp.float32), unroll=4)

    def block_step(tok, x_at, send_at, start, b, carry):
        steps = ROWS // tok
        acc = None
        x = x_at[pl.ds(pl.multiple_of(b * ROWS, ROWS), ROWS), :]
        for n in range(hidden // TILE):
            pre = jnp.dot(x, w1_ref[:, n * TILE:(n + 1) * TILE], preferred_element_type=jnp.float32)
            parts = []
            for s in range(steps):
                j = b * steps + s
                h = pre[s * tok:(s + 1) * tok] * mods[j, pl.ds(n, 1), :] + mods[j, pl.ds(n_rows + n, 1), :]
                parts.append(h)
            act = half_gelu(jnp.concatenate(parts, axis=0)).astype(jnp.bfloat16)
            prod = jnp.dot(act, w2[n * TILE:(n + 1) * TILE, :], preferred_element_type=jnp.float32)
            acc = prod if acc is None else acc + prod
        total = prefix[0:tok, :]
        for s in range(0, steps, 2):
            j = b * steps + s
            news = []
            for i in range(2):
                news.append(start + total)
                send_at[j + i, :, 0:chans] = news[i][:tok // 2]
                send_at[j + i, :, chans:2 * chans] = news[i][tok // 2:]
                total = total + mods[j + i, pl.ds(2 * n_rows, 1), :][:, :chans] * acc[(s + i) * tok:(s + i + 1) * tok, :]
            x_at[pl.ds(pl.multiple_of(j * tok, 2 * tok), 2 * tok), :] = jnp.concatenate(news, axis=0).astype(jnp.bfloat16)
        prefix[0:tok, :] = total
        return carry

    def later_sweeps(tok, x_at, send_at, start):
        def sweep(i, carry):
            prefix[...] = jnp.zeros_like(prefix)
            return lax.fori_loop(0, n_time * tok // ROWS, functools.partial(block_step, tok, x_at, send_at, start), carry)

        lax.fori_loop(1, SWEEPS, sweep, 0)

    def own_copy(q, send_at, out_at):
        return pltpu.make_async_copy(send_at.at[me], out_at.at[me], own_sem.at[q])

    def exchange(q, send_at, out_at):
        def out_copy(dst):
            return pltpu.make_async_remote_copy(
                src_ref=send_at.at[dst], dst_ref=out_at.at[me], send_sem=out_send_sem.at[q], recv_sem=out_recv_sem.at[q],
                device_id={'time': dst}, device_id_type=MESH)

        for other in other_chips():
            out_copy(2 * other + core).start()
            out_copy(2 * other + 1 - core).start()
        out_copy(partner).start()
        own_copy(q, send_at, out_at).start()

    later_sweeps(TOKENS[0], x_a, send_a, x0[0:TOKENS[0], :])
    exchange(0, send_a, out_a)

    def small_chunk(i, carry):
        start = x0[pl.ds(pl.multiple_of(TOKENS[0] + i * TOKENS[1], TOKENS[1]), TOKENS[1]), :]
        later_sweeps(TOKENS[1], x_b.at[i], send_b.at[i], start)
        exchange(1 + i, send_b.at[i], out_b.at[i])
        return carry

    lax.fori_loop(0, n_chunks - 1, small_chunk, 0)

    half_block = mod_recv.at[pl.ds(0, n_chips)]
    wait_bytes(half_block, pair_send_sem)
    wait_bytes(mod_recv.at[pl.ds(0, n_chips - 1)], mod_send_sem)
    for q in range(n_chunks):
        send_at, out_at = (send_a, out_a) if q == 0 else (send_b.at[q - 1], out_b.at[q - 1])
        own_copy(q, send_at, out_at).wait()
        wait_bytes(out_at.at[pl.ds(0, n_time - 1)], out_recv_sem.at[q])
        wait_bytes(send_at.at[pl.ds(0, n_time - 1)], out_send_sem.at[q])


def spread(a_hbm, b_hbm, out_hbm, rows, cols, in_sem, out_sem):
    chans, tokens = out_hbm.shape
    part = rows.shape[0] // SPREAD
    loads = []
    for i in range(SPREAD):
        src, at = (a_hbm, i * part) if i < SPREAD // 2 else (b_hbm, i * part - a_hbm.shape[0])
        loads.append(pltpu.make_async_copy(src.at[pl.ds(at, part)], rows.at[pl.ds(i * part, part)], in_sem.at[i]))
    for load in loads:
        load.start()
    stores = []
    for i in range(SPREAD):
        loads[i].wait()
        for at in range(i * part, (i + 1) * part, 128):
            block = rows[at:at + 128, :].T
            cols[:, at:at + 128] = block[:chans]
            cols[:, tokens // 2 + at:tokens // 2 + at + 128] = block[chans:]
        for half in range(2):
            at = pl.ds(half * (tokens // 2) + i * part, part)
            stores.append(pltpu.make_async_copy(cols.at[:, at], out_hbm.at[:, at], out_sem.at[2 * i + half]))
            stores[-1].start()
    for store in stores:
        store.wait()


def solution(mesh):
    n_time = mesh.shape['time']

    def per_device(x_init, w_in, w_out, mod_scale, mod_shift, step_size):
        _, tokens, chans = x_init.shape
        hidden = w_in.shape[1]
        n_tok = sum(TOKENS)
        f32, bf16 = jnp.float32, jnp.bfloat16
        vmem, hbm = pl.BlockSpec(memory_space=pltpu.VMEM), pl.BlockSpec(memory_space=pltpu.HBM)
        shape_a = (n_time, TOKENS[0] // 2, 2 * chans)
        shape_b = (len(TOKENS) - 1, n_time, TOKENS[1] // 2, 2 * chans)
        out_a, out_b = pl.pallas_call(
            functools.partial(kernel, n_time),
            out_shape=[jax.ShapeDtypeStruct(shape_a, f32), jax.ShapeDtypeStruct(shape_b, f32)],
            in_specs=[hbm] * 5 + [vmem],
            out_specs=[hbm, hbm],
            scratch_shapes=[
                pltpu.VMEM((chans, hidden), bf16),
                pltpu.VMEM((chans, hidden), bf16),
                pltpu.VMEM((1, hidden), bf16),
                pltpu.VMEM((1, hidden), bf16),
                pltpu.VMEM((2 * len(TOKENS), chans, 128), f32),
                pltpu.VMEM((2 * len(TOKENS), 128, chans), f32),
                pltpu.VMEM((n_tok, chans), f32),
                pltpu.VMEM((hidden, chans), bf16),
                pltpu.VMEM((16, TILE), bf16),
                pltpu.VMEM((n_time, 16, TILE), bf16),
                pltpu.VMEM((n_time, 16, TILE), f32),
                pltpu.VMEM((n_tok, hidden), f32),
                pltpu.VMEM((n_time, n_tok, chans), f32),
                pltpu.VMEM((n_time * TOKENS[0], chans), bf16),
                pltpu.VMEM((len(TOKENS) - 1, n_time * TOKENS[1], chans), bf16),
                pltpu.VMEM(shape_a, f32),
                pltpu.VMEM(shape_b, f32),
                pltpu.VMEM((TOKENS[0], chans), f32),
                pltpu.SemaphoreType.DMA((4,)),
                pltpu.SemaphoreType.DMA((2 * len(TOKENS),)),
                pltpu.SemaphoreType.DMA,
                pltpu.SemaphoreType.DMA((n_time // 2,)),
                pltpu.SemaphoreType.DMA,
                pltpu.SemaphoreType.DMA((n_time // 2,)),
                pltpu.SemaphoreType.DMA((len(TOKENS),)),
                pltpu.SemaphoreType.DMA((len(TOKENS),)),
                pltpu.SemaphoreType.DMA((len(TOKENS),)),
            ],
            compiler_params=pltpu.CompilerParams(has_side_effects=True, collective_id=0),
            name='sweeps',
        )(x_init[0].T, w_in, w_out.T, mod_scale, mod_shift, step_size[None])
        out = pl.pallas_call(
            spread, out_shape=jax.ShapeDtypeStruct((chans, tokens), f32), in_specs=[hbm, hbm], out_specs=hbm,
            scratch_shapes=[
                pltpu.VMEM((tokens // 2, 2 * chans), f32),
                pltpu.VMEM((chans, tokens), f32),
                pltpu.SemaphoreType.DMA((SPREAD,)),
                pltpu.SemaphoreType.DMA((2 * SPREAD,)),
            ],
            name='spread',
        )(out_a.reshape(-1, 2 * chans), out_b.reshape(-1, 2 * chans))
        return out.T.reshape(1, 1, tokens, chans)

    return jax.shard_map(per_device, mesh=mesh, in_specs=(P('data'), P(), P(), P('time'), P('time'), P('time')), out_specs=P('time', 'data'), check_vma=False)
```

```python
import functools

import jax
import jax.numpy as jnp
from jax import lax
from jax.experimental import pallas as pl
from jax.experimental.pallas import tpu as pltpu
from jax.sharding import PartitionSpec as P

SWEEPS = 4
C0 = 0.7978845608028654
C1 = C0 * 0.044715
TILE = 256
ROWS = 1024
TOKENS = (16, 8, 8)
SPREAD = 2
SIDE = 4
ARRIVE = 8
MESH = pl.DeviceIdType.MESH


def half_gelu(h):
    t = jnp.tanh(h * (h * h * (8.0 * C1) + 2.0 * C0))
    return h + h * t


def wait_bytes(ref, sem):
    pltpu.make_async_copy(ref, ref, sem).wait()


NEAR = (0, 1, 3, 2)


def hop(t):
    return t + (t // 2) * (1 - 2 * lax.rem(t, 2))


def kernel(n_time, x_hbm, w1_hbm, w2t_hbm, scale_hbm, shift_hbm, step_ref, out_a, out_b,
           w1_ref, w2t_ref, scale_ref, shift_ref, xcol, xrow, x0, w2, mod_send, mod_recv, mods, p0, drift, x_a, x_b, send_a, send_b, prefix,
           load_sem, x_sem, mod_send_sem, mod_recv_sem, pair_send_sem, pair_recv_sem, out_send_sem, out_recv_sem, own_sem):
    me = lax.axis_index('time')
    n_chips = n_time // 2
    chip = me // 2
    core = lax.rem(me, 2)
    partner = me + 1 - 2 * core
    chans, hidden = w1_ref.shape
    n_rows = hidden // TILE
    tokens = x_hbm.shape[1]
    n_chunks, n_tok = len(TOKENS), sum(TOKENS)
    first_tok = [sum(TOKENS[:q]) for q in range(n_chunks)]

    barrier = pltpu.get_barrier_semaphore()

    place_x, place_y, place_z = lax.rem(chip, SIDE), lax.rem(chip // SIDE, SIDE), chip // (SIDE * SIDE)

    def along(place, step):
        return lax.rem(place + step + SIDE, SIDE)

    xs = [along(place_x, step) for step in NEAR]
    ys = [along(place_y, step) * SIDE for step in NEAR]
    zs = [along(place_z, step) * (SIDE * SIDE) for step in NEAR]

    def other_chips():
        for k in range(n_chips - 1, 0, -1):
            yield zs[k // (SIDE * SIDE)] + ys[k // SIDE % SIDE] + xs[k % SIDE]

    def arrive(dst):
        pl.semaphore_signal(barrier, inc=1, device_id={'time': dst}, device_id_type=MESH)

    for other in other_chips():
        arrive(2 * other)
        arrive(2 * other + 1)
    arrive(partner)

    loads = [pltpu.make_async_copy(src, dst, load_sem.at[i]) for i, (src, dst) in enumerate(
        [(scale_hbm, scale_ref), (shift_hbm, shift_ref), (w2t_hbm, w2t_ref), (w1_hbm, w1_ref)])]
    for load in loads:
        load.start()
    x_copies = []
    for q in range(n_chunks):
        near = TOKENS[q] // 2
        for half in range(2):
            i = 2 * q + half
            start = half * (tokens // 2) + first_tok[q] // 2 * n_time + (me * near // 128) * 128
            x_copies.append(pltpu.make_async_copy(
                x_hbm.at[:, pl.ds(pl.multiple_of(start, 128), 128)], xcol.at[i], x_sem.at[i]))
            x_copies[-1].start()

    loads[0].wait()
    loads[1].wait()
    for n in range(n_rows):
        mod_send[pl.ds(n, 1), :] = scale_ref[:, n * TILE:(n + 1) * TILE]
        mod_send[pl.ds(n_rows + n, 1), :] = shift_ref[:, n * TILE:(n + 1) * TILE]
    step = jnp.broadcast_to(step_ref[...], (1, TILE))
    high = step.astype(jnp.bfloat16)
    rest = step - high.astype(jnp.float32)
    mid = rest.astype(jnp.bfloat16)
    low = (rest - mid.astype(jnp.float32)).astype(jnp.bfloat16)
    mod_send[pl.ds(2 * n_rows, 1), :] = high
    mod_send[pl.ds(2 * n_rows + 1, 1), :] = mid
    mod_send[pl.ds(2 * n_rows + 2, 1), :] = low
    mod_recv[me] = mod_send[...]

    loads[2].wait()
    w2[...] = w2t_ref[...].astype(jnp.float32).T.astype(jnp.bfloat16)
    for q in range(n_chunks):
        near = TOKENS[q] // 2
        lo = lax.rem(me * near, 128) // 8 * 8
        for half in range(2):
            i = 2 * q + half
            x_copies[i].wait()
            xrow[i] = xcol[i].T
            eight = xrow[i, pl.ds(pl.multiple_of(lo, 8), 8), :]
            if near == 4:
                eight = jnp.where(core == 1, eight[4:], eight[:4])
            x0[first_tok[q] + half * near:first_tok[q] + (half + 1) * near, :] = eight
    loads[3].wait()
    x0_rounded = x0[...].astype(jnp.bfloat16)
    for n in range(hidden // TILE):
        p0[:, n * TILE:(n + 1) * TILE] = jnp.dot(
            x0_rounded, w1_ref[:, n * TILE:(n + 1) * TILE], preferred_element_type=jnp.float32)

    pl.semaphore_wait(barrier, n_time - 1)

    def group(g, sign):
        z = along(place_z, sign * hop(g // 2)) * (SIDE * SIDE)
        chips = []
        for i in range(2):
            zy = z + along(place_y, sign * hop(2 * lax.rem(g, 2) + i)) * SIDE
            chips += [zy + along(place_x, sign * step) for step in NEAR]
        return chips

    def mod_copy(k, dst):
        return pltpu.make_async_remote_copy(
            src_ref=mod_send, dst_ref=mod_recv.at[me], send_sem=mod_send_sem, recv_sem=mod_recv_sem.at[k],
            device_id={'time': dst}, device_id_type=MESH)

    def pair_copy(k, src, src_ref):
        return pltpu.make_async_remote_copy(
            src_ref=src_ref, dst_ref=mod_recv.at[src], send_sem=pair_send_sem, recv_sem=pair_recv_sem.at[k],
            device_id={'time': partner}, device_id_type=MESH)

    def send_group(g, first=0):
        for i, other in enumerate(group(g, 1)[first:], first):
            mod_copy(g * ARRIVE + i, 2 * other + core).start()

    def relay_group(g, first=0):
        for i, other in enumerate(group(g, -1)[first:], first):
            mod_copy(g * ARRIVE + i, me).wait_recv()
            src = 2 * other + core
            pair_copy(g * ARRIVE + i, src, mod_recv.at[src]).start()

    def pair_wait(g):
        for i in range(ARRIVE):
            pair_copy(g * ARRIVE + i, me, mod_send).wait_recv()

    def unpack(g):
        for other in group(g, -1):
            for j in (2 * other, 2 * other + 1):
                block = mod_recv[j].astype(jnp.float32)
                mods[j, pl.ds(0, n_rows), :] = 0.5 * (1.0 + block[:n_rows])
                mods[j, pl.ds(n_rows, n_rows), :] = 0.5 * block[n_rows:2 * n_rows]
                mods[j, pl.ds(2 * n_rows, 1), :] = (block[2 * n_rows:2 * n_rows + 1] + block[2 * n_rows + 1:2 * n_rows + 2]) + block[2 * n_rows + 2:2 * n_rows + 3]

    n_groups = n_chips // ARRIVE
    pair_copy(0, me, mod_send).start()
    send_group(0, 1)
    for g in range(1, n_groups):
        send_group(g)
    relay_group(0, 1)
    pair_wait(0)
    unpack(0)

    def first_sweep(g, carry):
        pl.when(g + 1 < n_groups)(lambda: relay_group(g + 1))
        steps = [2 * other + c for other in group(g, -1) for c in range(2)]
        acc = None
        for n in range(hidden // TILE):
            parts = []
            for j in steps:
                h = p0[:, n * TILE:(n + 1) * TILE] * mods[j, pl.ds(n, 1), :] + mods[j, pl.ds(n_rows + n, 1), :]
                parts.append(half_gelu(h).astype(jnp.bfloat16))
            act = jnp.concatenate(parts, axis=0)
            prod = jnp.dot(act, w2[n * TILE:(n + 1) * TILE, :], preferred_element_type=jnp.float32)
            acc = prod if acc is None else acc + prod
        for i, j in enumerate(steps):
            drift[j] = mods[j, pl.ds(2 * n_rows, 1), :][:, :chans] * acc[i * n_tok:(i + 1) * n_tok, :]

        @pl.when(g + 1 < n_groups)
        def _():
            pair_wait(g + 1)
            unpack(g + 1)

        return carry

    lax.fori_loop(0, n_groups, first_sweep, 0)

    def first_prefix(i, total):
        news = []
        for j in (2 * i, 2 * i + 1):
            news.append(x0[...] + total)
            total = total + drift[j]
        for q in range(n_chunks):
            rows = slice(first_tok[q], first_tok[q] + TOKENS[q])
            pair = jnp.concatenate([news[0][rows], news[1][rows]], axis=0).astype(jnp.bfloat16)
            at = pl.ds(pl.multiple_of(i * 2 * TOKENS[q], 16), 2 * TOKENS[q])
            if q == 0:
                x_a[at, :] = pair
            else:
                x_b[q - 1, at, :] = pair
        return total

    lax.fori_loop(0, n_time // 2, first_prefix, jnp.zeros((n_tok, chans), jnp.float32), unroll=4)

    def block_step(tok, x_at, send_at, start, b, carry):
        steps = ROWS // tok
        acc = None
        x = x_at[pl.ds(pl.multiple_of(b * ROWS, ROWS), ROWS), :]
        for n in range(hidden // TILE):
            pre = jnp.dot(x, w1_ref[:, n * TILE:(n + 1) * TILE], preferred_element_type=jnp.float32)
            parts = []
            for s in range(steps):
                j = b * steps + s
                h = pre[s * tok:(s + 1) * tok] * mods[j, pl.ds(n, 1), :] + mods[j, pl.ds(n_rows + n, 1), :]
                parts.append(h)
            act = half_gelu(jnp.concatenate(parts, axis=0)).astype(jnp.bfloat16)
            prod = jnp.dot(act, w2[n * TILE:(n + 1) * TILE, :], preferred_element_type=jnp.float32)
            acc = prod if acc is None else acc + prod
        total = prefix[0:tok, :]
        for s in range(0, steps, 2):
            j = b * steps + s
            news = []
            for i in range(2):
                news.append(start + total)
                send_at[j + i, :, 0:chans] = news[i][:tok // 2]
                send_at[j + i, :, chans:2 * chans] = news[i][tok // 2:]
                total = total + mods[j + i, pl.ds(2 * n_rows, 1), :][:, :chans] * acc[(s + i) * tok:(s + i + 1) * tok, :]
            x_at[pl.ds(pl.multiple_of(j * tok, 2 * tok), 2 * tok), :] = jnp.concatenate(news, axis=0).astype(jnp.bfloat16)
        prefix[0:tok, :] = total
        return carry

    def later_sweeps(tok, x_at, send_at, start):
        def sweep(i, carry):
            prefix[...] = jnp.zeros_like(prefix)
            return lax.fori_loop(0, n_time * tok // ROWS, functools.partial(block_step, tok, x_at, send_at, start), carry)

        lax.fori_loop(1, SWEEPS, sweep, 0)

    def own_copy(q, send_at, out_at):
        return pltpu.make_async_copy(send_at.at[me], out_at.at[me], own_sem.at[q])

    def exchange(q, send_at, out_at):
        def out_copy(dst):
            return pltpu.make_async_remote_copy(
                src_ref=send_at.at[dst], dst_ref=out_at.at[me], send_sem=out_send_sem.at[q], recv_sem=out_recv_sem.at[q],
                device_id={'time': dst}, device_id_type=MESH)

        for other in other_chips():
            out_copy(2 * other + core).start()
            out_copy(2 * other + 1 - core).start()
        out_copy(partner).start()
        own_copy(q, send_at, out_at).start()

    later_sweeps(TOKENS[0], x_a, send_a, x0[0:TOKENS[0], :])
    exchange(0, send_a, out_a)

    def small_chunk(i, carry):
        start = x0[pl.ds(pl.multiple_of(TOKENS[0] + i * TOKENS[1], TOKENS[1]), TOKENS[1]), :]
        later_sweeps(TOKENS[1], x_b.at[i], send_b.at[i], start)
        exchange(1 + i, send_b.at[i], out_b.at[i])
        return carry

    lax.fori_loop(0, n_chunks - 1, small_chunk, 0)

    half_block = mod_recv.at[pl.ds(0, n_chips)]
    wait_bytes(half_block, pair_send_sem)
    wait_bytes(mod_recv.at[pl.ds(0, n_chips - 1)], mod_send_sem)
    for q in range(n_chunks):
        send_at, out_at = (send_a, out_a) if q == 0 else (send_b.at[q - 1], out_b.at[q - 1])
        own_copy(q, send_at, out_at).wait()
        wait_bytes(out_at.at[pl.ds(0, n_time - 1)], out_recv_sem.at[q])
        wait_bytes(send_at.at[pl.ds(0, n_time - 1)], out_send_sem.at[q])


def spread(a_hbm, b_hbm, out_hbm, rows, cols, in_sem, out_sem):
    chans, tokens = out_hbm.shape
    part = rows.shape[0] // SPREAD
    loads = []
    for i in range(SPREAD):
        src, at = (a_hbm, i * part) if i < SPREAD // 2 else (b_hbm, i * part - a_hbm.shape[0])
        loads.append(pltpu.make_async_copy(src.at[pl.ds(at, part)], rows.at[pl.ds(i * part, part)], in_sem.at[i]))
    for load in loads:
        load.start()
    stores = []
    for i in range(SPREAD):
        loads[i].wait()
        for at in range(i * part, (i + 1) * part, 128):
            block = rows[at:at + 128, :].T
            cols[:, at:at + 128] = block[:chans]
            cols[:, tokens // 2 + at:tokens // 2 + at + 128] = block[chans:]
        for half in range(2):
            at = pl.ds(half * (tokens // 2) + i * part, part)
            stores.append(pltpu.make_async_copy(cols.at[:, at], out_hbm.at[:, at], out_sem.at[2 * i + half]))
            stores[-1].start()
    for store in stores:
        store.wait()


def solution(mesh):
    n_time = mesh.shape['time']

    def per_device(x_init, w_in, w_out, mod_scale, mod_shift, step_size):
        _, tokens, chans = x_init.shape
        hidden = w_in.shape[1]
        n_tok = sum(TOKENS)
        f32, bf16 = jnp.float32, jnp.bfloat16
        vmem, hbm = pl.BlockSpec(memory_space=pltpu.VMEM), pl.BlockSpec(memory_space=pltpu.HBM)
        shape_a = (n_time, TOKENS[0] // 2, 2 * chans)
        shape_b = (len(TOKENS) - 1, n_time, TOKENS[1] // 2, 2 * chans)
        out_a, out_b = pl.pallas_call(
            functools.partial(kernel, n_time),
            out_shape=[jax.ShapeDtypeStruct(shape_a, f32), jax.ShapeDtypeStruct(shape_b, f32)],
            in_specs=[hbm] * 5 + [vmem],
            out_specs=[hbm, hbm],
            scratch_shapes=[
                pltpu.VMEM((chans, hidden), bf16),
                pltpu.VMEM((chans, hidden), bf16),
                pltpu.VMEM((1, hidden), bf16),
                pltpu.VMEM((1, hidden), bf16),
                pltpu.VMEM((2 * len(TOKENS), chans, 128), f32),
                pltpu.VMEM((2 * len(TOKENS), 128, chans), f32),
                pltpu.VMEM((n_tok, chans), f32),
                pltpu.VMEM((hidden, chans), bf16),
                pltpu.VMEM((16, TILE), bf16),
                pltpu.VMEM((n_time, 16, TILE), bf16),
                pltpu.VMEM((n_time, 24, TILE), f32),
                pltpu.VMEM((n_tok, hidden), f32),
                pltpu.VMEM((n_time, n_tok, chans), f32),
                pltpu.VMEM((n_time * TOKENS[0], chans), bf16),
                pltpu.VMEM((len(TOKENS) - 1, n_time * TOKENS[1], chans), bf16),
                pltpu.VMEM(shape_a, f32),
                pltpu.VMEM(shape_b, f32),
                pltpu.VMEM((TOKENS[0], chans), f32),
                pltpu.SemaphoreType.DMA((4,)),
                pltpu.SemaphoreType.DMA((2 * len(TOKENS),)),
                pltpu.SemaphoreType.DMA,
                pltpu.SemaphoreType.DMA((n_time // 2,)),
                pltpu.SemaphoreType.DMA,
                pltpu.SemaphoreType.DMA((n_time // 2,)),
                pltpu.SemaphoreType.DMA((len(TOKENS),)),
                pltpu.SemaphoreType.DMA((len(TOKENS),)),
                pltpu.SemaphoreType.DMA((len(TOKENS),)),
            ],
            compiler_params=pltpu.CompilerParams(has_side_effects=True, collective_id=0),
            name='sweeps',
        )(x_init[0].T, w_in, w_out.T, mod_scale, mod_shift, step_size[None])
        out = pl.pallas_call(
            spread, out_shape=jax.ShapeDtypeStruct((chans, tokens), f32), in_specs=[hbm, hbm], out_specs=hbm,
            scratch_shapes=[
                pltpu.VMEM((tokens // 2, 2 * chans), f32),
                pltpu.VMEM((chans, tokens), f32),
                pltpu.SemaphoreType.DMA((SPREAD,)),
                pltpu.SemaphoreType.DMA((2 * SPREAD,)),
            ],
            name='spread',
        )(out_a.reshape(-1, 2 * chans), out_b.reshape(-1, 2 * chans))
        return out.T.reshape(1, 1, tokens, chans)

    return jax.shard_map(per_device, mesh=mesh, in_specs=(P('data'), P(), P(), P('time'), P('time'), P('time')), out_specs=P('time', 'data'), check_vma=False)
```

```python
import functools

import jax
import jax.numpy as jnp
from jax import lax
from jax.experimental import pallas as pl
from jax.experimental.pallas import tpu as pltpu
from jax.sharding import PartitionSpec as P

SWEEPS = 4
C0 = 0.7978845608028654
C1 = C0 * 0.044715
TILE = 256
ROWS = 1024
TOKENS = (16, 8, 8)
SPREAD = 4
SIDE = 4
ARRIVE = 8
MESH = pl.DeviceIdType.MESH


def half_gelu(h):
    t = jnp.tanh(h * (h * h * (8.0 * C1) + 2.0 * C0))
    return h + h * t


def wait_bytes(ref, sem):
    pltpu.make_async_copy(ref, ref, sem).wait()


def plane(t):
    return t + (1 - 2 * (t // 2)) * lax.rem((t + 1) // 2, 2)


NEAR = (0, 1, 3, 2)


def hop(t):
    return t + (t // 2) * (1 - 2 * lax.rem(t, 2))


def kernel(n_time, x_hbm, w1_hbm, w2t_hbm, scale_hbm, shift_hbm, step_ref, out_a, out_b,
           w1_ref, w2t_ref, scale_ref, shift_ref, xcol, xrow, x0, w2, mod_send, mod_recv, mods, p0, drift, x_a, x_b, send_a, send_b, prefix,
           load_sem, x_sem, mod_send_sem, mod_recv_sem, pair_send_sem, pair_recv_sem, out_send_sem, out_recv_sem, own_sem):
    me = lax.axis_index('time')
    n_chips = n_time // 2
    chip = me // 2
    core = lax.rem(me, 2)
    partner = me + 1 - 2 * core
    chans, hidden = w1_ref.shape
    n_rows = hidden // TILE
    tokens = x_hbm.shape[1]
    n_chunks, n_tok = len(TOKENS), sum(TOKENS)
    first_tok = [sum(TOKENS[:q]) for q in range(n_chunks)]

    barrier = pltpu.get_barrier_semaphore()

    place_x, place_y, place_z = lax.rem(chip, SIDE), lax.rem(chip // SIDE, SIDE), chip // (SIDE * SIDE)

    def along(place, step):
        return lax.rem(place + step + SIDE, SIDE)

    xs = [along(place_x, step) for step in NEAR]
    ys = [along(place_y, step) * SIDE for step in NEAR]
    zs = [along(place_z, step) * (SIDE * SIDE) for step in NEAR]

    def other_chips():
        for k in range(n_chips - 1, 0, -1):
            yield zs[k // (SIDE * SIDE)] + ys[k // SIDE % SIDE] + xs[k % SIDE]

    def arrive(dst):
        pl.semaphore_signal(barrier, inc=1, device_id={'time': dst}, device_id_type=MESH)

    for other in other_chips():
        arrive(2 * other)
        arrive(2 * other + 1)
    arrive(partner)

    loads = [pltpu.make_async_copy(src, dst, load_sem.at[i]) for i, (src, dst) in enumerate(
        [(scale_hbm, scale_ref), (shift_hbm, shift_ref), (w2t_hbm, w2t_ref), (w1_hbm, w1_ref)])]
    for load in loads:
        load.start()
    x_copies = []
    for q in range(n_chunks):
        near = TOKENS[q] // 2
        for half in range(2):
            i = 2 * q + half
            start = half * (tokens // 2) + first_tok[q] // 2 * n_time + (me * near // 128) * 128
            x_copies.append(pltpu.make_async_copy(
                x_hbm.at[:, pl.ds(pl.multiple_of(start, 128), 128)], xcol.at[i], x_sem.at[i]))
            x_copies[-1].start()

    loads[0].wait()
    loads[1].wait()
    for n in range(n_rows):
        mod_send[pl.ds(n, 1), :] = scale_ref[:, n * TILE:(n + 1) * TILE]
        mod_send[pl.ds(n_rows + n, 1), :] = shift_ref[:, n * TILE:(n + 1) * TILE]
    step = jnp.broadcast_to(step_ref[...], (1, TILE))
    high = step.astype(jnp.bfloat16)
    rest = step - high.astype(jnp.float32)
    mid = rest.astype(jnp.bfloat16)
    low = (rest - mid.astype(jnp.float32)).astype(jnp.bfloat16)
    mod_send[pl.ds(2 * n_rows, 1), :] = high
    mod_send[pl.ds(2 * n_rows + 1, 1), :] = mid
    mod_send[pl.ds(2 * n_rows + 2, 1), :] = low
    mod_recv[me] = mod_send[...]

    loads[2].wait()
    w2[...] = w2t_ref[...].astype(jnp.float32).T.astype(jnp.bfloat16)
    for q in range(n_chunks):
        near = TOKENS[q] // 2
        lo = lax.rem(me * near, 128) // 8 * 8
        for half in range(2):
            i = 2 * q + half
            x_copies[i].wait()
            xrow[i] = xcol[i].T
            eight = xrow[i, pl.ds(pl.multiple_of(lo, 8), 8), :]
            if near == 4:
                eight = jnp.where(core == 1, eight[4:], eight[:4])
            x0[first_tok[q] + half * near:first_tok[q] + (half + 1) * near, :] = eight
    loads[3].wait()
    x0_rounded = x0[...].astype(jnp.bfloat16)
    for n in range(hidden // TILE):
        p0[:, n * TILE:(n + 1) * TILE] = jnp.dot(
            x0_rounded, w1_ref[:, n * TILE:(n + 1) * TILE], preferred_element_type=jnp.float32)

    pl.semaphore_wait(barrier, n_time - 1)

    def group(g, sign):
        z = along(place_z, sign * plane(g // 2)) * (SIDE * SIDE)
        chips = []
        for i in range(2):
            zy = z + along(place_y, sign * hop(2 * lax.rem(g, 2) + i)) * SIDE
            chips += [zy + along(place_x, sign * step) for step in NEAR]
        return chips

    def mod_copy(k, dst):
        return pltpu.make_async_remote_copy(
            src_ref=mod_send, dst_ref=mod_recv.at[me], send_sem=mod_send_sem, recv_sem=mod_recv_sem.at[k],
            device_id={'time': dst}, device_id_type=MESH)

    def pair_copy(k, src, src_ref):
        return pltpu.make_async_remote_copy(
            src_ref=src_ref, dst_ref=mod_recv.at[src], send_sem=pair_send_sem, recv_sem=pair_recv_sem.at[k],
            device_id={'time': partner}, device_id_type=MESH)

    def send_group(g, first=0):
        for i, other in enumerate(group(g, 1)[first:], first):
            mod_copy(g * ARRIVE + i, 2 * other + core).start()

    def relay_group(g, first=0):
        for i, other in enumerate(group(g, -1)[first:], first):
            mod_copy(g * ARRIVE + i, me).wait_recv()
            src = 2 * other + core
            pair_copy(g * ARRIVE + i, src, mod_recv.at[src]).start()

    def pair_wait(g):
        for i in range(ARRIVE):
            pair_copy(g * ARRIVE + i, me, mod_send).wait_recv()

    def unpack(g):
        for other in group(g, -1):
            for j in (2 * other, 2 * other + 1):
                block = mod_recv[j].astype(jnp.float32)
                mods[j, pl.ds(0, n_rows), :] = 0.5 * (1.0 + block[:n_rows])
                mods[j, pl.ds(n_rows, n_rows), :] = 0.5 * block[n_rows:2 * n_rows]
                mods[j, pl.ds(2 * n_rows, 1), :] = (block[2 * n_rows:2 * n_rows + 1] + block[2 * n_rows + 1:2 * n_rows + 2]) + block[2 * n_rows + 2:2 * n_rows + 3]

    n_groups = n_chips // ARRIVE
    pair_copy(0, me, mod_send).start()
    send_group(0, 1)
    for g in range(1, n_groups):
        send_group(g)
    relay_group(0, 1)
    pair_wait(0)
    unpack(0)

    def first_sweep(g, carry):
        pl.when(g + 1 < n_groups)(lambda: relay_group(g + 1))
        steps = [2 * other + c for other in group(g, -1) for c in range(2)]
        acc = None
        for n in range(hidden // TILE):
            parts = []
            for j in steps:
                h = p0[:, n * TILE:(n + 1) * TILE] * mods[j, pl.ds(n, 1), :] + mods[j, pl.ds(n_rows + n, 1), :]
                parts.append(half_gelu(h).astype(jnp.bfloat16))
            act = jnp.concatenate(parts, axis=0)
            prod = jnp.dot(act, w2[n * TILE:(n + 1) * TILE, :], preferred_element_type=jnp.float32)
            acc = prod if acc is None else acc + prod
        for i, j in enumerate(steps):
            drift[j] = mods[j, pl.ds(2 * n_rows, 1), :][:, :chans] * acc[i * n_tok:(i + 1) * n_tok, :]

        @pl.when(g + 1 < n_groups)
        def _():
            pair_wait(g + 1)
            unpack(g + 1)

        return carry

    lax.fori_loop(0, n_groups, first_sweep, 0)

    def first_prefix(i, total):
        news = []
        for j in (2 * i, 2 * i + 1):
            news.append(x0[...] + total)
            total = total + drift[j]
        for q in range(n_chunks):
            rows = slice(first_tok[q], first_tok[q] + TOKENS[q])
            pair = jnp.concatenate([news[0][rows], news[1][rows]], axis=0).astype(jnp.bfloat16)
            at = pl.ds(pl.multiple_of(i * 2 * TOKENS[q], 16), 2 * TOKENS[q])
            if q == 0:
                x_a[at, :] = pair
            else:
                x_b[q - 1, at, :] = pair
        return total

    lax.fori_loop(0, n_time // 2, first_prefix, jnp.zeros((n_tok, chans), jnp.float32), unroll=4)

    def block_step(tok, x_at, send_at, start, b, carry):
        steps = ROWS // tok
        acc = None
        x = x_at[pl.ds(pl.multiple_of(b * ROWS, ROWS), ROWS), :]
        for n in range(hidden // TILE):
            pre = jnp.dot(x, w1_ref[:, n * TILE:(n + 1) * TILE], preferred_element_type=jnp.float32)
            parts = []
            for s in range(steps):
                j = b * steps + s
                h = pre[s * tok:(s + 1) * tok] * mods[j, pl.ds(n, 1), :] + mods[j, pl.ds(n_rows + n, 1), :]
                parts.append(h)
            act = half_gelu(jnp.concatenate(parts, axis=0)).astype(jnp.bfloat16)
            prod = jnp.dot(act, w2[n * TILE:(n + 1) * TILE, :], preferred_element_type=jnp.float32)
            acc = prod if acc is None else acc + prod
        total = prefix[0:tok, :]
        for s in range(0, steps, 2):
            j = b * steps + s
            news = []
            for i in range(2):
                news.append(start + total)
                send_at[j + i, :, 0:chans] = news[i][:tok // 2]
                send_at[j + i, :, chans:2 * chans] = news[i][tok // 2:]
                total = total + mods[j + i, pl.ds(2 * n_rows, 1), :][:, :chans] * acc[(s + i) * tok:(s + i + 1) * tok, :]
            x_at[pl.ds(pl.multiple_of(j * tok, 2 * tok), 2 * tok), :] = jnp.concatenate(news, axis=0).astype(jnp.bfloat16)
        prefix[0:tok, :] = total
        return carry

    def later_sweeps(tok, x_at, send_at, start):
        def sweep(i, carry):
            prefix[...] = jnp.zeros_like(prefix)
            return lax.fori_loop(0, n_time * tok // ROWS, functools.partial(block_step, tok, x_at, send_at, start), carry)

        lax.fori_loop(1, SWEEPS, sweep, 0)

    def own_copy(q, send_at, out_at):
        return pltpu.make_async_copy(send_at.at[me], out_at.at[me], own_sem.at[q])

    def exchange(q, send_at, out_at):
        def out_copy(dst):
            return pltpu.make_async_remote_copy(
                src_ref=send_at.at[dst], dst_ref=out_at.at[me], send_sem=out_send_sem.at[q], recv_sem=out_recv_sem.at[q],
                device_id={'time': dst}, device_id_type=MESH)

        for other in other_chips():
            out_copy(2 * other + core).start()
            out_copy(2 * other + 1 - core).start()
        out_copy(partner).start()
        own_copy(q, send_at, out_at).start()

    later_sweeps(TOKENS[0], x_a, send_a, x0[0:TOKENS[0], :])
    exchange(0, send_a, out_a)

    def small_chunk(i, carry):
        start = x0[pl.ds(pl.multiple_of(TOKENS[0] + i * TOKENS[1], TOKENS[1]), TOKENS[1]), :]
        later_sweeps(TOKENS[1], x_b.at[i], send_b.at[i], start)
        exchange(1 + i, send_b.at[i], out_b.at[i])
        return carry

    lax.fori_loop(0, n_chunks - 1, small_chunk, 0)

    half_block = mod_recv.at[pl.ds(0, n_chips)]
    wait_bytes(half_block, pair_send_sem)
    wait_bytes(mod_recv.at[pl.ds(0, n_chips - 1)], mod_send_sem)
    for q in range(n_chunks):
        send_at, out_at = (send_a, out_a) if q == 0 else (send_b.at[q - 1], out_b.at[q - 1])
        own_copy(q, send_at, out_at).wait()
        wait_bytes(out_at.at[pl.ds(0, n_time - 1)], out_recv_sem.at[q])
        wait_bytes(send_at.at[pl.ds(0, n_time - 1)], out_send_sem.at[q])


def spread(a_hbm, b_hbm, out_hbm, rows, cols, in_sem, out_sem):
    chans, tokens = out_hbm.shape
    part = rows.shape[0] // SPREAD
    loads = []
    for i in range(SPREAD):
        src, at = (a_hbm, i * part) if i < SPREAD // 2 else (b_hbm, i * part - a_hbm.shape[0])
        loads.append(pltpu.make_async_copy(src.at[pl.ds(at, part)], rows.at[pl.ds(i * part, part)], in_sem.at[i]))
    for load in loads:
        load.start()
    stores = []
    for i in range(SPREAD):
        loads[i].wait()
        for at in range(i * part, (i + 1) * part, 128):
            block = rows[at:at + 128, :].T
            cols[:, at:at + 128] = block[:chans]
            cols[:, tokens // 2 + at:tokens // 2 + at + 128] = block[chans:]
        for half in range(2):
            at = pl.ds(half * (tokens // 2) + i * part, part)
            stores.append(pltpu.make_async_copy(cols.at[:, at], out_hbm.at[:, at], out_sem.at[2 * i + half]))
            stores[-1].start()
    for store in stores:
        store.wait()


def solution(mesh):
    n_time = mesh.shape['time']

    def per_device(x_init, w_in, w_out, mod_scale, mod_shift, step_size):
        _, tokens, chans = x_init.shape
        hidden = w_in.shape[1]
        n_tok = sum(TOKENS)
        f32, bf16 = jnp.float32, jnp.bfloat16
        vmem, hbm = pl.BlockSpec(memory_space=pltpu.VMEM), pl.BlockSpec(memory_space=pltpu.HBM)
        shape_a = (n_time, TOKENS[0] // 2, 2 * chans)
        shape_b = (len(TOKENS) - 1, n_time, TOKENS[1] // 2, 2 * chans)
        out_a, out_b = pl.pallas_call(
            functools.partial(kernel, n_time),
            out_shape=[jax.ShapeDtypeStruct(shape_a, f32), jax.ShapeDtypeStruct(shape_b, f32)],
            in_specs=[hbm] * 5 + [vmem],
            out_specs=[hbm, hbm],
            scratch_shapes=[
                pltpu.VMEM((chans, hidden), bf16),
                pltpu.VMEM((chans, hidden), bf16),
                pltpu.VMEM((1, hidden), bf16),
                pltpu.VMEM((1, hidden), bf16),
                pltpu.VMEM((2 * len(TOKENS), chans, 128), f32),
                pltpu.VMEM((2 * len(TOKENS), 128, chans), f32),
                pltpu.VMEM((n_tok, chans), f32),
                pltpu.VMEM((hidden, chans), bf16),
                pltpu.VMEM((16, TILE), bf16),
                pltpu.VMEM((n_time, 16, TILE), bf16),
                pltpu.VMEM((n_time, 24, TILE), f32),
                pltpu.VMEM((n_tok, hidden), f32),
                pltpu.VMEM((n_time, n_tok, chans), f32),
                pltpu.VMEM((n_time * TOKENS[0], chans), bf16),
                pltpu.VMEM((len(TOKENS) - 1, n_time * TOKENS[1], chans), bf16),
                pltpu.VMEM(shape_a, f32),
                pltpu.VMEM(shape_b, f32),
                pltpu.VMEM((TOKENS[0], chans), f32),
                pltpu.SemaphoreType.DMA((4,)),
                pltpu.SemaphoreType.DMA((2 * len(TOKENS),)),
                pltpu.SemaphoreType.DMA,
                pltpu.SemaphoreType.DMA((n_time // 2,)),
                pltpu.SemaphoreType.DMA,
                pltpu.SemaphoreType.DMA((n_time // 2,)),
                pltpu.SemaphoreType.DMA((len(TOKENS),)),
                pltpu.SemaphoreType.DMA((len(TOKENS),)),
                pltpu.SemaphoreType.DMA((len(TOKENS),)),
            ],
            compiler_params=pltpu.CompilerParams(has_side_effects=True, collective_id=0),
            name='sweeps',
        )(x_init[0].T, w_in, w_out.T, mod_scale, mod_shift, step_size[None])
        out = pl.pallas_call(
            spread, out_shape=jax.ShapeDtypeStruct((chans, tokens), f32), in_specs=[hbm, hbm], out_specs=hbm,
            scratch_shapes=[
                pltpu.VMEM((tokens // 2, 2 * chans), f32),
                pltpu.VMEM((chans, tokens), f32),
                pltpu.SemaphoreType.DMA((SPREAD,)),
                pltpu.SemaphoreType.DMA((2 * SPREAD,)),
            ],
            name='spread',
        )(out_a.reshape(-1, 2 * chans), out_b.reshape(-1, 2 * chans))
        return out.T.reshape(1, 1, tokens, chans)

    return jax.shard_map(per_device, mesh=mesh, in_specs=(P('data'), P(), P(), P('time'), P('time'), P('time')), out_specs=P('time', 'data'), check_vma=False)
```

```python
import functools

import jax
import jax.numpy as jnp
from jax import lax
from jax.experimental import pallas as pl
from jax.experimental.pallas import tpu as pltpu
from jax.sharding import PartitionSpec as P

SWEEPS = 4
C0 = 0.7978845608028654
C1 = C0 * 0.044715
BF16_MAX = float(jnp.finfo(jnp.bfloat16).max)
TILE = 256
ROWS = 1024
TOKENS = (16, 8, 8)
SPREAD = 2
SIDE = 4
ARRIVE = 8
MESH = pl.DeviceIdType.MESH


def half_gelu(h):
    t = jnp.tanh(h * (h * h * (8.0 * C1) + 2.0 * C0))
    return h + h * t


def wait_bytes(ref, sem):
    pltpu.make_async_copy(ref, ref, sem).wait()


NEAR = (0, 1, 3, 2)


def hop(t):
    return t + (t // 2) * (1 - 2 * lax.rem(t, 2))


def kernel(n_time, x_hbm, w1_hbm, w2t_hbm, scale_hbm, shift_hbm, step_ref, out_a, out_b,
           w1_ref, w2t_ref, scale_ref, shift_ref, xcol, xrow, x0, w2, mod_send, mod_recv, mods, p0, drift, x_a, x_b, send_a, send_b, prefix,
           load_sem, x_sem, mod_send_sem, mod_recv_sem, pair_send_sem, pair_recv_sem, out_send_sem, out_recv_sem, own_sem):
    me = lax.axis_index('time')
    n_chips = n_time // 2
    chip = me // 2
    core = lax.rem(me, 2)
    partner = me + 1 - 2 * core
    chans, hidden = w1_ref.shape
    n_rows = hidden // TILE
    tokens = x_hbm.shape[1]
    n_chunks, n_tok = len(TOKENS), sum(TOKENS)
    first_tok = [sum(TOKENS[:q]) for q in range(n_chunks)]

    barrier = pltpu.get_barrier_semaphore()

    place_x, place_y, place_z = lax.rem(chip, SIDE), lax.rem(chip // SIDE, SIDE), chip // (SIDE * SIDE)

    def along(place, step):
        return lax.rem(place + step + SIDE, SIDE)

    xs = [along(place_x, step) for step in NEAR]
    ys = [along(place_y, step) * SIDE for step in NEAR]
    zs = [along(place_z, step) * (SIDE * SIDE) for step in NEAR]

    def other_chips():
        for k in range(n_chips - 1, 0, -1):
            yield zs[k // (SIDE * SIDE)] + ys[k // SIDE % SIDE] + xs[k % SIDE]

    def arrive(dst):
        pl.semaphore_signal(barrier, inc=1, device_id={'time': dst}, device_id_type=MESH)

    for other in other_chips():
        arrive(2 * other)
        arrive(2 * other + 1)
    arrive(partner)

    loads = [pltpu.make_async_copy(src, dst, load_sem.at[i]) for i, (src, dst) in enumerate(
        [(scale_hbm, scale_ref), (shift_hbm, shift_ref), (w2t_hbm, w2t_ref), (w1_hbm, w1_ref)])]
    for load in loads:
        load.start()
    x_copies = []
    for q in range(n_chunks):
        near = TOKENS[q] // 2
        for half in range(2):
            i = 2 * q + half
            start = half * (tokens // 2) + first_tok[q] // 2 * n_time + (me * near // 128) * 128
            x_copies.append(pltpu.make_async_copy(
                x_hbm.at[:, pl.ds(pl.multiple_of(start, 128), 128)], xcol.at[i], x_sem.at[i]))
            x_copies[-1].start()

    loads[0].wait()
    loads[1].wait()
    for n in range(n_rows):
        mod_send[pl.ds(n, 1), :] = scale_ref[:, n * TILE:(n + 1) * TILE]
        mod_send[pl.ds(n_rows + n, 1), :] = shift_ref[:, n * TILE:(n + 1) * TILE]
    step = jnp.broadcast_to(step_ref[...], (1, TILE))
    high = jnp.minimum(step, BF16_MAX).astype(jnp.bfloat16)
    rest = step - high.astype(jnp.float32)
    mid = rest.astype(jnp.bfloat16)
    low = (rest - mid.astype(jnp.float32)).astype(jnp.bfloat16)
    mod_send[pl.ds(2 * n_rows, 1), :] = high
    mod_send[pl.ds(2 * n_rows + 1, 1), :] = mid
    mod_send[pl.ds(2 * n_rows + 2, 1), :] = low
    mod_recv[me] = mod_send[...]

    loads[2].wait()
    w2[...] = w2t_ref[...].astype(jnp.float32).T.astype(jnp.bfloat16)
    for q in range(n_chunks):
        near = TOKENS[q] // 2
        lo = lax.rem(me * near, 128) // 8 * 8
        for half in range(2):
            i = 2 * q + half
            x_copies[i].wait()
            xrow[i] = xcol[i].T
            eight = xrow[i, pl.ds(pl.multiple_of(lo, 8), 8), :]
            if near == 4:
                eight = jnp.where(core == 1, eight[4:], eight[:4])
            x0[first_tok[q] + half * near:first_tok[q] + (half + 1) * near, :] = eight
    loads[3].wait()
    x0_rounded = x0[...].astype(jnp.bfloat16)
    for n in range(hidden // TILE):
        p0[:, n * TILE:(n + 1) * TILE] = jnp.dot(
            x0_rounded, w1_ref[:, n * TILE:(n + 1) * TILE], preferred_element_type=jnp.float32)

    pl.semaphore_wait(barrier, n_time - 1)

    def group(g, sign):
        z = along(place_z, sign * hop(g // 2)) * (SIDE * SIDE)
        chips = []
        for i in range(2):
            zy = z + along(place_y, sign * hop(2 * lax.rem(g, 2) + i)) * SIDE
            chips += [zy + along(place_x, sign * step) for step in NEAR]
        return chips

    def mod_copy(k, dst):
        return pltpu.make_async_remote_copy(
            src_ref=mod_send, dst_ref=mod_recv.at[me], send_sem=mod_send_sem, recv_sem=mod_recv_sem.at[k],
            device_id={'time': dst}, device_id_type=MESH)

    def pair_copy(k, src, src_ref):
        return pltpu.make_async_remote_copy(
            src_ref=src_ref, dst_ref=mod_recv.at[src], send_sem=pair_send_sem, recv_sem=pair_recv_sem.at[k],
            device_id={'time': partner}, device_id_type=MESH)

    def send_group(g, first=0):
        for i, other in enumerate(group(g, 1)[first:], first):
            mod_copy(g * ARRIVE + i, 2 * other + core).start()

    def relay_group(g, first=0):
        for i, other in enumerate(group(g, -1)[first:], first):
            mod_copy(g * ARRIVE + i, me).wait_recv()
            src = 2 * other + core
            pair_copy(g * ARRIVE + i, src, mod_recv.at[src]).start()

    def pair_wait(g):
        for i in range(ARRIVE):
            pair_copy(g * ARRIVE + i, me, mod_send).wait_recv()

    def unpack(g):
        for other in group(g, -1):
            for j in (2 * other, 2 * other + 1):
                block = mod_recv[j].astype(jnp.float32)
                mods[j, pl.ds(0, n_rows), :] = 0.5 * (1.0 + block[:n_rows])
                mods[j, pl.ds(n_rows, n_rows), :] = 0.5 * block[n_rows:2 * n_rows]
                mods[j, pl.ds(2 * n_rows, 1), :] = (block[2 * n_rows:2 * n_rows + 1] + block[2 * n_rows + 1:2 * n_rows + 2]) + block[2 * n_rows + 2:2 * n_rows + 3]

    n_groups = n_chips // ARRIVE
    pair_copy(0, me, mod_send).start()
    send_group(0, 1)
    for g in range(1, n_groups):
        send_group(g)
    relay_group(0, 1)
    pair_wait(0)
    unpack(0)

    def first_sweep(g, carry):
        pl.when(g + 1 < n_groups)(lambda: relay_group(g + 1))
        steps = [2 * other + c for other in group(g, -1) for c in range(2)]
        acc = None
        for n in range(hidden // TILE):
            parts = []
            for j in steps:
                h = p0[:, n * TILE:(n + 1) * TILE] * mods[j, pl.ds(n, 1), :] + mods[j, pl.ds(n_rows + n, 1), :]
                parts.append(half_gelu(h).astype(jnp.bfloat16))
            act = jnp.concatenate(parts, axis=0)
            prod = jnp.dot(act, w2[n * TILE:(n + 1) * TILE, :], preferred_element_type=jnp.float32)
            acc = prod if acc is None else acc + prod
        for i, j in enumerate(steps):
            drift[j] = mods[j, pl.ds(2 * n_rows, 1), :][:, :chans] * acc[i * n_tok:(i + 1) * n_tok, :]

        @pl.when(g + 1 < n_groups)
        def _():
            pair_wait(g + 1)
            unpack(g + 1)

        return carry

    lax.fori_loop(0, n_groups, first_sweep, 0)

    def first_prefix(i, total):
        news = []
        for j in (2 * i, 2 * i + 1):
            news.append(x0[...] + total)
            total = total + drift[j]
        for q in range(n_chunks):
            rows = slice(first_tok[q], first_tok[q] + TOKENS[q])
            pair = jnp.concatenate([news[0][rows], news[1][rows]], axis=0).astype(jnp.bfloat16)
            at = pl.ds(pl.multiple_of(i * 2 * TOKENS[q], 16), 2 * TOKENS[q])
            if q == 0:
                x_a[at, :] = pair
            else:
                x_b[q - 1, at, :] = pair
        return total

    lax.fori_loop(0, n_time // 2, first_prefix, jnp.zeros((n_tok, chans), jnp.float32), unroll=4)

    def block_step(tok, x_at, send_at, start, b, carry):
        steps = ROWS // tok
        acc = None
        x = x_at[pl.ds(pl.multiple_of(b * ROWS, ROWS), ROWS), :]
        for n in range(hidden // TILE):
            pre = jnp.dot(x, w1_ref[:, n * TILE:(n + 1) * TILE], preferred_element_type=jnp.float32)
            parts = []
            for s in range(steps):
                j = b * steps + s
                h = pre[s * tok:(s + 1) * tok] * mods[j, pl.ds(n, 1), :] + mods[j, pl.ds(n_rows + n, 1), :]
                parts.append(h)
            act = half_gelu(jnp.concatenate(parts, axis=0)).astype(jnp.bfloat16)
            prod = jnp.dot(act, w2[n * TILE:(n + 1) * TILE, :], preferred_element_type=jnp.float32)
            acc = prod if acc is None else acc + prod
        total = prefix[0:tok, :]
        for s in range(0, steps, 2):
            j = b * steps + s
            news = []
            for i in range(2):
                news.append(start + total)
                send_at[j + i, :, 0:chans] = news[i][:tok // 2]
                send_at[j + i, :, chans:2 * chans] = news[i][tok // 2:]
                total = total + mods[j + i, pl.ds(2 * n_rows, 1), :][:, :chans] * acc[(s + i) * tok:(s + i + 1) * tok, :]
            x_at[pl.ds(pl.multiple_of(j * tok, 2 * tok), 2 * tok), :] = jnp.concatenate(news, axis=0).astype(jnp.bfloat16)
        prefix[0:tok, :] = total
        return carry

    def later_sweeps(tok, x_at, send_at, start):
        def sweep(i, carry):
            prefix[...] = jnp.zeros_like(prefix)
            return lax.fori_loop(0, n_time * tok // ROWS, functools.partial(block_step, tok, x_at, send_at, start), carry)

        lax.fori_loop(1, SWEEPS, sweep, 0)

    def own_copy(q, send_at, out_at):
        return pltpu.make_async_copy(send_at.at[me], out_at.at[me], own_sem.at[q])

    def exchange(q, send_at, out_at):
        def out_copy(dst):
            return pltpu.make_async_remote_copy(
                src_ref=send_at.at[dst], dst_ref=out_at.at[me], send_sem=out_send_sem.at[q], recv_sem=out_recv_sem.at[q],
                device_id={'time': dst}, device_id_type=MESH)

        for other in other_chips():
            out_copy(2 * other + core).start()
            out_copy(2 * other + 1 - core).start()
        out_copy(partner).start()
        own_copy(q, send_at, out_at).start()

    later_sweeps(TOKENS[0], x_a, send_a, x0[0:TOKENS[0], :])
    exchange(0, send_a, out_a)

    def small_chunk(i, carry):
        start = x0[pl.ds(pl.multiple_of(TOKENS[0] + i * TOKENS[1], TOKENS[1]), TOKENS[1]), :]
        later_sweeps(TOKENS[1], x_b.at[i], send_b.at[i], start)
        exchange(1 + i, send_b.at[i], out_b.at[i])
        return carry

    lax.fori_loop(0, n_chunks - 1, small_chunk, 0)

    half_block = mod_recv.at[pl.ds(0, n_chips)]
    wait_bytes(half_block, pair_send_sem)
    wait_bytes(mod_recv.at[pl.ds(0, n_chips - 1)], mod_send_sem)
    for q in range(n_chunks):
        send_at, out_at = (send_a, out_a) if q == 0 else (send_b.at[q - 1], out_b.at[q - 1])
        own_copy(q, send_at, out_at).wait()
        wait_bytes(out_at.at[pl.ds(0, n_time - 1)], out_recv_sem.at[q])
        wait_bytes(send_at.at[pl.ds(0, n_time - 1)], out_send_sem.at[q])


def spread(a_hbm, b_hbm, out_hbm, rows, cols, in_sem, out_sem):
    chans, tokens = out_hbm.shape
    part = rows.shape[0] // SPREAD
    loads = []
    for i in range(SPREAD):
        src, at = (a_hbm, i * part) if i < SPREAD // 2 else (b_hbm, i * part - a_hbm.shape[0])
        loads.append(pltpu.make_async_copy(src.at[pl.ds(at, part)], rows.at[pl.ds(i * part, part)], in_sem.at[i]))
    for load in loads:
        load.start()
    stores = []
    for i in range(SPREAD):
        loads[i].wait()
        for at in range(i * part, (i + 1) * part, 128):
            block = rows[at:at + 128, :].T
            cols[:, at:at + 128] = block[:chans]
            cols[:, tokens // 2 + at:tokens // 2 + at + 128] = block[chans:]
        for half in range(2):
            at = pl.ds(half * (tokens // 2) + i * part, part)
            stores.append(pltpu.make_async_copy(cols.at[:, at], out_hbm.at[:, at], out_sem.at[2 * i + half]))
            stores[-1].start()
    for store in stores:
        store.wait()


def solution(mesh):
    n_time = mesh.shape['time']

    def per_device(x_init, w_in, w_out, mod_scale, mod_shift, step_size):
        _, tokens, chans = x_init.shape
        hidden = w_in.shape[1]
        n_tok = sum(TOKENS)
        f32, bf16 = jnp.float32, jnp.bfloat16
        vmem, hbm = pl.BlockSpec(memory_space=pltpu.VMEM), pl.BlockSpec(memory_space=pltpu.HBM)
        shape_a = (n_time, TOKENS[0] // 2, 2 * chans)
        shape_b = (len(TOKENS) - 1, n_time, TOKENS[1] // 2, 2 * chans)
        out_a, out_b = pl.pallas_call(
            functools.partial(kernel, n_time),
            out_shape=[jax.ShapeDtypeStruct(shape_a, f32), jax.ShapeDtypeStruct(shape_b, f32)],
            in_specs=[hbm] * 5 + [vmem],
            out_specs=[hbm, hbm],
            scratch_shapes=[
                pltpu.VMEM((chans, hidden), bf16),
                pltpu.VMEM((chans, hidden), bf16),
                pltpu.VMEM((1, hidden), bf16),
                pltpu.VMEM((1, hidden), bf16),
                pltpu.VMEM((2 * len(TOKENS), chans, 128), f32),
                pltpu.VMEM((2 * len(TOKENS), 128, chans), f32),
                pltpu.VMEM((n_tok, chans), f32),
                pltpu.VMEM((hidden, chans), bf16),
                pltpu.VMEM((16, TILE), bf16),
                pltpu.VMEM((n_time, 16, TILE), bf16),
                pltpu.VMEM((n_time, 24, TILE), f32),
                pltpu.VMEM((n_tok, hidden), f32),
                pltpu.VMEM((n_time, n_tok, chans), f32),
                pltpu.VMEM((n_time * TOKENS[0], chans), bf16),
                pltpu.VMEM((len(TOKENS) - 1, n_time * TOKENS[1], chans), bf16),
                pltpu.VMEM(shape_a, f32),
                pltpu.VMEM(shape_b, f32),
                pltpu.VMEM((TOKENS[0], chans), f32),
                pltpu.SemaphoreType.DMA((4,)),
                pltpu.SemaphoreType.DMA((2 * len(TOKENS),)),
                pltpu.SemaphoreType.DMA,
                pltpu.SemaphoreType.DMA((n_time // 2,)),
                pltpu.SemaphoreType.DMA,
                pltpu.SemaphoreType.DMA((n_time // 2,)),
                pltpu.SemaphoreType.DMA((len(TOKENS),)),
                pltpu.SemaphoreType.DMA((len(TOKENS),)),
                pltpu.SemaphoreType.DMA((len(TOKENS),)),
            ],
            compiler_params=pltpu.CompilerParams(has_side_effects=True, collective_id=0),
            name='sweeps',
        )(x_init[0].T, w_in, w_out.T, mod_scale, mod_shift, step_size[None])
        out = pl.pallas_call(
            spread, out_shape=jax.ShapeDtypeStruct((chans, tokens), f32), in_specs=[hbm, hbm], out_specs=hbm,
            scratch_shapes=[
                pltpu.VMEM((tokens // 2, 2 * chans), f32),
                pltpu.VMEM((chans, tokens), f32),
                pltpu.SemaphoreType.DMA((SPREAD,)),
                pltpu.SemaphoreType.DMA((2 * SPREAD,)),
            ],
            name='spread',
        )(out_a.reshape(-1, 2 * chans), out_b.reshape(-1, 2 * chans))
        return out.T.reshape(1, 1, tokens, chans)

    return jax.shard_map(per_device, mesh=mesh, in_specs=(P('data'), P(), P(), P('time'), P('time'), P('time')), out_specs=P('time', 'data'), check_vma=False)
```
